8 devices in a mesh: dp: 1 (over z), tp: 2 (over y), sp: 4 (over x, core).
Axes of the slice: x: 2, y: 2, z: 1, core: 2. Of those that a mesh axis runs over, the one named last changes fastest.
Arguments:
- step_emb: bfloat16 [4, 32, 1024], P(None, 'dp')
- v_cache: bfloat16 [2, 32, 1024, 1024], P(None, 'dp', 'sp', 'tp')
- z_cache: bfloat16 [2, 32, 1024, 1024], P(None, 'dp', 'sp', 'tp')
- short_state: bfloat16 [2, 32, 2, 3, 1024], P(None, 'dp', None, None, 'tp')
- w_in: bfloat16 [2, 1024, 3, 1024], P(None, None, None, 'tp')
- b_in: float32 [2, 3, 1024], P(None, None, 'tp')
- short_taps: float32 [2, 3, 3, 1024], P(None, None, None, 'tp')
- long_filt: float32 [2, 2, 1024, 1024], P(None, None, None, 'tp')
- skip_gain: float32 [2, 2, 1024], P(None, None, 'tp')
- w_out: bfloat16 [2, 1024, 1024], P(None, 'tp')
- b_out: float32 [2, 1024], replicated
- w_up: bfloat16 [2, 1024, 4096], P(None, None, 'tp')
- w_down: bfloat16 [2, 4096, 1024], P(None, 'tp')
Outputs:
- output 1: float32 [4, 32, 1024], P(None, 'dp')
- output 2: bfloat16 [2, 32, 1024, 1024], P(None, 'dp', 'sp', 'tp')
- output 3: bfloat16 [2, 32, 1024, 1024], P(None, 'dp', 'sp', 'tp')
- output 4: bfloat16 [2, 32, 2, 3, 1024], P(None, 'dp', None, None, 'tp')
All inputs are finite; a program needn't handle non-finite values.
Results may differ from the reference program's by a relative error of at most 0.0117668.
Values sent between devices are 32-bit elements.
A program may use at most 1 GiB of HBM per device.

```python
import jax
import jax.numpy as jnp
from jax import lax

MODEL_DIM = 1024
MLP_DIM = 4096
NUM_SEQ = 32
CACHE_LEN = 1024
NUM_STEPS = 4
NUM_LAYERS = 2
START_POS = CACHE_LEN * 3 // 4


def setup_inputs(seed: int = 0, part: int = 0) -> dict:
    root_key = jax.random.key(seed)
    part_root, shared_root = jax.random.split(root_key)
    part_keys = jax.random.split(jax.random.fold_in(part_root, part), 4)
    shared_keys = jax.random.split(shared_root, 9)
    filled_mask = (jnp.arange(CACHE_LEN) < START_POS)[None, None, :, None]
    lag_pos = jnp.arange(CACHE_LEN).astype(jnp.float32)
    decay_rows = jnp.exp(-0.5 * lag_pos / CACHE_LEN)[:, None]
    cache_shape = (NUM_LAYERS, NUM_SEQ, CACHE_LEN, MODEL_DIM)
    step_emb = jax.random.normal(part_keys[0], (NUM_STEPS, NUM_SEQ, MODEL_DIM), jnp.float32)
    v_cache = jax.random.normal(part_keys[1], cache_shape, jnp.float32) * filled_mask
    z_cache = jax.random.normal(part_keys[2], cache_shape, jnp.float32) * filled_mask
    short_state = jax.random.normal(part_keys[3], (NUM_LAYERS, NUM_SEQ, 2, 3, MODEL_DIM), jnp.float32)
    w_in = jax.random.normal(shared_keys[0], (NUM_LAYERS, MODEL_DIM, 3, MODEL_DIM), jnp.float32) * MODEL_DIM ** -0.5
    b_in = 0.5 * jax.random.normal(shared_keys[1], (NUM_LAYERS, 3, MODEL_DIM), jnp.float32)
    short_taps = 0.6 * jax.random.normal(shared_keys[2], (NUM_LAYERS, 3, 3, MODEL_DIM), jnp.float32)
    long_filt = jax.random.normal(shared_keys[3], (NUM_LAYERS, 2, CACHE_LEN, MODEL_DIM), jnp.float32) * decay_rows * (1.4 * CACHE_LEN ** -0.5)
    skip_gain = 0.6 * jax.random.normal(shared_keys[4], (NUM_LAYERS, 2, MODEL_DIM), jnp.float32)
    w_out = jax.random.normal(shared_keys[5], (NUM_LAYERS, MODEL_DIM, MODEL_DIM), jnp.float32) * MODEL_DIM ** -0.5
    b_out = 0.5 * jax.random.normal(shared_keys[6], (NUM_LAYERS, MODEL_DIM), jnp.float32)
    w_up = jax.random.normal(shared_keys[7], (NUM_LAYERS, MODEL_DIM, MLP_DIM), jnp.float32) * MODEL_DIM ** -0.5
    w_down = jax.random.normal(shared_keys[8], (NUM_LAYERS, MLP_DIM, MODEL_DIM), jnp.float32) * (1.5 * MLP_DIM ** -0.5)
    return {
        "step_emb": step_emb.astype(jnp.bfloat16),
        "v_cache": v_cache.astype(jnp.bfloat16),
        "z_cache": z_cache.astype(jnp.bfloat16),
        "short_state": short_state.astype(jnp.bfloat16),
        "w_in": w_in.astype(jnp.bfloat16),
        "b_in": b_in,
        "short_taps": short_taps,
        "long_filt": long_filt,
        "skip_gain": skip_gain,
        "w_out": w_out.astype(jnp.bfloat16),
        "b_out": b_out,
        "w_up": w_up.astype(jnp.bfloat16),
        "w_down": w_down.astype(jnp.bfloat16),
    }


def layer_norm(rows_in):
    mean_val = jnp.mean(rows_in, axis=-1, keepdims=True)
    centered = rows_in - mean_val
    var_val = jnp.mean(centered * centered, axis=-1, keepdims=True)
    return centered * lax.rsqrt(var_val + 1e-5)


def long_conv(cache_rows, filt_rows, pos_now):
    lag_pos = pos_now - jnp.arange(CACHE_LEN)
    taps_now = jnp.take(filt_rows, jnp.maximum(lag_pos, 0), axis=0)
    taps_now = jnp.where((lag_pos >= 0)[:, None], taps_now, 0.0)
    return jnp.sum(cache_rows.astype(jnp.float32) * taps_now[None], axis=1)


def reference(step_emb, v_cache, z_cache, short_state, w_in, b_in, short_taps, long_filt, skip_gain, w_out, b_out, w_up, w_down):
    def one_step(carry, step_in):
        v_list, z_list, state_list = carry
        emb_row, step_idx = step_in
        pos_now = START_POS + step_idx
        hidden = emb_row.astype(jnp.float32)
        new_v = []
        new_z = []
        new_state = []
        for layer_idx in range(NUM_LAYERS):
            normed = layer_norm(hidden).astype(jnp.bfloat16)
            w_flat = w_in[layer_idx].reshape(MODEL_DIM, 3 * MODEL_DIM)
            proj_row = jnp.dot(normed, w_flat, preferred_element_type=jnp.float32).reshape(-1, 3, MODEL_DIM)
            proj_row = (proj_row + b_in[layer_idx]).astype(jnp.bfloat16)
            prev_state = state_list[layer_idx]
            tap_rows = short_taps[layer_idx]
            mixed_rows = (tap_rows[0] * proj_row.astype(jnp.float32)
                          + tap_rows[1] * prev_state[:, 1].astype(jnp.float32)
                          + tap_rows[2] * prev_state[:, 0].astype(jnp.float32))
            new_state.append(jnp.stack([prev_state[:, 1], proj_row], axis=1))
            value_row = mixed_rows[:, 2].astype(jnp.bfloat16)
            v_layer = lax.dynamic_update_slice(v_list[layer_idx], value_row[:, None, :], (0, pos_now, 0))
            long_one = long_conv(v_layer, long_filt[layer_idx, 0], pos_now) + skip_gain[layer_idx, 0] * value_row.astype(jnp.float32)
            z_row = (mixed_rows[:, 0] * long_one).astype(jnp.bfloat16)
            z_layer = lax.dynamic_update_slice(z_list[layer_idx], z_row[:, None, :], (0, pos_now, 0))
            long_two = long_conv(z_layer, long_filt[layer_idx, 1], pos_now) + skip_gain[layer_idx, 1] * z_row.astype(jnp.float32)
            y_row = (mixed_rows[:, 1] * long_two).astype(jnp.bfloat16)
            hidden = hidden + jnp.dot(y_row, w_out[layer_idx], preferred_element_type=jnp.float32) + b_out[layer_idx]
            inner_act = jax.nn.gelu(jnp.dot(layer_norm(hidden).astype(jnp.bfloat16), w_up[layer_idx], preferred_element_type=jnp.float32)).astype(jnp.bfloat16)
            hidden = hidden + jnp.dot(inner_act, w_down[layer_idx], preferred_element_type=jnp.float32)
            new_v.append(v_layer)
            new_z.append(z_layer)
        return (tuple(new_v), tuple(new_z), tuple(new_state)), hidden

    init_carry = (
        tuple(v_cache[layer_idx] for layer_idx in range(NUM_LAYERS)),
        tuple(z_cache[layer_idx] for layer_idx in range(NUM_LAYERS)),
        tuple(short_state[layer_idx] for layer_idx in range(NUM_LAYERS)),
    )
    final_carry, hiddens = lax.scan(one_step, init_carry, (step_emb, jnp.arange(NUM_STEPS)))
    v_out, z_out, state_out = final_carry
    return (hiddens, jnp.stack(v_out), jnp.stack(z_out), jnp.stack(state_out))
```

```python
import functools

import jax
import jax.numpy as jnp
from jax import lax
from jax.experimental import pallas as pl
from jax.experimental.pallas import tpu as pltpu
from jax.sharding import PartitionSpec as P

F32 = jnp.float32
BF16 = jnp.bfloat16
NUM_STEPS = 4
NUM_LAYERS = 2
SEQ = 32
BLK = 8
DIM = 1024
CH = 512
UP = 2048
SHARD = 256
NCH = 2
CW = DIM // NCH
MESH = pl.DeviceIdType.MESH


def reduce_rows(accs):
    sub = lax.broadcasted_iota(jnp.int32, (8, 128), 0)
    low4 = sub < 4
    low2 = (sub % 4) < 2
    low1 = (sub % 2) < 1
    lev = [jnp.where(low4, accs[i], accs[i + 4]) + pltpu.roll(jnp.where(low4, accs[i + 4], accs[i]), 4, 0) for i in range(4)]
    lev = [jnp.where(low2, lev[i] + pltpu.roll(lev[i], 6, 0), lev[i + 2] + pltpu.roll(lev[i + 2], 2, 0)) for i in range(2)]
    return jnp.where(low1, lev[0] + pltpu.roll(lev[0], 7, 0), lev[1] + pltpu.roll(lev[1], 1, 0))


def conv_kernel(shard_ref, v_ref, z_ref, filt_ref, tail_ref, v_out, z_out, part_ref, win, sems):
    layer = pl.program_id(0)
    blk = pl.program_id(1)
    copies = []
    for idx, (src, dst) in enumerate(((v_ref, v_out), (z_ref, z_out))):
        copy = pltpu.make_async_copy(src.at[0], dst.at[layer, pl.ds(blk * BLK, BLK)], sems.at[idx])
        copy.start()
        copies.append(copy)

    @pl.when(blk == 0)
    def _():
        flip = 7 - lax.broadcasted_iota(jnp.int32, (8, CH), 0)
        for f in range(2):
            for j in range(NUM_STEPS):
                for m in range(SHARD // 8):
                    lo = SHARD + j - 8 * m - 7
                    if m == 0:
                        rows = jnp.concatenate([filt_ref[f, lo:SHARD, :], tail_ref[f, 0:j + 1, :]], axis=0)
                    else:
                        rows = filt_ref[f, lo:lo + 8, :]
                    win[f, j, 8 * m:8 * m + 8, :] = jnp.take_along_axis(rows, flip, axis=0)

    for f, src in enumerate((v_ref, z_ref)):
        for ct in range(CH // 128):
            lanes = slice(128 * ct, 128 * ct + 128)

            def body(pt, accs, f=f, src=src, lanes=lanes):
                base = pl.multiple_of(pt * 16, 16)
                w = [[win[f, j, pl.ds(base + 8 * h, 8), lanes] for h in range(2)] for j in range(NUM_STEPS)]
                out = []
                for b in range(BLK):
                    x = src[0, b, pl.ds(base, 16), lanes].astype(F32)
                    for j in range(NUM_STEPS):
                        out.append(accs[b * NUM_STEPS + j] + x[:8] * w[j][0] + x[8:] * w[j][1])
                return tuple(out)

            zero = jnp.zeros((8, 128), F32)
            accs = lax.fori_loop(0, SHARD // 16, body, (zero,) * (BLK * NUM_STEPS))
            for j in range(NUM_STEPS):
                part_ref[f, j, :, lanes] = reduce_rows([accs[b * NUM_STEPS + j] for b in range(BLK)])
    for copy in copies:
        copy.wait()


def conv_call(shard, v_cache, z_cache, long_filt):
    sq = pl.Squeezed()
    cache_spec = pl.BlockSpec((1, BLK, SHARD, CH), lambda l, b, s: (l, b, 0, 0))
    return pl.pallas_call(
        conv_kernel,
        out_shape=(
            jax.ShapeDtypeStruct(v_cache.shape, BF16),
            jax.ShapeDtypeStruct(z_cache.shape, BF16),
            jax.ShapeDtypeStruct((SEQ // BLK, NUM_LAYERS, 2, NUM_STEPS, BLK, CH), F32),
        ),
        grid_spec=pltpu.PrefetchScalarGridSpec(
            num_scalar_prefetch=1,
            grid=(NUM_LAYERS, SEQ // BLK),
            in_specs=[
                cache_spec,
                cache_spec,
                pl.BlockSpec((sq, 2, SHARD, CH), lambda l, b, s: (l, 0, jnp.maximum(2 - s[0], 0), 0)),
                pl.BlockSpec((sq, 2, 8, CH), lambda l, b, s: (l, 0, (jnp.maximum(2 - s[0], 0) + 1) * (SHARD // 8), 0)),
            ],
            out_specs=[
                pl.BlockSpec(memory_space=pl.ANY),
                pl.BlockSpec(memory_space=pl.ANY),
                pl.BlockSpec((sq, sq, 2, NUM_STEPS, BLK, CH), lambda l, b, s: (b, l, 0, 0, 0, 0)),
            ],
            scratch_shapes=[
                pltpu.VMEM((2, NUM_STEPS, SHARD, CH), F32),
                pltpu.SemaphoreType.DMA((2,)),
            ],
        ),
        compiler_params=pltpu.CompilerParams(dimension_semantics=("arbitrary", "arbitrary"), vmem_limit_bytes=60 << 20),
        name="conv_stream",
    )(shard, v_cache, z_cache, long_filt, long_filt)


def norm_rows(rows_in):
    mean_val = jnp.mean(rows_in, axis=-1, keepdims=True)
    centered = rows_in - mean_val
    var_val = jnp.mean(centered * centered, axis=-1, keepdims=True)
    return centered * lax.rsqrt(var_val + 1e-5)


def round_bf16(x):
    return x.astype(BF16).astype(F32)


def layer_kernel(part_ref, emb_ref, state_ref, b_in_ref, taps_ref, lag_ref, gain_ref, b_out_ref,
                 w_in_hbm, w_out_hbm, w_up_hbm, w_down_hbm,
                 hid_ref, st_ref, rows_ref,
                 w_in, w_out, w_up, w_down, emb32, p_all, rs_buf, x_send, x_recv, hid_buf, st_buf, row_buf,
                 w_sem, rs_send, rs_recv, x_ssem, x_rsem, st_ssem, st_rsem, row_ssem, row_rsem, g_ssem, g_rsem):
    k = lax.axis_index("sp")
    t = lax.axis_index("tp")
    others = [lax.rem(k + d, 4) for d in range(1, 4)]
    mate = k + 1 - 2 * lax.rem(k, 2)
    across = lax.rem(k + 2, 4)
    own = pl.ds(pl.multiple_of(k * BLK, BLK), BLK)

    w_copies = []
    for layer in range(NUM_LAYERS):
        for idx, (src, dst) in enumerate(((w_in_hbm, w_in), (w_out_hbm, w_out), (w_up_hbm, w_up), (w_down_hbm, w_down))):
            copy = pltpu.make_async_copy(src.at[layer], dst.at[layer], w_sem.at[layer, idx])
            copy.start()
            w_copies.append(copy)

    barrier = pltpu.get_barrier_semaphore()
    for dev in others:
        pl.semaphore_signal(barrier, inc=1, device_id={"sp": dev}, device_id_type=MESH)
    pl.semaphore_signal(barrier, inc=1, device_id={"tp": 1 - t}, device_id_type=MESH)
    pl.semaphore_wait(barrier, 4)

    def rs_copy(layer, f, d):
        dev = others[d]
        return pltpu.make_async_remote_copy(
            src_ref=part_ref.at[dev, layer, f], dst_ref=rs_buf.at[jnp.minimum(k, 2), layer, f],
            send_sem=rs_send.at[layer, f, d], recv_sem=rs_recv.at[layer, f, d],
            device_id={"sp": dev}, device_id_type=MESH)

    @pl.when(k < 3)
    def _():
        for layer in range(NUM_LAYERS):
            for f in range(2):
                for d in range(3):
                    rs_copy(layer, f, d).start()
        rs_buf[jnp.minimum(k, 2)] = part_ref[k]

    def cached_sum(layer, f):
        for d in range(3):
            @pl.when(lax.rem(k + 3 - d, 4) < 3)
            def _():
                rs_copy(layer, f, d).wait_recv()
        return (rs_buf[0, layer, f] + rs_buf[1, layer, f]) + rs_buf[2, layer, f]

    def tap_mix(layer, g, cur, prev1, prev2):
        return (taps_ref[layer, 0, g:g + 1] * cur + taps_ref[layer, 1, g:g + 1] * prev1
                + taps_ref[layer, 2, g:g + 1] * prev2)

    def x_copy(n, c):
        return pltpu.make_async_remote_copy(
            src_ref=x_send.at[n, c], dst_ref=x_recv.at[n, c], send_sem=x_ssem.at[n, c], recv_sem=x_rsem.at[n, c],
            device_id={"tp": 1 - t}, device_id_type=MESH)

    def row_copy(n, which, layer):
        piece = row_buf.at[which, layer, :, own]
        return pltpu.make_async_remote_copy(
            src_ref=piece, dst_ref=piece, send_sem=row_ssem.at[n], recv_sem=row_rsem.at[n, k],
            device_id={"sp": 3}, device_id_type=MESH)

    def send_rows(n, which, layer):
        @pl.when(k < 3)
        def _():
            row_copy(n, which, layer).start()

    def long_conv(layer, f, cached, vals):
        outs = []
        for j in range(NUM_STEPS):
            acc = cached[j]
            for i in range(j + 1):
                acc = acc + lag_ref[layer, f, j - i:j - i + 1] * vals[i]
            outs.append(acc + gain_ref[layer, f:f + 1] * vals[j])
        return outs

    def gates(layer, x1, x2, vals):
        a = long_conv(layer, 0, cached_sum(layer, 0), vals)
        z = [round_bf16(x1[j] * a[j]) for j in range(NUM_STEPS)]
        for j in range(NUM_STEPS):
            row_buf[1, layer, j, own] = z[j]
        send_rows(layer * 2, 1, layer)
        b = long_conv(layer, 1, cached_sum(layer, 1), z)
        return jnp.concatenate([x2[j] * b[j] for j in range(NUM_STEPS)], axis=0).astype(BF16)

    def matmul_exchange(n, lhs, w_ref):
        for c in range(NCH):
            x_send[n, c] = jnp.dot(lhs, w_ref[:, c * CW:(c + 1) * CW], preferred_element_type=F32)
            x_copy(n, c).start()

    def add_exchange(n, c, base):
        x_copy(n, c).wait_recv()
        return base + (x_send[n, c] + x_recv[n, c])

    def mlp(layer, mixed):
        act = norm_rows(mixed).astype(BF16)
        w_copies[layer * 4 + 2].wait()
        inner = jax.nn.gelu(jnp.dot(act, w_up[layer], preferred_element_type=F32)).astype(BF16)
        w_copies[layer * 4 + 3].wait()
        matmul_exchange(layer * 2 + 1, inner, w_down.at[layer])

    def mixed_rows(layer, rows_in):
        n = layer * 2
        return jnp.concatenate(
            [add_exchange(n, c, rows_in[:, c * CW:(c + 1) * CW]) + b_out_ref[layer:layer + 1, c * CW:(c + 1) * CW]
             for c in range(NCH)], axis=1)

    emb32[...] = emb_ref[...].astype(F32)
    normed = norm_rows(emb32[...].reshape(NUM_STEPS * SEQ, DIM)).astype(BF16)
    w_copies[0].wait()
    for g in range(3):
        proj = jnp.dot(normed, w_in[0, g], preferred_element_type=F32) + b_in_ref[0, g:g + 1]
        p_all[g] = round_bf16(proj).reshape(NUM_STEPS, SEQ, CH)

    def p0(g, j, rows):
        return p_all[g, j, rows] if j >= 0 else state_ref[0, j + 2, g, rows]

    everyone = slice(0, SEQ)
    for g in range(3):
        for s in range(2):
            st_ref[0, s, g] = p_all[g, 2 + s]
    for j in range(NUM_STEPS):
        row_buf[0, 0, j] = round_bf16(tap_mix(0, 2, *[p0(2, j - i, everyone) for i in range(3)]))
    x1 = [tap_mix(0, 0, *[p0(0, j - i, own) for i in range(3)]) for j in range(NUM_STEPS)]
    x2 = [tap_mix(0, 1, *[p0(1, j - i, own) for i in range(3)]) for j in range(NUM_STEPS)]
    y = gates(0, x1, x2, [row_buf[0, 0, j, own] for j in range(NUM_STEPS)])
    w_copies[1].wait()
    matmul_exchange(0, y, w_out.at[0])
    mixed = mixed_rows(0, jnp.concatenate([emb32[j, own] for j in range(NUM_STEPS)], axis=0))
    mlp(0, mixed)
    hidden = jnp.concatenate([add_exchange(1, c, mixed[:, c * CW:(c + 1) * CW]) for c in range(NCH)], axis=1)

    normed = norm_rows(hidden).astype(BF16)
    w_copies[4].wait()
    p1 = []
    for g in range(3):
        proj = round_bf16(jnp.dot(normed, w_in[1, g], preferred_element_type=F32) + b_in_ref[1, g:g + 1])
        p1.append([state_ref[1, 0, g, own], state_ref[1, 1, g, own]] + [proj[BLK * j:BLK * j + BLK] for j in range(NUM_STEPS)])
        for s in range(2):
            st_buf[s, g, own] = proj[BLK * (2 + s):BLK * (3 + s)]

    def st_copy(d):
        piece = st_buf.at[:, :, own]
        return pltpu.make_async_remote_copy(
            src_ref=piece, dst_ref=piece, send_sem=st_ssem.at[d], recv_sem=st_rsem.at[d],
            device_id={"sp": others[d]}, device_id_type=MESH)

    for d in range(3):
        st_copy(d).start()
    mix1 = [[tap_mix(1, g, p1[g][j + 2], p1[g][j + 1], p1[g][j]) for j in range(NUM_STEPS)] for g in range(3)]
    vals = [round_bf16(mix1[2][j]) for j in range(NUM_STEPS)]
    for j in range(NUM_STEPS):
        row_buf[0, 1, j, own] = vals[j]
    send_rows(1, 0, 1)
    y = gates(1, mix1[0], mix1[1], vals)
    w_copies[5].wait()
    matmul_exchange(2, y, w_out.at[1])
    mixed = mixed_rows(1, hidden)
    mlp(1, mixed)

    def g_copy(c, hop):
        block = k if hop < 2 else across
        dev = across if hop == 1 else mate
        piece = hid_buf.at[c, :, pl.ds(pl.multiple_of(block * BLK, BLK), BLK)]
        return pltpu.make_async_remote_copy(
            src_ref=piece, dst_ref=piece, send_sem=g_ssem.at[c, hop], recv_sem=g_rsem.at[c, hop],
            device_id={"sp": dev}, device_id_type=MESH)

    for c in range(NCH):
        done = add_exchange(3, c, mixed[:, c * CW:(c + 1) * CW])
        for j in range(NUM_STEPS):
            hid_buf[c, j, own] = done[BLK * j:BLK * j + BLK]
        g_copy(c, 1).start()
        g_copy(c, 0).start()
    for c in range(NCH):
        g_copy(c, 1).wait_recv()
        g_copy(c, 2).start()

    for d in range(3):
        st_copy(d).wait_recv()
    st_ref[1] = st_buf[...]

    @pl.when(k == 3)
    def _():
        for n, which, layer in ((0, 1, 0), (1, 0, 1), (2, 1, 1)):
            for src in range(3):
                piece = row_buf.at[which, layer, :, src * BLK:src * BLK + BLK]
                pltpu.make_async_remote_copy(
                    src_ref=piece, dst_ref=piece, send_sem=row_ssem.at[n], recv_sem=row_rsem.at[n, src],
                    device_id={"sp": 3}, device_id_type=MESH).wait_recv()
        rows_ref[...] = row_buf[...]

    for c in range(NCH):
        g_copy(c, 0).wait_recv()
        g_copy(c, 2).wait_recv()
        for j in range(NUM_STEPS):
            hid_ref[j, :, c * CW:(c + 1) * CW] = hid_buf[c, j]

    for c in range(NCH):
        for n in range(4):
            x_copy(n, c).wait_send()
        for hop in range(3):
            g_copy(c, hop).wait_send()
    for d in range(3):
        st_copy(d).wait_send()

    @pl.when(k < 3)
    def _():
        for n, which, layer in ((0, 1, 0), (1, 0, 1), (2, 1, 1)):
            row_copy(n, which, layer).wait_send()
        for layer in range(NUM_LAYERS):
            for f in range(2):
                for d in range(3):
                    rs_copy(layer, f, d).wait_send()


def layer_call(part, step_emb, state, b_in, taps, lags, gain, b_out, w_in, w_out, w_up, w_down):
    vm = pl.BlockSpec(memory_space=pltpu.VMEM)
    hbm = pl.BlockSpec(memory_space=pl.ANY)
    dma = pltpu.SemaphoreType.DMA
    return pl.pallas_call(
        layer_kernel,
        out_shape=(
            jax.ShapeDtypeStruct((NUM_STEPS, SEQ, DIM), F32),
            jax.ShapeDtypeStruct((NUM_LAYERS, 2, 3, SEQ, CH), F32),
            jax.ShapeDtypeStruct((2, NUM_LAYERS, NUM_STEPS, SEQ, CH), F32),
        ),
        in_specs=[vm] * 8 + [hbm] * 4,
        out_specs=[vm] * 3,
        scratch_shapes=[
            pltpu.VMEM(w_in.shape, BF16),
            pltpu.VMEM(w_out.shape, BF16),
            pltpu.VMEM(w_up.shape, BF16),
            pltpu.VMEM(w_down.shape, BF16),
            pltpu.VMEM((NUM_STEPS, SEQ, DIM), F32),
            pltpu.VMEM((3, NUM_STEPS, SEQ, CH), F32),
            pltpu.VMEM((3, NUM_LAYERS, 2, NUM_STEPS, BLK, CH), F32),
            pltpu.VMEM((4, NCH, NUM_STEPS * BLK, CW), F32),
            pltpu.VMEM((4, NCH, NUM_STEPS * BLK, CW), F32),
            pltpu.VMEM((NCH, NUM_STEPS, SEQ, CW), F32),
            pltpu.VMEM((2, 3, SEQ, CH), F32),
            pltpu.VMEM((2, NUM_LAYERS, NUM_STEPS, SEQ, CH), F32),
            dma((NUM_LAYERS, 4)),
            dma((NUM_LAYERS, 2, 3)),
            dma((NUM_LAYERS, 2, 3)),
            dma((4, NCH)),
            dma((4, NCH)),
            dma((3,)),
            dma((3,)),
            dma((3,)),
            dma((3, 4)),
            dma((NCH, 3)),
            dma((NCH, 3)),
        ],
        compiler_params=pltpu.CompilerParams(collective_id=0, has_side_effects=True, vmem_limit_bytes=56 << 20),
        name="layers",
    )(part, step_emb, state, b_in, taps, lags, gain, b_out, w_in, w_out, w_up, w_down)


def put_kernel(rows_ref, v_in, z_in, v_out, z_out, wide, tile, sems):
    @pl.when(lax.axis_index("sp") == 3)
    def _():
        wide[...] = jnp.zeros_like(wide)
        copies = []
        for which, dst in enumerate((v_out, z_out)):
            for layer in range(NUM_LAYERS):
                for j in range(NUM_STEPS):
                    wide[which, layer, :, j, :] = rows_ref[which, layer, j]
                tile[which, layer] = wide[which, layer].astype(BF16)
                copy = pltpu.make_async_copy(tile.at[which, layer], dst.at[layer, :, 0:8, :], sems.at[which, layer])
                copy.start()
                copies.append(copy)
        for copy in copies:
            copy.wait()


def put_call(rows, v_new, z_new):
    hbm = pl.BlockSpec(memory_space=pl.ANY)
    return pl.pallas_call(
        put_kernel,
        out_shape=(jax.ShapeDtypeStruct(v_new.shape, BF16), jax.ShapeDtypeStruct(z_new.shape, BF16)),
        in_specs=[pl.BlockSpec(memory_space=pltpu.VMEM), hbm, hbm],
        out_specs=[hbm, hbm],
        scratch_shapes=[
            pltpu.VMEM((2, NUM_LAYERS, SEQ, 8, CH), F32),
            pltpu.VMEM((2, NUM_LAYERS, SEQ, 8, CH), BF16),
            pltpu.SemaphoreType.DMA((2, NUM_LAYERS)),
        ],
        input_output_aliases={1: 0, 2: 1},
        compiler_params=pltpu.CompilerParams(vmem_limit_bytes=16 << 20),
        name="put_rows",
    )(rows, v_new, z_new)


def solution(mesh):
    def device_fn(step_emb, v_cache, z_cache, short_state, w_in, b_in, short_taps, long_filt, skip_gain, w_out, b_out, w_up, w_down):
        shard = lax.axis_index("sp").astype(jnp.int32).reshape(1)
        v_new, z_new, part = conv_call(shard, v_cache, z_cache, long_filt)
        state = jnp.transpose(short_state, (0, 2, 3, 1, 4)).astype(F32)
        hidden, states, rows = layer_call(
            part, step_emb, state, b_in, short_taps, long_filt[:, :, :8], skip_gain, b_out,
            jnp.transpose(w_in, (0, 2, 1, 3)), w_out, w_up, w_down)
        v_new, z_new = put_call(rows, v_new, z_new)
        return hidden, v_new, z_new, jnp.transpose(states, (0, 3, 1, 2, 4)).astype(BF16)

    specs_in = (
        P(None, "dp", None),
        P(None, "dp", "sp", "tp"),
        P(None, "dp", "sp", "tp"),
        P(None, "dp", None, None, "tp"),
        P(None, None, None, "tp"),
        P(None, None, "tp"),
        P(None, None, None, "tp"),
        P(None, None, None, "tp"),
        P(None, None, "tp"),
        P(None, "tp", None),
        P(None, None),
        P(None, None, "tp"),
        P(None, "tp", None),
    )
    specs_out = (
        P(None, "dp", None),
        P(None, "dp", "sp", "tp"),
        P(None, "dp", "sp", "tp"),
        P(None, "dp", None, None, "tp"),
    )
    return jax.shard_map(device_fn, mesh=mesh, in_specs=specs_in, out_specs=specs_out, check_vma=False)
```

```python
import functools

import jax
import jax.numpy as jnp
from jax import lax
from jax.experimental import pallas as pl
from jax.experimental.pallas import tpu as pltpu
from jax.sharding import PartitionSpec as P

F32 = jnp.float32
BF16 = jnp.bfloat16
NUM_STEPS = 4
NUM_LAYERS = 2
SEQ = 32
BLK = 8
DIM = 1024
CH = 512
UP = 2048
SHARD = 256
NCH = 2
CW = DIM // NCH
SLOTS = 5
MESH = pl.DeviceIdType.MESH


def pair_rows(lo, hi, shift):
    clear = (lax.broadcasted_iota(jnp.int32, (8, 128), 0) // shift) % 2 == 0
    if shift == 4:
        return jnp.where(clear, lo, hi) + pltpu.roll(jnp.where(clear, hi, lo), 4, 0)
    return jnp.where(clear, lo + pltpu.roll(lo, 8 - shift, 0), hi + pltpu.roll(hi, shift, 0))


def fill_window(win, filt_rows):
    flip = 7 - lax.broadcasted_iota(jnp.int32, (8, 128), 0)
    for ct in range(CH // 128):
        for m in range(SHARD // 8 + 1):
            rows = filt_rows[SHARD - 8 * m:SHARD - 8 * m + 8, 128 * ct:128 * ct + 128]
            win[ct, 8 * m:8 * m + 8] = jnp.take_along_axis(rows, flip, axis=0)


def conv_block(src, win, dst):
    @pl.loop(0, CH // 128)
    def _(ct):
        lanes = pl.ds(pl.multiple_of(ct * 128, 128), 128)
        half = []
        for seqs in ((0, 4, 1, 5), (2, 6, 3, 7)):
            accs = [[None] * NUM_STEPS for _ in seqs]
            for pt in range(SHARD // 16):
                w = [[win[ct, 16 * pt + 8 * h + 7 - j:16 * pt + 8 * h + 15 - j] for h in range(2)] for j in range(NUM_STEPS)]
                for i, b in enumerate(seqs):
                    x = src[b, 16 * pt:16 * pt + 16, lanes].astype(F32)
                    for j in range(NUM_STEPS):
                        for h in range(2):
                            term = x[8 * h:8 * h + 8] * w[j][h]
                            accs[i][j] = term if accs[i][j] is None else accs[i][j] + term
            half.append([[pair_rows(accs[0][j], accs[1][j], 4), pair_rows(accs[2][j], accs[3][j], 4)] for j in range(NUM_STEPS)])
        for j in range(NUM_STEPS):
            dst[j, :, lanes] = pair_rows(pair_rows(half[0][j][0], half[1][j][0], 2), pair_rows(half[0][j][1], half[1][j][1], 2), 1)


def stream_kernel(layer, num_in, *refs):
    v_in, z_in, filt = refs[:3]
    v_out, z_out = refs[num_in:num_in + 2]
    parts = refs[num_in + 2:num_in + 6]
    ring, rows, win, in_sem, out_sem, filt_sem = refs[num_in + 6:]
    k = lax.axis_index("sp")
    first = pl.multiple_of(jnp.maximum(2 - k, 0) * SHARD, SHARD)
    units = [(f, d) for f in range(2) for d in range(4)]

    def in_copy(u):
        f, d = units[u]
        seqs = pl.ds(pl.multiple_of(lax.rem(k + d, 4) * BLK, BLK), BLK)
        return pltpu.make_async_copy((v_in, z_in)[f].at[layer, seqs], ring.at[u % SLOTS], in_sem.at[u])

    def out_copy(u):
        f, d = units[u]
        seqs = pl.ds(pl.multiple_of(lax.rem(k + d, 4) * BLK, BLK), BLK)
        return pltpu.make_async_copy(ring.at[u % SLOTS], (v_out, z_out)[f].at[layer, seqs], out_sem.at[u])

    filt_copies = [pltpu.make_async_copy(filt.at[layer, f, pl.ds(first, SHARD + 8)], rows.at[f], filt_sem.at[f]) for f in range(2)]
    filt_copies[0].start()
    in_copy(0).start()
    filt_copies[1].start()
    for u in range(1, SLOTS):
        in_copy(u).start()
    for u, (f, d) in enumerate(units):
        if d == 0:
            filt_copies[f].wait()
            fill_window(win, rows.at[f])
        in_copy(u).wait()
        out_copy(u).start()
        conv_block(ring.at[u % SLOTS], win, parts[d].at[f])
        if u >= 1:
            out_copy(u - 1).wait()
            if u - 1 + SLOTS < len(units):
                in_copy(u - 1 + SLOTS).start()
    out_copy(len(units) - 1).wait()


def stream_call(layer, v_cache, z_cache, long_filt, earlier=()):
    hbm = pl.BlockSpec(memory_space=pl.ANY)
    num_in = 3 + len(earlier)
    part = jax.ShapeDtypeStruct((2, NUM_STEPS, BLK, CH), F32)
    return pl.pallas_call(
        functools.partial(stream_kernel, layer, num_in),
        out_shape=(jax.ShapeDtypeStruct(v_cache.shape, BF16), jax.ShapeDtypeStruct(z_cache.shape, BF16)) + (part,) * 4,
        in_specs=[hbm] * num_in,
        out_specs=[hbm] * 2 + [pl.BlockSpec(memory_space=pltpu.VMEM)] * 4,
        scratch_shapes=[
            pltpu.VMEM((SLOTS, BLK, SHARD, CH), BF16),
            pltpu.VMEM((2, SHARD + 8, CH), F32),
            pltpu.VMEM((CH // 128, SHARD + 8, 128), F32),
            pltpu.SemaphoreType.DMA((8,)),
            pltpu.SemaphoreType.DMA((8,)),
            pltpu.SemaphoreType.DMA((2,)),
        ],
        input_output_aliases={3: 0, 4: 1} if earlier else {},
        cost_estimate=pl.CostEstimate(flops=SEQ * SHARD * CH * 16, bytes_accessed=4 * SEQ * SHARD * CH * 2, transcendentals=0),
        compiler_params=pltpu.CompilerParams(vmem_limit_bytes=30 << 20),
        name=f"stream_{layer}",
    )(v_cache, z_cache, long_filt, *earlier)


def norm_rows(rows_in):
    mean_val = jnp.mean(rows_in, axis=-1, keepdims=True)
    centered = rows_in - mean_val
    var_val = jnp.mean(centered * centered, axis=-1, keepdims=True)
    return centered * lax.rsqrt(var_val + 1e-5)


def round_bf16(x):
    return x.astype(BF16).astype(F32)


def layer_kernel(*refs):
    sums0 = refs[:4]
    parts1 = refs[4:8]
    (emb_ref, b_in_ref, taps_ref, gain_ref, b_out_ref, filt_hbm, state_hbm, w_in_hbm, w_out_hbm, w_up_hbm, w_down_hbm,
     hid_ref, st_ref, rows_ref,
     w_in, w_out, w_up, w_down, emb32, state, lags, rs_buf, x_send, x_recv, hid_buf, st_buf, row_buf,
     w_sem, s_sem, rs_send, rs_recv, x_ssem, x_rsem, st_ssem, st_rsem, row_ssem, row_rsem, g_ssem, g_rsem) = refs[8:]
    k = lax.axis_index("sp")
    t = lax.axis_index("tp")
    others = [lax.rem(k + d, 4) for d in range(1, 4)]
    mate = k + 1 - 2 * lax.rem(k, 2)
    across = lax.rem(k + 2, 4)
    own = pl.ds(pl.multiple_of(k * BLK, BLK), BLK)

    small = [pltpu.make_async_copy(state_hbm.at[:, own], state, s_sem.at[0]),
             pltpu.make_async_copy(filt_hbm.at[:, :, 0:8], lags, s_sem.at[1])]
    for copy in small:
        copy.start()
    w_copies = []
    for layer in range(NUM_LAYERS):
        for idx, (src, dst) in enumerate(((w_in_hbm, w_in), (w_out_hbm, w_out), (w_up_hbm, w_up), (w_down_hbm, w_down))):
            copy = pltpu.make_async_copy(src.at[layer], dst.at[layer], w_sem.at[layer, idx])
            copy.start()
            w_copies.append(copy)

    barrier = pltpu.get_barrier_semaphore()
    for dev in others:
        pl.semaphore_signal(barrier, inc=1, device_id={"sp": dev}, device_id_type=MESH)
    pl.semaphore_signal(barrier, inc=1, device_id={"tp": 1 - t}, device_id_type=MESH)
    pl.semaphore_wait(barrier, 4)

    def rs_copy(f, d):
        return pltpu.make_async_remote_copy(
            src_ref=parts1[d].at[f], dst_ref=rs_buf.at[d - 1, f], send_sem=rs_send.at[f, d - 1], recv_sem=rs_recv.at[f, d - 1],
            device_id={"sp": others[d - 1]}, device_id_type=MESH)

    for f in range(2):
        for d in range(1, 4):
            rs_copy(f, d).start()

    def cached_sum(layer, f):
        if layer == 0:
            return (sums0[0][f] + sums0[1][f]) + (sums0[2][f] + sums0[3][f])
        for d in range(1, 4):
            rs_copy(f, d).wait_recv()
        return (parts1[0][f] + rs_buf[0, f]) + (rs_buf[1, f] + rs_buf[2, f])

    def x_copy(n, c):
        return pltpu.make_async_remote_copy(
            src_ref=x_send.at[n, c], dst_ref=x_recv.at[n, c], send_sem=x_ssem.at[n, c], recv_sem=x_rsem.at[n, c],
            device_id={"tp": 1 - t}, device_id_type=MESH)

    def row_copy(which, layer, src=None):
        piece = row_buf.at[which, layer, own if src is None else pl.ds(src * BLK, BLK)]
        return pltpu.make_async_remote_copy(
            src_ref=piece, dst_ref=piece, send_sem=row_ssem.at[which, layer],
            recv_sem=row_rsem.at[which, layer, k if src is None else src],
            device_id={"sp": 3}, device_id_type=MESH)

    def st_copy(layer, d):
        piece = st_buf.at[layer, own]
        return pltpu.make_async_remote_copy(
            src_ref=piece, dst_ref=piece, send_sem=st_ssem.at[layer, d], recv_sem=st_rsem.at[layer, d],
            device_id={"sp": others[d]}, device_id_type=MESH)

    def keep_rows(which, layer, vals):
        for b in range(BLK):
            for j in range(NUM_STEPS):
                row_buf[which, layer, k * BLK + b, j:j + 1, :] = vals[j][b:b + 1]

        @pl.when(k < 3)
        def _():
            row_copy(which, layer).start()

    def long_conv(layer, f, cached, vals):
        outs = []
        for j in range(NUM_STEPS):
            acc = cached[j]
            for i in range(j + 1):
                acc = acc + lags[layer, f, j - i:j - i + 1] * vals[i]
            outs.append(acc + gain_ref[layer, f:f + 1] * vals[j])
        return outs

    def matmul_exchange(n, lhs, w_ref):
        for c in range(NCH):
            x_send[n, c] = jnp.dot(lhs, w_ref[:, c * CW:(c + 1) * CW], preferred_element_type=F32)
            x_copy(n, c).start()

    def add_exchange(n, c, base):
        x_copy(n, c).wait_recv()
        return base + (x_send[n, c] + x_recv[n, c])

    def finish_states(layer):
        for d in range(3):
            st_copy(layer, d).wait_recv()
        st_ref[layer] = st_buf[layer].astype(BF16)

    def layer_rows(layer, rows_in, filler):
        normed = norm_rows(rows_in).astype(BF16)
        w_copies[layer * 4].wait()
        mixed = []
        steps = []
        for g in range(3):
            proj = jnp.dot(normed, w_in[layer, g], preferred_element_type=F32) + b_in_ref[g, layer:layer + 1]
            proj = round_bf16(proj)
            prev = [jnp.concatenate([state[layer, b, g, s:s + 1].astype(F32) for b in range(BLK)], axis=0) for s in range(2)]
            seq = prev + [proj[BLK * j:BLK * j + BLK] for j in range(NUM_STEPS)]
            steps.append(seq)
            tap = [taps_ref[i, g, layer:layer + 1] for i in range(3)]
            mixed.append([tap[0] * seq[j + 2] + tap[1] * seq[j + 1] + tap[2] * seq[j] for j in range(NUM_STEPS)])
        vals = [round_bf16(x) for x in mixed[2]]
        a = long_conv(layer, 0, cached_sum(layer, 0), vals)
        z = [round_bf16(mixed[0][j] * a[j]) for j in range(NUM_STEPS)]
        b = long_conv(layer, 1, cached_sum(layer, 1), z)
        y = jnp.concatenate([mixed[1][j] * b[j] for j in range(NUM_STEPS)], axis=0).astype(BF16)
        w_copies[layer * 4 + 1].wait()
        matmul_exchange(layer * 2, y, w_out.at[layer])
        keep_rows(0, layer, vals)
        keep_rows(1, layer, z)
        for g in range(3):
            for s in range(2):
                for i in range(BLK):
                    st_buf[layer, k * BLK + i, g, s:s + 1, :] = steps[g][4 + s][i:i + 1]
        for d in range(3):
            st_copy(layer, d).start()
        out = jnp.concatenate(
            [add_exchange(layer * 2, c, rows_in[:, c * CW:(c + 1) * CW]) + b_out_ref[layer:layer + 1, c * CW:(c + 1) * CW]
             for c in range(NCH)], axis=1)
        act = norm_rows(out).astype(BF16)
        w_copies[layer * 4 + 2].wait()
        inner = jax.nn.gelu(jnp.dot(act, w_up[layer], preferred_element_type=F32)).astype(BF16)
        w_copies[layer * 4 + 3].wait()
        matmul_exchange(layer * 2 + 1, inner, w_down.at[layer])
        filler()
        return out

    emb32[...] = emb_ref[...].astype(F32)
    for copy in small:
        copy.wait()
    out = layer_rows(0, jnp.concatenate([emb32[j, own] for j in range(NUM_STEPS)], axis=0), lambda: finish_states(0))
    hidden = jnp.concatenate([add_exchange(1, c, out[:, c * CW:(c + 1) * CW]) for c in range(NCH)], axis=1)
    out = layer_rows(1, hidden, lambda: finish_states(1))

    def g_copy(c, hop):
        block = k if hop < 2 else across
        dev = across if hop == 1 else mate
        piece = hid_buf.at[c, :, pl.ds(pl.multiple_of(block * BLK, BLK), BLK)]
        return pltpu.make_async_remote_copy(
            src_ref=piece, dst_ref=piece, send_sem=g_ssem.at[c, hop], recv_sem=g_rsem.at[c, hop],
            device_id={"sp": dev}, device_id_type=MESH)

    for c in range(NCH):
        done = add_exchange(3, c, out[:, c * CW:(c + 1) * CW])
        for j in range(NUM_STEPS):
            hid_buf[c, j, own] = done[BLK * j:BLK * j + BLK]
        g_copy(c, 1).start()
        g_copy(c, 0).start()

    @pl.when(k == 3)
    def _():
        for layer in range(NUM_LAYERS):
            for which in range(2):
                for src in range(3):
                    row_copy(which, layer, src).wait_recv()
        rows_ref[...] = row_buf[...]

    for c in range(NCH):
        g_copy(c, 1).wait_recv()
        g_copy(c, 2).start()
    for c in range(NCH):
        g_copy(c, 0).wait_recv()
        g_copy(c, 2).wait_recv()
        for j in range(NUM_STEPS):
            hid_ref[j, :, c * CW:(c + 1) * CW] = hid_buf[c, j]

    for c in range(NCH):
        for n in range(4):
            x_copy(n, c).wait_send()
        for hop in range(3):
            g_copy(c, hop).wait_send()
    for f in range(2):
        for d in range(1, 4):
            rs_copy(f, d).wait_send()
    for layer in range(NUM_LAYERS):
        for d in range(3):
            st_copy(layer, d).wait_send()

    @pl.when(k < 3)
    def _():
        for layer in range(NUM_LAYERS):
            for which in range(2):
                row_copy(which, layer).wait_send()


def layer_call(sums0, parts1, step_emb, b_in, taps, gain, b_out, long_filt, state, w_in, w_out, w_up, w_down):
    vm = pl.BlockSpec(memory_space=pltpu.VMEM)
    hbm = pl.BlockSpec(memory_space=pl.ANY)
    dma = pltpu.SemaphoreType.DMA
    return pl.pallas_call(
        layer_kernel,
        out_shape=(
            jax.ShapeDtypeStruct((NUM_STEPS, SEQ, DIM), F32),
            jax.ShapeDtypeStruct((NUM_LAYERS, SEQ, 3, 2, CH), BF16),
            jax.ShapeDtypeStruct((2, NUM_LAYERS, SEQ, NUM_STEPS, CH), F32),
        ),
        in_specs=[vm] * 13 + [hbm] * 6,
        out_specs=[vm] * 3,
        scratch_shapes=[
            pltpu.VMEM(w_in.shape, BF16),
            pltpu.VMEM(w_out.shape, BF16),
            pltpu.VMEM(w_up.shape, BF16),
            pltpu.VMEM(w_down.shape, BF16),
            pltpu.VMEM((NUM_STEPS, SEQ, DIM), F32),
            pltpu.VMEM((NUM_LAYERS, BLK, 3, 2, CH), BF16),
            pltpu.VMEM((NUM_LAYERS, 2, 8, CH), F32),
            pltpu.VMEM((3, 2, NUM_STEPS, BLK, CH), F32),
            pltpu.VMEM((4, NCH, NUM_STEPS * BLK, CW), F32),
            pltpu.VMEM((4, NCH, NUM_STEPS * BLK, CW), F32),
            pltpu.VMEM((NCH, NUM_STEPS, SEQ, CW), F32),
            pltpu.VMEM((NUM_LAYERS, SEQ, 3, 2, CH), F32),
            pltpu.VMEM((2, NUM_LAYERS, SEQ, NUM_STEPS, CH), F32),
            dma((NUM_LAYERS, 4)),
            dma((2,)),
            dma((2, 3)),
            dma((2, 3)),
            dma((4, NCH)),
            dma((4, NCH)),
            dma((NUM_LAYERS, 3)),
            dma((NUM_LAYERS, 3)),
            dma((2, NUM_LAYERS)),
            dma((2, NUM_LAYERS, 4)),
            dma((NCH, 3)),
            dma((NCH, 3)),
        ],
        compiler_params=pltpu.CompilerParams(collective_id=0, has_side_effects=True, vmem_limit_bytes=44 << 20),
        name="layers",
    )(*sums0, *parts1, step_emb, b_in, taps, gain, b_out, long_filt, state, w_in, w_out, w_up, w_down)


def put_kernel(hid_in, st_in, rows_ref, v_in, z_in, hid_out, st_out, v_out, z_out, wide, tile, sems, o_sem):
    copies = [pltpu.make_async_copy(hid_in, hid_out, o_sem.at[0]), pltpu.make_async_copy(st_in, st_out, o_sem.at[1])]
    for copy in copies:
        copy.start()

    @pl.when(lax.axis_index("sp") == 3)
    def _():
        row_copies = []
        for which, dst in enumerate((v_out, z_out)):
            for layer in range(NUM_LAYERS):
                wide[:, 4:8, :] = jnp.zeros((SEQ, 4, CH), F32)
                wide[:, 0:4, :] = rows_ref[which, layer]
                tile[which, layer] = wide[...].astype(BF16)
                copy = pltpu.make_async_copy(tile.at[which, layer], dst.at[layer, :, 0:8, :], sems.at[which, layer])
                copy.start()
                row_copies.append(copy)
        for copy in row_copies:
            copy.wait()

    for copy in copies:
        copy.wait()


def put_call(hidden, states, rows, v_new, z_new):
    hbm = pl.BlockSpec(memory_space=pl.ANY)
    vm = pl.BlockSpec(memory_space=pltpu.VMEM)
    return pl.pallas_call(
        put_kernel,
        out_shape=(jax.ShapeDtypeStruct(hidden.shape, F32), jax.ShapeDtypeStruct(states.shape, BF16),
                   jax.ShapeDtypeStruct(v_new.shape, BF16), jax.ShapeDtypeStruct(z_new.shape, BF16)),
        in_specs=[vm] * 3 + [hbm] * 2,
        out_specs=[hbm] * 4,
        scratch_shapes=[
            pltpu.VMEM((SEQ, 8, CH), F32),
            pltpu.VMEM((2, NUM_LAYERS, SEQ, 8, CH), BF16),
            pltpu.SemaphoreType.DMA((2, NUM_LAYERS)),
            pltpu.SemaphoreType.DMA((2,)),
        ],
        input_output_aliases={3: 2, 4: 3},
        compiler_params=pltpu.CompilerParams(vmem_limit_bytes=16 << 20),
        name="put_rows",
    )(hidden, states, rows, v_new, z_new)


def solution(mesh):
    def device_fn(step_emb, v_cache, z_cache, short_state, w_in, b_in, short_taps, long_filt, skip_gain, w_out, b_out, w_up, w_down):
        v_new, z_new, *parts0 = stream_call(0, v_cache, z_cache, long_filt)
        sums0 = [parts0[0]] + [lax.ppermute(parts0[d], "sp", [(i, (i + d) % 4) for i in range(4)]) for d in range(1, 4)]
        v_new, z_new, *parts1 = stream_call(1, v_cache, z_cache, long_filt, (v_new, z_new))
        hidden, states, rows = layer_call(
            sums0, parts1, step_emb, jnp.transpose(b_in, (1, 0, 2)), jnp.transpose(short_taps, (1, 2, 0, 3)),
            skip_gain, b_out, long_filt, jnp.transpose(short_state, (0, 1, 3, 2, 4)),
            jnp.transpose(w_in, (0, 2, 1, 3)), w_out, w_up, w_down)
        hidden, states, v_new, z_new = put_call(hidden, states, rows, v_new, z_new)
        return hidden, v_new, z_new, jnp.transpose(states, (0, 1, 3, 2, 4))

    specs_in = (
        P(None, "dp", None),
        P(None, "dp", "sp", "tp"),
        P(None, "dp", "sp", "tp"),
        P(None, "dp", None, None, "tp"),
        P(None, None, None, "tp"),
        P(None, None, "tp"),
        P(None, None, None, "tp"),
        P(None, None, None, "tp"),
        P(None, None, "tp"),
        P(None, "tp", None),
        P(None, None),
        P(None, None, "tp"),
        P(None, "tp", None),
    )
    specs_out = (
        P(None, "dp", None),
        P(None, "dp", "sp", "tp"),
        P(None, "dp", "sp", "tp"),
        P(None, "dp", None, None, "tp"),
    )
    return jax.shard_map(device_fn, mesh=mesh, in_specs=specs_in, out_specs=specs_out, check_vma=False)
```

```python
import functools

import jax
import jax.numpy as jnp
from jax import lax
from jax.experimental import pallas as pl
from jax.experimental.pallas import tpu as pltpu
from jax.sharding import PartitionSpec as P

F32 = jnp.float32
BF16 = jnp.bfloat16
NUM_STEPS = 4
NUM_LAYERS = 2
SEQ = 32
BLK = 8
DIM = 1024
CH = 512
UP = 2048
SHARD = 256
NCH = 2
CW = DIM // NCH
SLOTS = 5
MESH = pl.DeviceIdType.MESH


def pair_rows(lo, hi, shift):
    clear = (lax.broadcasted_iota(jnp.int32, (8, 128), 0) // shift) % 2 == 0
    if shift == 4:
        return jnp.where(clear, lo, hi) + pltpu.roll(jnp.where(clear, hi, lo), 4, 0)
    return jnp.where(clear, lo + pltpu.roll(lo, 8 - shift, 0), hi + pltpu.roll(hi, shift, 0))


def fill_window(win, filt_rows):
    flip = 7 - lax.broadcasted_iota(jnp.int32, (8, 128), 0)
    for ct in range(CH // 128):
        for m in range(SHARD // 8 + 1):
            rows = filt_rows[SHARD - 8 * m:SHARD - 8 * m + 8, 128 * ct:128 * ct + 128]
            win[ct, 8 * m:8 * m + 8] = jnp.take_along_axis(rows, flip, axis=0)


def conv_block(src, win, dst):
    @pl.loop(0, CH // 128)
    def _(ct):
        lanes = pl.ds(pl.multiple_of(ct * 128, 128), 128)
        half = []
        for seqs in ((0, 4, 1, 5), (2, 6, 3, 7)):
            accs = [[None] * NUM_STEPS for _ in seqs]
            for pt in range(SHARD // 16):
                w = [[win[ct, 16 * pt + 8 * h + 7 - j:16 * pt + 8 * h + 15 - j] for h in range(2)] for j in range(NUM_STEPS)]
                for i, b in enumerate(seqs):
                    x = src[b, 16 * pt:16 * pt + 16, lanes].astype(F32)
                    for j in range(NUM_STEPS):
                        for h in range(2):
                            term = x[8 * h:8 * h + 8] * w[j][h]
                            accs[i][j] = term if accs[i][j] is None else accs[i][j] + term
            half.append([[pair_rows(accs[0][j], accs[1][j], 4), pair_rows(accs[2][j], accs[3][j], 4)] for j in range(NUM_STEPS)])
        for j in range(NUM_STEPS):
            dst[j, :, lanes] = pair_rows(pair_rows(half[0][j][0], half[1][j][0], 2), pair_rows(half[0][j][1], half[1][j][1], 2), 1)


def stream_kernel(layer, num_in, *refs):
    v_in, z_in, filt = refs[:3]
    v_out, z_out = refs[num_in:num_in + 2]
    parts = refs[num_in + 2:num_in + 6]
    ring, rows, win, in_sem, out_sem, filt_sem = refs[num_in + 6:]
    k = lax.axis_index("sp")
    first = pl.multiple_of(jnp.maximum(2 - k, 0) * SHARD, SHARD)
    units = [(f, d) for f in range(2) for d in range(4)]

    def in_copy(u):
        f, d = units[u]
        seqs = pl.ds(pl.multiple_of(lax.rem(k + d, 4) * BLK, BLK), BLK)
        return pltpu.make_async_copy((v_in, z_in)[f].at[layer, seqs], ring.at[u % SLOTS], in_sem.at[u])

    def out_copy(u):
        f, d = units[u]
        seqs = pl.ds(pl.multiple_of(lax.rem(k + d, 4) * BLK, BLK), BLK)
        return pltpu.make_async_copy(ring.at[u % SLOTS], (v_out, z_out)[f].at[layer, seqs], out_sem.at[u])

    filt_copies = [pltpu.make_async_copy(filt.at[layer, f, pl.ds(first, SHARD + 8)], rows.at[f], filt_sem.at[f]) for f in range(2)]
    filt_copies[0].start()
    in_copy(0).start()
    filt_copies[1].start()
    in_copy(1).start()
    for u, (f, d) in enumerate(units):
        if d == 0:
            filt_copies[f].wait()
            fill_window(win, rows.at[f])
        in_copy(u).wait()
        if u == 0:
            for ahead in range(2, SLOTS):
                in_copy(ahead).start()
        out_copy(u).start()
        conv_block(ring.at[u % SLOTS], win, parts[d].at[f])
        if u >= 1:
            out_copy(u - 1).wait()
            if u - 1 + SLOTS < len(units):
                in_copy(u - 1 + SLOTS).start()
    out_copy(len(units) - 1).wait()


def stream_call(layer, v_cache, z_cache, long_filt, earlier=()):
    hbm = pl.BlockSpec(memory_space=pltpu.HBM)
    num_in = 3 + len(earlier)
    part = jax.ShapeDtypeStruct((2, NUM_STEPS, BLK, CH), F32)
    return pl.pallas_call(
        functools.partial(stream_kernel, layer, num_in),
        out_shape=(jax.ShapeDtypeStruct(v_cache.shape, BF16), jax.ShapeDtypeStruct(z_cache.shape, BF16)) + (part,) * 4,
        in_specs=[hbm] * num_in,
        out_specs=[hbm] * 2 + [pl.BlockSpec(memory_space=pltpu.VMEM)] * 4,
        scratch_shapes=[
            pltpu.VMEM((SLOTS, BLK, SHARD, CH), BF16),
            pltpu.VMEM((2, SHARD + 8, CH), F32),
            pltpu.VMEM((CH // 128, SHARD + 8, 128), F32),
            pltpu.SemaphoreType.DMA((8,)),
            pltpu.SemaphoreType.DMA((8,)),
            pltpu.SemaphoreType.DMA((2,)),
        ],
        input_output_aliases={3: 0, 4: 1} if earlier else {},
        cost_estimate=pl.CostEstimate(flops=SEQ * SHARD * CH * 16, bytes_accessed=4 * SEQ * SHARD * CH * 2, transcendentals=0),
        compiler_params=pltpu.CompilerParams(vmem_limit_bytes=58 << 20),
        name=f"stream_{layer}",
    )(v_cache, z_cache, long_filt, *earlier)


def norm_rows(rows_in):
    mean_val = jnp.mean(rows_in, axis=-1, keepdims=True)
    centered = rows_in - mean_val
    var_val = jnp.mean(centered * centered, axis=-1, keepdims=True)
    return centered * lax.rsqrt(var_val + 1e-5)


def round_bf16(x):
    return x.astype(BF16).astype(F32)


def layer_kernel(*refs):
    sums0 = refs[:4]
    parts1 = refs[4:8]
    (emb_ref, b_in_ref, taps_ref, gain_ref, b_out_ref, filt_hbm, state_hbm, w_in_hbm, w_out_hbm, w_up_hbm, w_down_hbm,
     hid_ref, st_ref, rows_ref,
     w_in, w_out, w_up, w_down, emb32, state, lags, rs_buf, x_send, x_recv, hid_buf, st_buf, row_buf,
     w_sem, s_sem, rs_send, rs_recv, x_ssem, x_rsem, st_ssem, st_rsem, row_ssem, row_rsem, g_ssem, g_rsem) = refs[8:]
    k = lax.axis_index("sp")
    t = lax.axis_index("tp")
    others = [lax.rem(k + d, 4) for d in range(1, 4)]
    mate = k + 1 - 2 * lax.rem(k, 2)
    across = lax.rem(k + 2, 4)
    own = pl.ds(pl.multiple_of(k * BLK, BLK), BLK)

    small = [pltpu.make_async_copy(state_hbm.at[:, own], state, s_sem.at[0]),
             pltpu.make_async_copy(filt_hbm.at[:, :, 0:8], lags, s_sem.at[1])]
    for copy in small:
        copy.start()
    w_copies = []
    for layer in range(NUM_LAYERS):
        for idx, (src, dst) in enumerate(((w_in_hbm, w_in), (w_out_hbm, w_out), (w_up_hbm, w_up), (w_down_hbm, w_down))):
            copy = pltpu.make_async_copy(src.at[layer], dst.at[layer], w_sem.at[layer, idx])
            copy.start()
            w_copies.append(copy)

    barrier = pltpu.get_barrier_semaphore()
    for dev in others:
        pl.semaphore_signal(barrier, inc=1, device_id={"sp": dev}, device_id_type=MESH)
    pl.semaphore_signal(barrier, inc=1, device_id={"tp": 1 - t}, device_id_type=MESH)

    def rs_copy(f, d):
        return pltpu.make_async_remote_copy(
            src_ref=parts1[d].at[f], dst_ref=rs_buf.at[d - 1, f], send_sem=rs_send.at[f, d - 1], recv_sem=rs_recv.at[f, d - 1],
            device_id={"sp": others[d - 1]}, device_id_type=MESH)

    def cached_sum(layer, f, j):
        if layer == 0:
            return (sums0[0][f, j] + sums0[1][f, j]) + (sums0[2][f, j] + sums0[3][f, j])
        return (parts1[0][f, j] + rs_buf[0, f, j]) + (rs_buf[1, f, j] + rs_buf[2, f, j])

    def x_copy(n, h, c):
        return pltpu.make_async_remote_copy(
            src_ref=x_send.at[n, h, c], dst_ref=x_recv.at[n, h, c], send_sem=x_ssem.at[n, h, c], recv_sem=x_rsem.at[n, h, c],
            device_id={"tp": 1 - t}, device_id_type=MESH)

    def row_copy(which, layer, src=None):
        piece = row_buf.at[which, layer, own if src is None else pl.ds(src * BLK, BLK)]
        return pltpu.make_async_remote_copy(
            src_ref=piece, dst_ref=piece, send_sem=row_ssem.at[which, layer],
            recv_sem=row_rsem.at[which, layer, k if src is None else src],
            device_id={"sp": 3}, device_id_type=MESH)

    def st_copy(layer, d):
        piece = st_buf.at[layer, own]
        return pltpu.make_async_remote_copy(
            src_ref=piece, dst_ref=piece, send_sem=st_ssem.at[layer, d], recv_sem=st_rsem.at[layer, d],
            device_id={"sp": others[d]}, device_id_type=MESH)

    def keep_rows(which, layer, vals):
        for b in range(BLK):
            for j in range(NUM_STEPS):
                row_buf[which, layer, k * BLK + b, j:j + 1, :] = vals[j][b:b + 1]

        @pl.when(k < 3)
        def _():
            row_copy(which, layer).start()

    def finish_states(layer):
        for d in range(3):
            st_copy(layer, d).wait_recv()
        st_ref[layer] = st_buf[layer].astype(BF16)

    def long_conv(layer, f, j, vals):
        acc = cached_sum(layer, f, j)
        for i in range(j + 1):
            acc = acc + lags[layer, f, j - i:j - i + 1] * vals[i]
        return acc + gain_ref[layer, f:f + 1] * vals[j]

    proj_rows = [[None] * 3 for _ in range(NUM_LAYERS)]
    v_rows = [[], []]
    z_rows = [[], []]

    def matmul_exchange(n, h, lhs, w_ref, first=False):
        for c in range(NCH):
            x_send[n, h, c] = jnp.dot(lhs, w_ref[:, c * CW:(c + 1) * CW], preferred_element_type=F32)
            if first and c == 0:
                pl.semaphore_wait(barrier, 4)
            x_copy(n, h, c).start()

    def add_exchange(n, h, base):
        outs = []
        for c in range(NCH):
            x_copy(n, h, c).wait_recv()
            outs.append(base[:, c * CW:(c + 1) * CW] + (x_send[n, h, c] + x_recv[n, h, c]))
        return jnp.concatenate(outs, axis=1)

    def front(layer, h, rows_in):
        normed = norm_rows(rows_in).astype(BF16)
        if h == 0:
            w_copies[layer * 4].wait()
        mixed = []
        for g in range(3):
            proj = jnp.dot(normed, w_in[layer, g], preferred_element_type=F32) + b_in_ref[g, layer:layer + 1]
            proj = round_bf16(proj)
            if h == 0:
                proj_rows[layer][g] = [
                    jnp.concatenate([state[layer, b, g, s:s + 1].astype(F32) for b in range(BLK)], axis=0) for s in range(2)]
            seq = proj_rows[layer][g]
            seq += [proj[BLK * i:BLK * i + BLK] for i in range(2)]
            tap = [taps_ref[i, g, layer:layer + 1] for i in range(3)]
            mixed.append([tap[0] * seq[j + 2] + tap[1] * seq[j + 1] + tap[2] * seq[j] for j in (2 * h, 2 * h + 1)])
        ys = []
        v_rows[layer] += [round_bf16(x) for x in mixed[2]]
        if layer == 1 and h == 0:
            for f in range(2):
                for d in range(1, 4):
                    rs_copy(f, d).wait_recv()
        for i in range(2):
            a = long_conv(layer, 0, 2 * h + i, v_rows[layer])
            z_rows[layer].append(round_bf16(mixed[0][i] * a))
            ys.append(mixed[1][i] * long_conv(layer, 1, 2 * h + i, z_rows[layer]))
        if h == 0:
            w_copies[layer * 4 + 1].wait()
        matmul_exchange(layer * 2, h, jnp.concatenate(ys, axis=0).astype(BF16), w_out.at[layer], first=layer == 0 and h == 0)

    def send_kept(layer):
        keep_rows(0, layer, v_rows[layer])
        keep_rows(1, layer, z_rows[layer])
        for g in range(3):
            for s in range(2):
                for i in range(BLK):
                    st_buf[layer, k * BLK + i, g, s:s + 1, :] = proj_rows[layer][g][4 + s][i:i + 1]
        for d in range(3):
            st_copy(layer, d).start()

    def middle(layer, h, rows_in):
        out = add_exchange(layer * 2, h, rows_in) + b_out_ref[layer:layer + 1]
        act = norm_rows(out).astype(BF16)
        if h == 0:
            w_copies[layer * 4 + 2].wait()
        inner = jax.nn.gelu(jnp.dot(act, w_up[layer], preferred_element_type=F32)).astype(BF16)
        if h == 0:
            w_copies[layer * 4 + 3].wait()
        matmul_exchange(layer * 2 + 1, h, inner, w_down.at[layer])
        return out

    for copy in small:
        copy.wait()
    rows_in = []
    for h in range(2):
        emb32[...] = emb_ref[2 * h:2 * h + 2].astype(F32)
        rows_in.append(jnp.concatenate([emb32[i, own] for i in range(2)], axis=0))
    front(0, 0, rows_in[0])
    front(0, 1, rows_in[1])
    for f in range(2):
        for d in range(1, 4):
            rs_copy(f, d).start()
    send_kept(0)
    outs = [middle(0, h, rows_in[h]) for h in range(2)]
    finish_states(0)
    rows_in = []
    for h in range(2):
        rows_in.append(add_exchange(1, h, outs[h]))
        front(1, h, rows_in[h])
    send_kept(1)
    outs = [middle(1, h, rows_in[h]) for h in range(2)]

    def g_copy(h, hop):
        block = k if hop < 2 else across
        dev = across if hop == 1 else mate
        piece = hid_buf.at[h, :, pl.ds(pl.multiple_of(block * BLK, BLK), BLK)]
        return pltpu.make_async_remote_copy(
            src_ref=piece, dst_ref=piece, send_sem=g_ssem.at[h, hop], recv_sem=g_rsem.at[h, hop],
            device_id={"sp": dev}, device_id_type=MESH)

    for h in range(2):
        done = add_exchange(3, h, outs[h])
        for i in range(2):
            hid_buf[h, i, own] = done[BLK * i:BLK * i + BLK]
        g_copy(h, 1).start()
        g_copy(h, 0).start()
    finish_states(1)

    @pl.when(k == 3)
    def _():
        for layer in range(NUM_LAYERS):
            for which in range(2):
                for src in range(3):
                    row_copy(which, layer, src).wait_recv()
        rows_ref[...] = row_buf[...]

    for h in range(2):
        g_copy(h, 1).wait_recv()
        g_copy(h, 2).start()
    for h in range(2):
        g_copy(h, 0).wait_recv()
        g_copy(h, 2).wait_recv()
        hid_ref[2 * h:2 * h + 2] = hid_buf[h]

    for h in range(2):
        for n in range(4):
            for c in range(NCH):
                x_copy(n, h, c).wait_send()
        for hop in range(3):
            g_copy(h, hop).wait_send()
    for f in range(2):
        for d in range(1, 4):
            rs_copy(f, d).wait_send()
    for layer in range(NUM_LAYERS):
        for d in range(3):
            st_copy(layer, d).wait_send()

    @pl.when(k < 3)
    def _():
        for layer in range(NUM_LAYERS):
            for which in range(2):
                row_copy(which, layer).wait_send()


def layer_call(sums0, parts1, step_emb, b_in, taps, gain, b_out, long_filt, state, w_in, w_out, w_up, w_down):
    vm = pl.BlockSpec(memory_space=pltpu.VMEM)
    hbm = pl.BlockSpec(memory_space=pltpu.HBM)
    dma = pltpu.SemaphoreType.DMA
    return pl.pallas_call(
        layer_kernel,
        out_shape=(
            jax.ShapeDtypeStruct((NUM_STEPS, SEQ, DIM), F32),
            jax.ShapeDtypeStruct((NUM_LAYERS, SEQ, 3, 2, CH), BF16),
            jax.ShapeDtypeStruct((2, NUM_LAYERS, SEQ, NUM_STEPS, CH), F32),
        ),
        in_specs=[vm] * 13 + [hbm] * 6,
        out_specs=[vm] * 3,
        scratch_shapes=[
            pltpu.VMEM(w_in.shape, BF16),
            pltpu.VMEM(w_out.shape, BF16),
            pltpu.VMEM(w_up.shape, BF16),
            pltpu.VMEM(w_down.shape, BF16),
            pltpu.VMEM((2, SEQ, DIM), F32),
            pltpu.VMEM((NUM_LAYERS, BLK, 3, 2, CH), BF16),
            pltpu.VMEM((NUM_LAYERS, 2, 8, CH), F32),
            pltpu.VMEM((3, 2, NUM_STEPS, BLK, CH), F32),
            pltpu.VMEM((4, 2, NCH, 2 * BLK, CW), F32),
            pltpu.VMEM((4, 2, NCH, 2 * BLK, CW), F32),
            pltpu.VMEM((2, 2, SEQ, DIM), F32),
            pltpu.VMEM((NUM_LAYERS, SEQ, 3, 2, CH), F32),
            pltpu.VMEM((2, NUM_LAYERS, SEQ, NUM_STEPS, CH), F32),
            dma((NUM_LAYERS, 4)),
            dma((2,)),
            dma((2, 3)),
            dma((2, 3)),
            dma((4, 2, NCH)),
            dma((4, 2, NCH)),
            dma((NUM_LAYERS, 3)),
            dma((NUM_LAYERS, 3)),
            dma((2, NUM_LAYERS)),
            dma((2, NUM_LAYERS, 4)),
            dma((2, 3)),
            dma((2, 3)),
        ],
        compiler_params=pltpu.CompilerParams(collective_id=0, has_side_effects=True, vmem_limit_bytes=44 << 20),
        name="layers",
    )(*sums0, *parts1, step_emb, b_in, taps, gain, b_out, long_filt, state, w_in, w_out, w_up, w_down)


def put_kernel(hid_in, st_in, rows_ref, v_in, z_in, hid_out, st_out, v_out, z_out, wide, tile, sems, o_sem):
    copies = [pltpu.make_async_copy(hid_in, hid_out, o_sem.at[0]), pltpu.make_async_copy(st_in, st_out, o_sem.at[1])]
    for copy in copies:
        copy.start()

    @pl.when(lax.axis_index("sp") == 3)
    def _():
        row_copies = []
        for which, dst in enumerate((v_out, z_out)):
            for layer in range(NUM_LAYERS):
                wide[:, 4:8, :] = jnp.zeros((SEQ, 4, CH), F32)
                wide[:, 0:4, :] = rows_ref[which, layer]
                tile[which, layer] = wide[...].astype(BF16)
                copy = pltpu.make_async_copy(tile.at[which, layer], dst.at[layer, :, 0:8, :], sems.at[which, layer])
                copy.start()
                row_copies.append(copy)
        for copy in row_copies:
            copy.wait()

    for copy in copies:
        copy.wait()


def put_call(hidden, states, rows, v_new, z_new):
    hbm = pl.BlockSpec(memory_space=pltpu.HBM)
    vm = pl.BlockSpec(memory_space=pltpu.VMEM)
    return pl.pallas_call(
        put_kernel,
        out_shape=(jax.ShapeDtypeStruct(hidden.shape, F32), jax.ShapeDtypeStruct(states.shape, BF16),
                   jax.ShapeDtypeStruct(v_new.shape, BF16), jax.ShapeDtypeStruct(z_new.shape, BF16)),
        in_specs=[vm] * 3 + [hbm] * 2,
        out_specs=[hbm] * 4,
        scratch_shapes=[
            pltpu.VMEM((SEQ, 8, CH), F32),
            pltpu.VMEM((2, NUM_LAYERS, SEQ, 8, CH), BF16),
            pltpu.SemaphoreType.DMA((2, NUM_LAYERS)),
            pltpu.SemaphoreType.DMA((2,)),
        ],
        input_output_aliases={3: 2, 4: 3},
        compiler_params=pltpu.CompilerParams(vmem_limit_bytes=16 << 20),
        name="put_rows",
    )(hidden, states, rows, v_new, z_new)


def solution(mesh):
    def device_fn(step_emb, v_cache, z_cache, short_state, w_in, b_in, short_taps, long_filt, skip_gain, w_out, b_out, w_up, w_down):
        v_new, z_new, *parts0 = stream_call(0, v_cache, z_cache, long_filt)
        sums0 = [parts0[0]] + [lax.ppermute(parts0[d], "sp", [(i, (i + d) % 4) for i in range(4)]) for d in range(1, 4)]
        v_new, z_new, *parts1 = stream_call(1, v_cache, z_cache, long_filt, (v_new, z_new))
        hidden, states, rows = layer_call(
            sums0, parts1, step_emb, jnp.transpose(b_in, (1, 0, 2)), jnp.transpose(short_taps, (1, 2, 0, 3)),
            skip_gain, b_out, long_filt, jnp.transpose(short_state, (0, 1, 3, 2, 4)),
            jnp.transpose(w_in, (0, 2, 1, 3)), w_out, w_up, w_down)
        hidden, states, v_new, z_new = put_call(hidden, states, rows, v_new, z_new)
        return hidden, v_new, z_new, jnp.transpose(states, (0, 1, 3, 2, 4))

    specs_in = (
        P(None, "dp", None),
        P(None, "dp", "sp", "tp"),
        P(None, "dp", "sp", "tp"),
        P(None, "dp", None, None, "tp"),
        P(None, None, None, "tp"),
        P(None, None, "tp"),
        P(None, None, None, "tp"),
        P(None, None, None, "tp"),
        P(None, None, "tp"),
        P(None, "tp", None),
        P(None, None),
        P(None, None, "tp"),
        P(None, "tp", None),
    )
    specs_out = (
        P(None, "dp", None),
        P(None, "dp", "sp", "tp"),
        P(None, "dp", "sp", "tp"),
        P(None, "dp", None, None, "tp"),
    )
    return jax.shard_map(device_fn, mesh=mesh, in_specs=specs_in, out_specs=specs_out, check_vma=False)
```

```python
import functools

import jax
import jax.numpy as jnp
from jax import lax
from jax.experimental import pallas as pl
from jax.experimental.pallas import tpu as pltpu
from jax.sharding import PartitionSpec as P

F32 = jnp.float32
BF16 = jnp.bfloat16
NUM_STEPS = 4
NUM_LAYERS = 2
SEQ = 32
BLK = 8
DIM = 1024
CH = 512
UP = 2048
SHARD = 256
NCH = 2
CW = DIM // NCH
SLOTS = 5
MESH = pl.DeviceIdType.MESH


def pair_rows(lo, hi, shift):
    clear = (lax.broadcasted_iota(jnp.int32, (8, 128), 0) // shift) % 2 == 0
    if shift == 4:
        return jnp.where(clear, lo, hi) + pltpu.roll(jnp.where(clear, hi, lo), 4, 0)
    return jnp.where(clear, lo + pltpu.roll(lo, 8 - shift, 0), hi + pltpu.roll(hi, shift, 0))


def fill_window(win, filt_rows):
    flip = 7 - lax.broadcasted_iota(jnp.int32, (8, 128), 0)
    for ct in range(CH // 128):
        for m in range(SHARD // 8 + 1):
            rows = filt_rows[SHARD - 8 * m:SHARD - 8 * m + 8, 128 * ct:128 * ct + 128]
            win[ct, 8 * m:8 * m + 8] = jnp.take_along_axis(rows, flip, axis=0)


def conv_block(src, win, dst):
    @pl.loop(0, CH // 128)
    def _(ct):
        lanes = pl.ds(pl.multiple_of(ct * 128, 128), 128)
        half = []
        for seqs in ((0, 4, 1, 5), (2, 6, 3, 7)):
            accs = [[None] * NUM_STEPS for _ in seqs]
            for pt in range(SHARD // 16):
                w = [[win[ct, 16 * pt + 8 * h + 7 - j:16 * pt + 8 * h + 15 - j] for h in range(2)] for j in range(NUM_STEPS)]
                for i, b in enumerate(seqs):
                    x = src[b, 16 * pt:16 * pt + 16, lanes].astype(F32)
                    for j in range(NUM_STEPS):
                        for h in range(2):
                            term = x[8 * h:8 * h + 8] * w[j][h]
                            accs[i][j] = term if accs[i][j] is None else accs[i][j] + term
            half.append([[pair_rows(accs[0][j], accs[1][j], 4), pair_rows(accs[2][j], accs[3][j], 4)] for j in range(NUM_STEPS)])
        for j in range(NUM_STEPS):
            dst[j, :, lanes] = pair_rows(pair_rows(half[0][j][0], half[1][j][0], 2), pair_rows(half[0][j][1], half[1][j][1], 2), 1)


def stream_kernel(layer, units, num_in, *refs):
    num_conv = 1 + max(f for f, _, conv in units if conv)
    v_in, z_in, filt = refs[:3]
    v_out, z_out = refs[num_in:num_in + 2]
    parts = refs[num_in + 2:num_in + 6]
    ring, rows, win, in_sem, out_sem, filt_sem = refs[num_in + 6:]
    k = lax.axis_index("sp")
    first = pl.multiple_of(jnp.maximum(2 - k, 0) * SHARD, SHARD)

    def seqs(u):
        return pl.ds(pl.multiple_of(lax.rem(k + units[u][1], 4) * BLK, BLK), BLK)

    def in_copy(u):
        return pltpu.make_async_copy((v_in, z_in)[units[u][0]].at[layer, seqs(u)], ring.at[u % SLOTS], in_sem.at[u])

    def out_copy(u):
        return pltpu.make_async_copy(ring.at[u % SLOTS], (v_out, z_out)[units[u][0]].at[layer, seqs(u)], out_sem.at[u])

    filt_copies = [pltpu.make_async_copy(filt.at[layer, f, pl.ds(first, SHARD + 8)], rows.at[f], filt_sem.at[f])
                   for f in range(num_conv)]
    filt_copies[0].start()
    in_copy(0).start()
    for copy in filt_copies[1:]:
        copy.start()
    for u in range(1, SLOTS):
        in_copy(u).start()
    filled = -1
    for u, (f, d, conv) in enumerate(units):
        if conv and f > filled:
            filt_copies[f].wait()
            fill_window(win, rows.at[f])
            filled = f
        in_copy(u).wait()
        out_copy(u).start()
        if conv:
            conv_block(ring.at[u % SLOTS], win, parts[d].at[f])
        if u >= 1:
            out_copy(u - 1).wait()
            if u - 1 + SLOTS < len(units):
                in_copy(u - 1 + SLOTS).start()
    out_copy(len(units) - 1).wait()


def stream_call(layer, units, v_cache, z_cache, long_filt, earlier=()):
    hbm = pl.BlockSpec(memory_space=pltpu.HBM)
    num_in = 3 + len(earlier)
    num_conv = 1 + max(f for f, _, conv in units if conv)
    part = jax.ShapeDtypeStruct((num_conv, NUM_STEPS, BLK, CH), F32)
    return pl.pallas_call(
        functools.partial(stream_kernel, layer, units, num_in),
        out_shape=(jax.ShapeDtypeStruct(v_cache.shape, BF16), jax.ShapeDtypeStruct(z_cache.shape, BF16)) + (part,) * 4,
        in_specs=[hbm] * num_in,
        out_specs=[hbm] * 2 + [pl.BlockSpec(memory_space=pltpu.VMEM)] * 4,
        scratch_shapes=[
            pltpu.VMEM((SLOTS, BLK, SHARD, CH), BF16),
            pltpu.VMEM((2, SHARD + 8, CH), F32),
            pltpu.VMEM((CH // 128, SHARD + 8, 128), F32),
            pltpu.SemaphoreType.DMA((len(units),)),
            pltpu.SemaphoreType.DMA((len(units),)),
            pltpu.SemaphoreType.DMA((2,)),
        ],
        input_output_aliases={3: 0, 4: 1} if earlier else {},
        cost_estimate=pl.CostEstimate(flops=SEQ * SHARD * CH * 16, bytes_accessed=4 * SEQ * SHARD * CH * 2, transcendentals=0),
        compiler_params=pltpu.CompilerParams(vmem_limit_bytes=30 << 20),
        name=f"stream_{layer}",
    )(v_cache, z_cache, long_filt, *earlier)


def norm_rows(rows_in):
    mean_val = jnp.mean(rows_in, axis=-1, keepdims=True)
    centered = rows_in - mean_val
    var_val = jnp.mean(centered * centered, axis=-1, keepdims=True)
    return centered * lax.rsqrt(var_val + 1e-5)


def round_bf16(x):
    return x.astype(BF16).astype(F32)


def layer_kernel(*refs):
    sums0 = refs[:4]
    parts1 = refs[4:8]
    (emb_ref, b_in_ref, taps_ref, gain_ref, b_out_ref, z_hbm, filt_hbm, state_hbm, w_in_hbm, w_out_hbm, w_up_hbm, w_down_hbm,
     hid_ref, st_ref, rows_ref,
     w_in, w_out, w_up, w_down, emb32, state, lags, rs_buf, z_ring, z_filt, win, z_part, st0_buf, x_send, x_recv, hid_buf, st_buf, row_buf,
     w_sem, s_sem, z_sem, rs_send, rs_recv, x_ssem, x_rsem, st_ssem, st_rsem, row_ssem, row_rsem, g_ssem, g_rsem) = refs[8:]
    k = lax.axis_index("sp")
    t = lax.axis_index("tp")
    others = [lax.rem(k + d, 4) for d in range(1, 4)]
    mate = k + 1 - 2 * lax.rem(k, 2)
    across = lax.rem(k + 2, 4)
    own = pl.ds(pl.multiple_of(k * BLK, BLK), BLK)

    small = [pltpu.make_async_copy(state_hbm.at[:, own], state, s_sem.at[0]),
             pltpu.make_async_copy(filt_hbm.at[:, :, 0:8], lags, s_sem.at[1])]
    for copy in small:
        copy.start()
    first = pl.multiple_of(jnp.maximum(2 - k, 0) * SHARD, SHARD)
    z_copies = [pltpu.make_async_copy(z_hbm.at[1, pl.ds(pl.multiple_of(lax.rem(k + d, 4) * BLK, BLK), BLK)], z_ring.at[d], z_sem.at[d])
                for d in range(4)]
    z_filt_copy = pltpu.make_async_copy(filt_hbm.at[1, 1, pl.ds(first, SHARD + 8)], z_filt, z_sem.at[4])
    w_copies = []
    for layer in range(NUM_LAYERS):
        for idx, (src, dst) in enumerate(((w_in_hbm, w_in), (w_out_hbm, w_out), (w_up_hbm, w_up), (w_down_hbm, w_down))):
            copy = pltpu.make_async_copy(src.at[layer], dst.at[layer], w_sem.at[layer, idx])
            copy.start()
            w_copies.append(copy)
            if layer == 0 and idx == 1:
                for copy in [z_filt_copy] + z_copies[1:] + z_copies[:1]:
                    copy.start()

    barrier = pltpu.get_barrier_semaphore()
    for dev in others:
        pl.semaphore_signal(barrier, inc=1, device_id={"sp": dev}, device_id_type=MESH)
    pl.semaphore_signal(barrier, inc=1, device_id={"tp": 1 - t}, device_id_type=MESH)
    pl.semaphore_wait(barrier, 4)

    def part1(f, d):
        return parts1[d].at[0] if f == 0 else z_part.at[d]

    def rs_copy(f, d):
        return pltpu.make_async_remote_copy(
            src_ref=part1(f, d), dst_ref=rs_buf.at[d - 1, f], send_sem=rs_send.at[f, d - 1], recv_sem=rs_recv.at[f, d - 1],
            device_id={"sp": others[d - 1]}, device_id_type=MESH)

    def cached_sum(layer, f, j):
        if layer == 0:
            return (sums0[0][f, j] + sums0[1][f, j]) + (sums0[2][f, j] + sums0[3][f, j])
        return (part1(f, 0)[j] + rs_buf[0, f, j]) + (rs_buf[1, f, j] + rs_buf[2, f, j])

    def x_copy(n, h, c):
        return pltpu.make_async_remote_copy(
            src_ref=x_send.at[n, h, c], dst_ref=x_recv.at[n, h, c], send_sem=x_ssem.at[n, h, c], recv_sem=x_rsem.at[n, h, c],
            device_id={"tp": 1 - t}, device_id_type=MESH)

    def row_copy(which, layer, src=None):
        piece = row_buf.at[which, layer, own if src is None else pl.ds(src * BLK, BLK)]
        return pltpu.make_async_remote_copy(
            src_ref=piece, dst_ref=piece, send_sem=row_ssem.at[which, layer],
            recv_sem=row_rsem.at[which, layer, k if src is None else src],
            device_id={"sp": 3}, device_id_type=MESH)

    def block_of(hop):
        return pl.ds(pl.multiple_of((k if hop < 2 else across) * BLK, BLK), BLK)

    def st_copy(hop):
        piece = st_buf.at[block_of(hop)]
        return pltpu.make_async_remote_copy(
            src_ref=piece, dst_ref=piece, send_sem=st_ssem.at[hop], recv_sem=st_rsem.at[hop],
            device_id={"sp": across if hop == 1 else mate}, device_id_type=MESH)

    def keep_rows(which, layer, vals):
        for b in range(BLK):
            for j in range(NUM_STEPS):
                row_buf[which, layer, k * BLK + b, j:j + 1, :] = vals[j][b:b + 1]

        @pl.when(k < 3)
        def _():
            row_copy(which, layer).start()

    def long_conv(layer, f, j, vals):
        acc = cached_sum(layer, f, j)
        for i in range(j + 1):
            acc = acc + lags[layer, f, j - i:j - i + 1] * vals[i]
        return acc + gain_ref[layer, f:f + 1] * vals[j]

    proj_rows = [[None] * 3 for _ in range(NUM_LAYERS)]
    v_rows = [[], []]
    z_rows = [[], []]

    def matmul_exchange(n, h, lhs, w_ref):
        for c in range(NCH):
            x_send[n, h, c] = jnp.dot(lhs, w_ref[:, c * CW:(c + 1) * CW], preferred_element_type=F32)
            x_copy(n, h, c).start()

    def add_exchange(n, h, base):
        outs = []
        for c in range(NCH):
            x_copy(n, h, c).wait_recv()
            outs.append(base[:, c * CW:(c + 1) * CW] + (x_send[n, h, c] + x_recv[n, h, c]))
        return jnp.concatenate(outs, axis=1)

    def front(layer, h, rows_in):
        normed = norm_rows(rows_in).astype(BF16)
        if h == 0:
            w_copies[layer * 4].wait()
        mixed = []
        for g in range(3):
            proj = jnp.dot(normed, w_in[layer, g], preferred_element_type=F32) + b_in_ref[g, layer:layer + 1]
            proj = round_bf16(proj)
            if h == 0:
                proj_rows[layer][g] = [
                    jnp.concatenate([state[layer, b, g, s:s + 1].astype(F32) for b in range(BLK)], axis=0) for s in range(2)]
            seq = proj_rows[layer][g]
            seq += [proj[BLK * i:BLK * i + BLK] for i in range(2)]
            tap = [taps_ref[i, g, layer:layer + 1] for i in range(3)]
            mixed.append([tap[0] * seq[j + 2] + tap[1] * seq[j + 1] + tap[2] * seq[j] for j in (2 * h, 2 * h + 1)])
        ys = []
        v_rows[layer] += [round_bf16(x) for x in mixed[2]]
        if layer == 1 and h == 0:
            for f in range(2):
                for d in range(1, 4):
                    rs_copy(f, d).wait_recv()
        for i in range(2):
            a = long_conv(layer, 0, 2 * h + i, v_rows[layer])
            z_rows[layer].append(round_bf16(mixed[0][i] * a))
            ys.append(mixed[1][i] * long_conv(layer, 1, 2 * h + i, z_rows[layer]))
        if h == 0:
            w_copies[layer * 4 + 1].wait()
        matmul_exchange(layer * 2, h, jnp.concatenate(ys, axis=0).astype(BF16), w_out.at[layer])

    def send_kept(layer):
        keep_rows(0, layer, v_rows[layer])
        keep_rows(1, layer, z_rows[layer])
    def middle(layer, h, rows_in):
        out = add_exchange(layer * 2, h, rows_in) + b_out_ref[layer:layer + 1]
        act = norm_rows(out).astype(BF16)
        if h == 0:
            w_copies[layer * 4 + 2].wait()
        inner = jax.nn.gelu(jnp.dot(act, w_up[layer], preferred_element_type=F32)).astype(BF16)
        if h == 0:
            w_copies[layer * 4 + 3].wait()
        matmul_exchange(layer * 2 + 1, h, inner, w_down.at[layer])
        return out

    for copy in small:
        copy.wait()
    rows_in = []
    for h in range(2):
        emb32[...] = emb_ref[2 * h:2 * h + 2].astype(F32)
        rows_in.append(jnp.concatenate([emb32[i, own] for i in range(2)], axis=0))
    for d in range(1, 4):
        rs_copy(0, d).start()
    front(0, 0, rows_in[0])
    front(0, 1, rows_in[1])
    send_kept(0)
    z_filt_copy.wait()
    fill_window(win, z_filt)
    for d in range(1, 4):
        z_copies[d].wait()
        conv_block(z_ring.at[d], win, z_part.at[d])
        rs_copy(1, d).start()
    outs = [middle(0, h, rows_in[h]) for h in range(2)]
    z_copies[0].wait()
    conv_block(z_ring.at[0], win, z_part.at[0])

    normed = norm_rows(emb_ref[2:4].astype(F32).reshape(2 * SEQ, DIM)).astype(BF16)
    for g in range(3):
        proj = jnp.dot(normed, w_in[0, g], preferred_element_type=F32) + b_in_ref[g, 0:1]
        for s in range(2):
            for b in range(SEQ):
                st0_buf[b, g, s:s + 1, :] = proj[s * SEQ + b:s * SEQ + b + 1]
    st_ref[0] = st0_buf[...].astype(BF16)

    rows_in = []
    for h in range(2):
        rows_in.append(add_exchange(1, h, outs[h]))
        front(1, h, rows_in[h])
    for g in range(3):
        for s in range(2):
            for i in range(BLK):
                st_buf[k * BLK + i, g, s:s + 1, :] = proj_rows[1][g][4 + s][i:i + 1]
    st_copy(1).start()
    st_copy(0).start()
    send_kept(1)
    outs = [middle(1, h, rows_in[h]) for h in range(2)]
    st_copy(1).wait_recv()
    st_copy(2).start()

    def g_copy(h, hop):
        piece = hid_buf.at[h, :, block_of(hop)]
        return pltpu.make_async_remote_copy(
            src_ref=piece, dst_ref=piece, send_sem=g_ssem.at[h, hop], recv_sem=g_rsem.at[h, hop],
            device_id={"sp": across if hop == 1 else mate}, device_id_type=MESH)

    for h in range(2):
        done = add_exchange(3, h, outs[h])
        for i in range(2):
            hid_buf[h, i, own] = done[BLK * i:BLK * i + BLK]
        g_copy(h, 1).start()
        g_copy(h, 0).start()
    st_copy(0).wait_recv()
    st_copy(2).wait_recv()
    st_ref[1] = st_buf[...].astype(BF16)

    @pl.when(k == 3)
    def _():
        for layer in range(NUM_LAYERS):
            for which in range(2):
                for src in range(3):
                    row_copy(which, layer, src).wait_recv()
        rows_ref[...] = row_buf[...]

    for h in range(2):
        g_copy(h, 1).wait_recv()
        g_copy(h, 2).start()
    for h in range(2):
        g_copy(h, 0).wait_recv()
        g_copy(h, 2).wait_recv()
        hid_ref[2 * h:2 * h + 2] = hid_buf[h]

    for h in range(2):
        for n in range(4):
            for c in range(NCH):
                x_copy(n, h, c).wait_send()
        for hop in range(3):
            g_copy(h, hop).wait_send()
    for f in range(2):
        for d in range(1, 4):
            rs_copy(f, d).wait_send()
    for hop in range(3):
        st_copy(hop).wait_send()

    @pl.when(k < 3)
    def _():
        for layer in range(NUM_LAYERS):
            for which in range(2):
                row_copy(which, layer).wait_send()


def layer_call(sums0, parts1, step_emb, b_in, taps, gain, b_out, z_cache, long_filt, state, w_in, w_out, w_up, w_down):
    vm = pl.BlockSpec(memory_space=pltpu.VMEM)
    hbm = pl.BlockSpec(memory_space=pltpu.HBM)
    dma = pltpu.SemaphoreType.DMA
    return pl.pallas_call(
        layer_kernel,
        out_shape=(
            jax.ShapeDtypeStruct((NUM_STEPS, SEQ, DIM), F32),
            jax.ShapeDtypeStruct((NUM_LAYERS, SEQ, 3, 2, CH), BF16),
            jax.ShapeDtypeStruct((2, NUM_LAYERS, SEQ, NUM_STEPS, CH), F32),
        ),
        in_specs=[vm] * 13 + [hbm] * 7,
        out_specs=[vm] * 3,
        scratch_shapes=[
            pltpu.VMEM(w_in.shape, BF16),
            pltpu.VMEM(w_out.shape, BF16),
            pltpu.VMEM(w_up.shape, BF16),
            pltpu.VMEM(w_down.shape, BF16),
            pltpu.VMEM((2, SEQ, DIM), F32),
            pltpu.VMEM((NUM_LAYERS, BLK, 3, 2, CH), BF16),
            pltpu.VMEM((NUM_LAYERS, 2, 8, CH), F32),
            pltpu.VMEM((3, 2, NUM_STEPS, BLK, CH), F32),
            pltpu.VMEM((4, BLK, SHARD, CH), BF16),
            pltpu.VMEM((SHARD + 8, CH), F32),
            pltpu.VMEM((CH // 128, SHARD + 8, 128), F32),
            pltpu.VMEM((4, NUM_STEPS, BLK, CH), F32),
            pltpu.VMEM((SEQ, 3, 2, CH), F32),
            pltpu.VMEM((4, 2, NCH, 2 * BLK, CW), F32),
            pltpu.VMEM((4, 2, NCH, 2 * BLK, CW), F32),
            pltpu.VMEM((2, 2, SEQ, DIM), F32),
            pltpu.VMEM((SEQ, 3, 2, CH), F32),
            pltpu.VMEM((2, NUM_LAYERS, SEQ, NUM_STEPS, CH), F32),
            dma((NUM_LAYERS, 4)),
            dma((2,)),
            dma((5,)),
            dma((2, 3)),
            dma((2, 3)),
            dma((4, 2, NCH)),
            dma((4, 2, NCH)),
            dma((3,)),
            dma((3,)),
            dma((2, NUM_LAYERS)),
            dma((2, NUM_LAYERS, 4)),
            dma((2, 3)),
            dma((2, 3)),
        ],
        compiler_params=pltpu.CompilerParams(collective_id=0, has_side_effects=True, vmem_limit_bytes=50 << 20),
        name="layers",
    )(*sums0, *parts1, step_emb, b_in, taps, gain, b_out, z_cache, long_filt, state, w_in, w_out, w_up, w_down)


def put_kernel(hid_in, st_in, rows_ref, v_in, z_in, hid_out, st_out, v_out, z_out, wide, tile, sems, o_sem):
    copies = [pltpu.make_async_copy(hid_in, hid_out, o_sem.at[0]), pltpu.make_async_copy(st_in, st_out, o_sem.at[1])]
    for copy in copies:
        copy.start()

    @pl.when(lax.axis_index("sp") == 3)
    def _():
        row_copies = []
        for which, dst in enumerate((v_out, z_out)):
            for layer in range(NUM_LAYERS):
                wide[:, 4:8, :] = jnp.zeros((SEQ, 4, CH), F32)
                wide[:, 0:4, :] = rows_ref[which, layer]
                tile[which, layer] = wide[...].astype(BF16)
                copy = pltpu.make_async_copy(tile.at[which, layer], dst.at[layer, :, 0:8, :], sems.at[which, layer])
                copy.start()
                row_copies.append(copy)
        for copy in row_copies:
            copy.wait()

    for copy in copies:
        copy.wait()


def put_call(hidden, states, rows, v_new, z_new):
    hbm = pl.BlockSpec(memory_space=pltpu.HBM)
    vm = pl.BlockSpec(memory_space=pltpu.VMEM)
    return pl.pallas_call(
        put_kernel,
        out_shape=(jax.ShapeDtypeStruct(hidden.shape, F32), jax.ShapeDtypeStruct(states.shape, BF16),
                   jax.ShapeDtypeStruct(v_new.shape, BF16), jax.ShapeDtypeStruct(z_new.shape, BF16)),
        in_specs=[vm] * 3 + [hbm] * 2,
        out_specs=[hbm] * 4,
        scratch_shapes=[
            pltpu.VMEM((SEQ, 8, CH), F32),
            pltpu.VMEM((2, NUM_LAYERS, SEQ, 8, CH), BF16),
            pltpu.SemaphoreType.DMA((2, NUM_LAYERS)),
            pltpu.SemaphoreType.DMA((2,)),
        ],
        input_output_aliases={3: 2, 4: 3},
        compiler_params=pltpu.CompilerParams(vmem_limit_bytes=16 << 20),
        name="put_rows",
    )(hidden, states, rows, v_new, z_new)


def solution(mesh):
    def device_fn(step_emb, v_cache, z_cache, short_state, w_in, b_in, short_taps, long_filt, skip_gain, w_out, b_out, w_up, w_down):
        v_cache, z_cache, long_filt, w_in, w_out, w_up, w_down = [
            pltpu.with_memory_space_constraint(x, pltpu.HBM)
            for x in (v_cache, z_cache, long_filt, jnp.transpose(w_in, (0, 2, 1, 3)), w_out, w_up, w_down)]
        both = tuple((f, d, True) for f in range(2) for d in range(4))
        v_new, z_new, *parts0 = stream_call(0, both, v_cache, z_cache, long_filt)
        sums0 = [parts0[0]] + [lax.ppermute(parts0[d], "sp", [(i, (i + d) % 4) for i in range(4)]) for d in range(1, 4)]
        mostly_copies = tuple((f, d, f == 0) for d in range(4) for f in range(2))
        v_new, z_new, *parts1 = stream_call(1, mostly_copies, v_cache, z_cache, long_filt, (v_new, z_new))
        hidden, states, rows = layer_call(
            sums0, parts1, step_emb, jnp.transpose(b_in, (1, 0, 2)), jnp.transpose(short_taps, (1, 2, 0, 3)),
            skip_gain, b_out, z_cache, long_filt, jnp.transpose(short_state, (0, 1, 3, 2, 4)),
            w_in, w_out, w_up, w_down)
        hidden, states, v_new, z_new = put_call(hidden, states, rows, v_new, z_new)
        return hidden, v_new, z_new, jnp.transpose(states, (0, 1, 3, 2, 4))

    specs_in = (
        P(None, "dp", None),
        P(None, "dp", "sp", "tp"),
        P(None, "dp", "sp", "tp"),
        P(None, "dp", None, None, "tp"),
        P(None, None, None, "tp"),
        P(None, None, "tp"),
        P(None, None, None, "tp"),
        P(None, None, None, "tp"),
        P(None, None, "tp"),
        P(None, "tp", None),
        P(None, None),
        P(None, None, "tp"),
        P(None, "tp", None),
    )
    specs_out = (
        P(None, "dp", None),
        P(None, "dp", "sp", "tp"),
        P(None, "dp", "sp", "tp"),
        P(None, "dp", None, None, "tp"),
    )
    return jax.shard_map(device_fn, mesh=mesh, in_specs=specs_in, out_specs=specs_out, check_vma=False)
```

```python
import functools

import jax
import jax.numpy as jnp
from jax import lax
from jax.experimental import pallas as pl
from jax.experimental.pallas import tpu as pltpu
from jax.sharding import PartitionSpec as P

F32 = jnp.float32
BF16 = jnp.bfloat16
NUM_STEPS = 4
NUM_LAYERS = 2
SEQ = 32
BLK = 8
DIM = 1024
CH = 512
UP = 2048
SHARD = 256
NCH = 2
CW = DIM // NCH
SLOTS = 8
MESH = pl.DeviceIdType.MESH


def pair_rows(lo, hi, shift):
    clear = (lax.broadcasted_iota(jnp.int32, (8, 128), 0) // shift) % 2 == 0
    if shift == 4:
        return jnp.where(clear, lo, hi) + pltpu.roll(jnp.where(clear, hi, lo), 4, 0)
    return jnp.where(clear, lo + pltpu.roll(lo, 8 - shift, 0), hi + pltpu.roll(hi, shift, 0))


def fill_window(win, filt_rows):
    flip = 7 - lax.broadcasted_iota(jnp.int32, (8, 128), 0)
    for ct in range(CH // 128):
        for m in range(SHARD // 8 + 1):
            rows = filt_rows[SHARD - 8 * m:SHARD - 8 * m + 8, 128 * ct:128 * ct + 128]
            win[ct, 8 * m:8 * m + 8] = jnp.take_along_axis(rows, flip, axis=0)


def conv_block(src, win, dst):
    @pl.loop(0, CH // 128)
    def _(ct):
        lanes = pl.ds(pl.multiple_of(ct * 128, 128), 128)
        half = []
        for seqs in ((0, 4, 1, 5), (2, 6, 3, 7)):
            accs = [[None] * NUM_STEPS for _ in seqs]
            for pt in range(SHARD // 16):
                w = [[win[ct, 16 * pt + 8 * h + 7 - j:16 * pt + 8 * h + 15 - j] for h in range(2)] for j in range(NUM_STEPS)]
                for i, b in enumerate(seqs):
                    x = src[b, 16 * pt:16 * pt + 16, lanes].astype(F32)
                    for j in range(NUM_STEPS):
                        for h in range(2):
                            term = x[8 * h:8 * h + 8] * w[j][h]
                            accs[i][j] = term if accs[i][j] is None else accs[i][j] + term
            half.append([[pair_rows(accs[0][j], accs[1][j], 4), pair_rows(accs[2][j], accs[3][j], 4)] for j in range(NUM_STEPS)])
        for j in range(NUM_STEPS):
            dst[j, :, lanes] = pair_rows(pair_rows(half[0][j][0], half[1][j][0], 2), pair_rows(half[0][j][1], half[1][j][1], 2), 1)


def stream_kernel(layer, units, num_in, *refs):
    num_conv = 1 + max(f for f, _, conv in units if conv)
    v_in, z_in, filt = refs[:3]
    v_out, z_out = refs[num_in:num_in + 2]
    parts = refs[num_in + 2:num_in + 6]
    ring, rows, win, in_sem, out_sem, filt_sem = refs[num_in + 6:]
    k = lax.axis_index("sp")
    first = pl.multiple_of(jnp.maximum(2 - k, 0) * SHARD, SHARD)

    def seqs(u):
        return pl.ds(pl.multiple_of(lax.rem(k + units[u][1], 4) * BLK, BLK), BLK)

    def in_copy(u):
        return pltpu.make_async_copy((v_in, z_in)[units[u][0]].at[layer, seqs(u)], ring.at[u % SLOTS], in_sem.at[u])

    def out_copy(u):
        return pltpu.make_async_copy(ring.at[u % SLOTS], (v_out, z_out)[units[u][0]].at[layer, seqs(u)], out_sem.at[u])

    filt_copies = [pltpu.make_async_copy(filt.at[layer, f, pl.ds(first, SHARD + 8)], rows.at[f], filt_sem.at[f])
                   for f in range(num_conv)]
    filt_copies[0].start()
    in_copy(0).start()
    for copy in filt_copies[1:]:
        copy.start()
    for u in range(1, SLOTS):
        in_copy(u).start()
    filled = -1
    for u, (f, d, conv) in enumerate(units):
        if conv and f > filled:
            filt_copies[f].wait()
            fill_window(win, rows.at[f])
            filled = f
        in_copy(u).wait()
        out_copy(u).start()
        if conv:
            conv_block(ring.at[u % SLOTS], win, parts[d].at[f])
        if u >= 1:
            out_copy(u - 1).wait()
            if u - 1 + SLOTS < len(units):
                in_copy(u - 1 + SLOTS).start()
    out_copy(len(units) - 1).wait()


def stream_call(layer, units, v_cache, z_cache, long_filt, earlier=()):
    hbm = pl.BlockSpec(memory_space=pltpu.HBM)
    num_in = 3 + len(earlier)
    num_conv = 1 + max(f for f, _, conv in units if conv)
    part = jax.ShapeDtypeStruct((num_conv, NUM_STEPS, BLK, CH), F32)
    return pl.pallas_call(
        functools.partial(stream_kernel, layer, units, num_in),
        out_shape=(jax.ShapeDtypeStruct(v_cache.shape, BF16), jax.ShapeDtypeStruct(z_cache.shape, BF16)) + (part,) * 4,
        in_specs=[hbm] * num_in,
        out_specs=[hbm] * 2 + [pl.BlockSpec(memory_space=pltpu.VMEM)] * 4,
        scratch_shapes=[
            pltpu.VMEM((SLOTS, BLK, SHARD, CH), BF16),
            pltpu.VMEM((2, SHARD + 8, CH), F32),
            pltpu.VMEM((CH // 128, SHARD + 8, 128), F32),
            pltpu.SemaphoreType.DMA((len(units),)),
            pltpu.SemaphoreType.DMA((len(units),)),
            pltpu.SemaphoreType.DMA((2,)),
        ],
        input_output_aliases={3: 0, 4: 1} if earlier else {},
        cost_estimate=pl.CostEstimate(flops=SEQ * SHARD * CH * 16, bytes_accessed=4 * SEQ * SHARD * CH * 2, transcendentals=0),
        compiler_params=pltpu.CompilerParams(vmem_limit_bytes=30 << 20),
        name=f"stream_{layer}",
    )(v_cache, z_cache, long_filt, *earlier)


def norm_rows(rows_in):
    mean_val = jnp.mean(rows_in, axis=-1, keepdims=True)
    centered = rows_in - mean_val
    var_val = jnp.mean(centered * centered, axis=-1, keepdims=True)
    return centered * lax.rsqrt(var_val + 1e-5)


def round_bf16(x):
    return x.astype(BF16).astype(F32)


def layer_kernel(*refs):
    sums0 = refs[:4]
    parts1 = refs[4:8]
    (emb_ref, b_in_ref, taps_ref, gain_ref, b_out_ref, filt_hbm, state_hbm, w_in_hbm, w_out_hbm, w_up_hbm, w_down_hbm,
     hid_ref, st_ref, rows_ref,
     w_in, w_out, w_up, w_down, emb32, state, lags, rs_buf, st0_buf, x_send, x_recv, hid_buf, st_buf, row_buf,
     w_sem, s_sem, rs_send, rs_recv, x_ssem, x_rsem, st_ssem, st_rsem, row_ssem, row_rsem, g_ssem, g_rsem) = refs[8:]
    k = lax.axis_index("sp")
    t = lax.axis_index("tp")
    others = [lax.rem(k + d, 4) for d in range(1, 4)]
    mate = k + 1 - 2 * lax.rem(k, 2)
    across = lax.rem(k + 2, 4)
    own = pl.ds(pl.multiple_of(k * BLK, BLK), BLK)

    small = [pltpu.make_async_copy(state_hbm.at[:, own], state, s_sem.at[0]),
             pltpu.make_async_copy(filt_hbm.at[:, :, 0:8], lags, s_sem.at[1])]
    for copy in small:
        copy.start()
    w_pairs = ((w_in_hbm, w_in), (w_out_hbm, w_out), (w_up_hbm, w_up), (w_down_hbm, w_down))
    w_copies = [pltpu.make_async_copy(src.at[layer], dst.at[layer], w_sem.at[layer, idx])
                for layer in range(NUM_LAYERS) for idx, (src, dst) in enumerate(w_pairs)]
    for copy in w_copies[:2]:
        copy.start()

    barrier = pltpu.get_barrier_semaphore()
    for dev in others:
        pl.semaphore_signal(barrier, inc=1, device_id={"sp": dev}, device_id_type=MESH)
    pl.semaphore_signal(barrier, inc=1, device_id={"tp": 1 - t}, device_id_type=MESH)
    pl.semaphore_wait(barrier, 4)

    def rs_copy(f, d):
        return pltpu.make_async_remote_copy(
            src_ref=parts1[d].at[f], dst_ref=rs_buf.at[d - 1, f], send_sem=rs_send.at[f, d - 1], recv_sem=rs_recv.at[f, d - 1],
            device_id={"sp": others[d - 1]}, device_id_type=MESH)

    def cached_sum(layer, f, j):
        if layer == 0:
            return (sums0[0][f, j] + sums0[1][f, j]) + (sums0[2][f, j] + sums0[3][f, j])
        return (parts1[0][f, j] + rs_buf[0, f, j]) + (rs_buf[1, f, j] + rs_buf[2, f, j])

    def x_copy(n, h, c):
        return pltpu.make_async_remote_copy(
            src_ref=x_send.at[n, h, c], dst_ref=x_recv.at[n, h, c], send_sem=x_ssem.at[n, h, c], recv_sem=x_rsem.at[n, h, c],
            device_id={"tp": 1 - t}, device_id_type=MESH)

    def row_copy(which, layer, src=None):
        piece = row_buf.at[which, layer, own if src is None else pl.ds(src * BLK, BLK)]
        return pltpu.make_async_remote_copy(
            src_ref=piece, dst_ref=piece, send_sem=row_ssem.at[which, layer],
            recv_sem=row_rsem.at[which, layer, k if src is None else src],
            device_id={"sp": 3}, device_id_type=MESH)

    def block_of(hop):
        return pl.ds(pl.multiple_of((k if hop < 2 else across) * BLK, BLK), BLK)

    def st_copy(hop):
        piece = st_buf.at[block_of(hop)]
        return pltpu.make_async_remote_copy(
            src_ref=piece, dst_ref=piece, send_sem=st_ssem.at[hop], recv_sem=st_rsem.at[hop],
            device_id={"sp": across if hop == 1 else mate}, device_id_type=MESH)

    def keep_rows(which, layer, vals):
        for b in range(BLK):
            for j in range(NUM_STEPS):
                row_buf[which, layer, k * BLK + b, j:j + 1, :] = vals[j][b:b + 1]

        @pl.when(k < 3)
        def _():
            row_copy(which, layer).start()

    def long_conv(layer, f, j, vals):
        acc = cached_sum(layer, f, j)
        for i in range(j + 1):
            acc = acc + lags[layer, f, j - i:j - i + 1] * vals[i]
        return acc + gain_ref[layer, f:f + 1] * vals[j]

    proj_rows = [[None] * 3 for _ in range(NUM_LAYERS)]
    v_rows = [[], []]
    z_rows = [[], []]

    def matmul_exchange(n, h, lhs, w_ref):
        for c in range(NCH):
            x_send[n, h, c] = jnp.dot(lhs, w_ref[:, c * CW:(c + 1) * CW], preferred_element_type=F32)
            x_copy(n, h, c).start()

    def add_exchange(n, h, base):
        outs = []
        for c in range(NCH):
            x_copy(n, h, c).wait_recv()
            outs.append(base[:, c * CW:(c + 1) * CW] + (x_send[n, h, c] + x_recv[n, h, c]))
        return jnp.concatenate(outs, axis=1)

    def front(layer, h, rows_in):
        normed = norm_rows(rows_in).astype(BF16)
        if h == 0:
            w_copies[layer * 4].wait()
            if layer == 0:
                w_copies[2].start()
        mixed = []
        for g in range(3):
            proj = jnp.dot(normed, w_in[layer, g], preferred_element_type=F32) + b_in_ref[g, layer:layer + 1]
            proj = round_bf16(proj)
            if h == 0:
                proj_rows[layer][g] = [
                    jnp.concatenate([state[layer, b, g, s:s + 1].astype(F32) for b in range(BLK)], axis=0) for s in range(2)]
            seq = proj_rows[layer][g]
            seq += [proj[BLK * i:BLK * i + BLK] for i in range(2)]
            tap = [taps_ref[i, g, layer:layer + 1] for i in range(3)]
            mixed.append([tap[0] * seq[j + 2] + tap[1] * seq[j + 1] + tap[2] * seq[j] for j in (2 * h, 2 * h + 1)])
        ys = []
        v_rows[layer] += [round_bf16(x) for x in mixed[2]]
        if layer == 1 and h == 0:
            for f in range(2):
                for d in range(1, 4):
                    rs_copy(f, d).wait_recv()
        for i in range(2):
            a = long_conv(layer, 0, 2 * h + i, v_rows[layer])
            z_rows[layer].append(round_bf16(mixed[0][i] * a))
            ys.append(mixed[1][i] * long_conv(layer, 1, 2 * h + i, z_rows[layer]))
        if h == 0:
            w_copies[layer * 4 + 1].wait()
        matmul_exchange(layer * 2, h, jnp.concatenate(ys, axis=0).astype(BF16), w_out.at[layer])

    def send_kept(layer):
        keep_rows(0, layer, v_rows[layer])
        keep_rows(1, layer, z_rows[layer])
    def middle(layer, h, rows_in):
        out = add_exchange(layer * 2, h, rows_in) + b_out_ref[layer:layer + 1]
        act = norm_rows(out).astype(BF16)
        if h == 0:
            w_copies[layer * 4 + 2].wait()
        inner = jax.nn.gelu(jnp.dot(act, w_up[layer], preferred_element_type=F32)).astype(BF16)
        if h == 0:
            w_copies[layer * 4 + 3].wait()
        matmul_exchange(layer * 2 + 1, h, inner, w_down.at[layer])
        return out

    for copy in small:
        copy.wait()
    rows_in = []
    for h in range(2):
        emb32[...] = emb_ref[2 * h:2 * h + 2].astype(F32)
        rows_in.append(jnp.concatenate([emb32[i, own] for i in range(2)], axis=0))
    front(0, 0, rows_in[0])
    w_copies[3].start()
    front(0, 1, rows_in[1])
    for copy in w_copies[4:6]:
        copy.start()
    for f in range(2):
        for d in range(1, 4):
            rs_copy(f, d).start()
    send_kept(0)
    outs = [middle(0, h, rows_in[h]) for h in range(2)]
    for copy in w_copies[6:8]:
        copy.start()

    normed = norm_rows(emb_ref[2:4].astype(F32).reshape(2 * SEQ, DIM)).astype(BF16)
    for g in range(3):
        proj = jnp.dot(normed, w_in[0, g], preferred_element_type=F32) + b_in_ref[g, 0:1]
        for s in range(2):
            for b in range(SEQ):
                st0_buf[b, g, s:s + 1, :] = proj[s * SEQ + b:s * SEQ + b + 1]
    st_ref[0] = st0_buf[...].astype(BF16)

    rows_in = []
    for h in range(2):
        rows_in.append(add_exchange(1, h, outs[h]))
        front(1, h, rows_in[h])
    for g in range(3):
        for s in range(2):
            for i in range(BLK):
                st_buf[k * BLK + i, g, s:s + 1, :] = proj_rows[1][g][4 + s][i:i + 1]
    st_copy(1).start()
    st_copy(0).start()
    send_kept(1)
    outs = [middle(1, h, rows_in[h]) for h in range(2)]
    st_copy(1).wait_recv()
    st_copy(2).start()

    def g_copy(h, hop):
        piece = hid_buf.at[h, :, block_of(hop)]
        return pltpu.make_async_remote_copy(
            src_ref=piece, dst_ref=piece, send_sem=g_ssem.at[h, hop], recv_sem=g_rsem.at[h, hop],
            device_id={"sp": across if hop == 1 else mate}, device_id_type=MESH)

    for h in range(2):
        done = add_exchange(3, h, outs[h])
        for i in range(2):
            hid_buf[h, i, own] = done[BLK * i:BLK * i + BLK]
        g_copy(h, 1).start()
        g_copy(h, 0).start()
    st_copy(0).wait_recv()
    st_copy(2).wait_recv()
    st_ref[1] = st_buf[...].astype(BF16)

    @pl.when(k == 3)
    def _():
        for layer in range(NUM_LAYERS):
            for which in range(2):
                for src in range(3):
                    row_copy(which, layer, src).wait_recv()
        rows_ref[...] = row_buf[...]

    for h in range(2):
        g_copy(h, 1).wait_recv()
        g_copy(h, 2).start()
    for h in range(2):
        g_copy(h, 0).wait_recv()
        g_copy(h, 2).wait_recv()
        hid_ref[2 * h:2 * h + 2] = hid_buf[h]

    for h in range(2):
        for n in range(4):
            for c in range(NCH):
                x_copy(n, h, c).wait_send()
        for hop in range(3):
            g_copy(h, hop).wait_send()
    for f in range(2):
        for d in range(1, 4):
            rs_copy(f, d).wait_send()
    for hop in range(3):
        st_copy(hop).wait_send()

    @pl.when(k < 3)
    def _():
        for layer in range(NUM_LAYERS):
            for which in range(2):
                row_copy(which, layer).wait_send()


def layer_call(sums0, parts1, step_emb, b_in, taps, gain, b_out, long_filt, state, w_in, w_out, w_up, w_down):
    vm = pl.BlockSpec(memory_space=pltpu.VMEM)
    hbm = pl.BlockSpec(memory_space=pltpu.HBM)
    dma = pltpu.SemaphoreType.DMA
    return pl.pallas_call(
        layer_kernel,
        out_shape=(
            jax.ShapeDtypeStruct((NUM_STEPS, SEQ, DIM), F32),
            jax.ShapeDtypeStruct((NUM_LAYERS, SEQ, 3, 2, CH), BF16),
            jax.ShapeDtypeStruct((2, NUM_LAYERS, SEQ, NUM_STEPS, CH), F32),
        ),
        in_specs=[vm] * 13 + [hbm] * 6,
        out_specs=[vm] * 3,
        scratch_shapes=[
            pltpu.VMEM(w_in.shape, BF16),
            pltpu.VMEM(w_out.shape, BF16),
            pltpu.VMEM(w_up.shape, BF16),
            pltpu.VMEM(w_down.shape, BF16),
            pltpu.VMEM((2, SEQ, DIM), F32),
            pltpu.VMEM((NUM_LAYERS, BLK, 3, 2, CH), BF16),
            pltpu.VMEM((NUM_LAYERS, 2, 8, CH), F32),
            pltpu.VMEM((3, 2, NUM_STEPS, BLK, CH), F32),
            pltpu.VMEM((SEQ, 3, 2, CH), F32),
            pltpu.VMEM((4, 2, NCH, 2 * BLK, CW), F32),
            pltpu.VMEM((4, 2, NCH, 2 * BLK, CW), F32),
            pltpu.VMEM((2, 2, SEQ, DIM), F32),
            pltpu.VMEM((SEQ, 3, 2, CH), F32),
            pltpu.VMEM((2, NUM_LAYERS, SEQ, NUM_STEPS, CH), F32),
            dma((NUM_LAYERS, 4)),
            dma((2,)),
            dma((2, 3)),
            dma((2, 3)),
            dma((4, 2, NCH)),
            dma((4, 2, NCH)),
            dma((3,)),
            dma((3,)),
            dma((2, NUM_LAYERS)),
            dma((2, NUM_LAYERS, 4)),
            dma((2, 3)),
            dma((2, 3)),
        ],
        compiler_params=pltpu.CompilerParams(collective_id=0, has_side_effects=True, vmem_limit_bytes=44 << 20),
        name="layers",
    )(*sums0, *parts1, step_emb, b_in, taps, gain, b_out, long_filt, state, w_in, w_out, w_up, w_down)


def put_kernel(hid_in, st_in, rows_ref, v_in, z_in, hid_out, st_out, v_out, z_out, wide, tile, sems, o_sem):
    copies = [pltpu.make_async_copy(hid_in, hid_out, o_sem.at[0]), pltpu.make_async_copy(st_in, st_out, o_sem.at[1])]
    for copy in copies:
        copy.start()

    @pl.when(lax.axis_index("sp") == 3)
    def _():
        row_copies = []
        for which, dst in enumerate((v_out, z_out)):
            for layer in range(NUM_LAYERS):
                wide[:, 4:8, :] = jnp.zeros((SEQ, 4, CH), F32)
                wide[:, 0:4, :] = rows_ref[which, layer]
                tile[which, layer] = wide[...].astype(BF16)
                copy = pltpu.make_async_copy(tile.at[which, layer], dst.at[layer, :, 0:8, :], sems.at[which, layer])
                copy.start()
                row_copies.append(copy)
        for copy in row_copies:
            copy.wait()

    for copy in copies:
        copy.wait()


def put_call(hidden, states, rows, v_new, z_new):
    hbm = pl.BlockSpec(memory_space=pltpu.HBM)
    vm = pl.BlockSpec(memory_space=pltpu.VMEM)
    return pl.pallas_call(
        put_kernel,
        out_shape=(jax.ShapeDtypeStruct(hidden.shape, F32), jax.ShapeDtypeStruct(states.shape, BF16),
                   jax.ShapeDtypeStruct(v_new.shape, BF16), jax.ShapeDtypeStruct(z_new.shape, BF16)),
        in_specs=[vm] * 3 + [hbm] * 2,
        out_specs=[hbm] * 4,
        scratch_shapes=[
            pltpu.VMEM((SEQ, 8, CH), F32),
            pltpu.VMEM((2, NUM_LAYERS, SEQ, 8, CH), BF16),
            pltpu.SemaphoreType.DMA((2, NUM_LAYERS)),
            pltpu.SemaphoreType.DMA((2,)),
        ],
        input_output_aliases={3: 2, 4: 3},
        compiler_params=pltpu.CompilerParams(vmem_limit_bytes=16 << 20),
        name="put_rows",
    )(hidden, states, rows, v_new, z_new)


def solution(mesh):
    def device_fn(step_emb, v_cache, z_cache, short_state, w_in, b_in, short_taps, long_filt, skip_gain, w_out, b_out, w_up, w_down):
        v_cache, z_cache, long_filt, w_in, w_out, w_up, w_down = [
            pltpu.with_memory_space_constraint(x, pltpu.HBM)
            for x in (v_cache, z_cache, long_filt, jnp.transpose(w_in, (0, 2, 1, 3)), w_out, w_up, w_down)]
        both = tuple((f, d, True) for f in range(2) for d in range(4))
        v_new, z_new, *parts0 = stream_call(0, both, v_cache, z_cache, long_filt)
        sums0 = [parts0[0]] + [lax.ppermute(parts0[d], "sp", [(i, (i + d) % 4) for i in range(4)]) for d in range(1, 4)]
        v_new, z_new, *parts1 = stream_call(1, both, v_cache, z_cache, long_filt, (v_new, z_new))
        hidden, states, rows = layer_call(
            sums0, parts1, step_emb, jnp.transpose(b_in, (1, 0, 2)), jnp.transpose(short_taps, (1, 2, 0, 3)),
            skip_gain, b_out, long_filt, jnp.transpose(short_state, (0, 1, 3, 2, 4)),
            w_in, w_out, w_up, w_down)
        hidden, states, v_new, z_new = put_call(hidden, states, rows, v_new, z_new)
        return hidden, v_new, z_new, jnp.transpose(states, (0, 1, 3, 2, 4))

    specs_in = (
        P(None, "dp", None),
        P(None, "dp", "sp", "tp"),
        P(None, "dp", "sp", "tp"),
        P(None, "dp", None, None, "tp"),
        P(None, None, None, "tp"),
        P(None, None, "tp"),
        P(None, None, None, "tp"),
        P(None, None, None, "tp"),
        P(None, None, "tp"),
        P(None, "tp", None),
        P(None, None),
        P(None, None, "tp"),
        P(None, "tp", None),
    )
    specs_out = (
        P(None, "dp", None),
        P(None, "dp", "sp", "tp"),
        P(None, "dp", "sp", "tp"),
        P(None, "dp", None, None, "tp"),
    )
    return jax.shard_map(device_fn, mesh=mesh, in_specs=specs_in, out_specs=specs_out, check_vma=False)
```

```python
import functools

import jax
import jax.numpy as jnp
from jax import lax
from jax.experimental import pallas as pl
from jax.experimental.pallas import tpu as pltpu
from jax.sharding import PartitionSpec as P

F32 = jnp.float32
BF16 = jnp.bfloat16
NUM_STEPS = 4
NUM_LAYERS = 2
SEQ = 32
BLK = 8
DIM = 1024
CH = 512
UP = 2048
SHARD = 256
NCH = 2
CW = DIM // NCH
SLOTS = 8
MESH = pl.DeviceIdType.MESH


def pair_rows(lo, hi, shift):
    clear = (lax.broadcasted_iota(jnp.int32, (8, 128), 0) // shift) % 2 == 0
    if shift == 4:
        return jnp.where(clear, lo, hi) + pltpu.roll(jnp.where(clear, hi, lo), 4, 0)
    return jnp.where(clear, lo + pltpu.roll(lo, 8 - shift, 0), hi + pltpu.roll(hi, shift, 0))


def fill_window(win, filt_rows, ct):
    flip = 7 - lax.broadcasted_iota(jnp.int32, (8, 128), 0)
    lanes = pl.ds(pl.multiple_of(ct * 128, 128), 128)
    for m in range(SHARD // 8 + 1):
        rows = filt_rows[SHARD - 8 * m:SHARD - 8 * m + 8, lanes]
        win[ct, 8 * m:8 * m + 8] = jnp.take_along_axis(rows, flip, axis=0)


def conv_block(src, win, dst, ready):
    @pl.loop(0, CH // 128)
    def _(ct):
        ready(ct)
        lanes = pl.ds(pl.multiple_of(ct * 128, 128), 128)
        half = []
        for seqs in ((0, 4, 1, 5), (2, 6, 3, 7)):
            accs = [[None] * NUM_STEPS for _ in seqs]
            for pt in range(SHARD // 16):
                w = [[win[ct, 16 * pt + 8 * h + 7 - j:16 * pt + 8 * h + 15 - j] for h in range(2)] for j in range(NUM_STEPS)]
                for i, b in enumerate(seqs):
                    x = src[b, 16 * pt:16 * pt + 16, lanes].astype(F32)
                    for j in range(NUM_STEPS):
                        for h in range(2):
                            term = x[8 * h:8 * h + 8] * w[j][h]
                            accs[i][j] = term if accs[i][j] is None else accs[i][j] + term
            half.append([[pair_rows(accs[0][j], accs[1][j], 4), pair_rows(accs[2][j], accs[3][j], 4)] for j in range(NUM_STEPS)])
        for j in range(NUM_STEPS):
            dst[j, :, lanes] = pair_rows(pair_rows(half[0][j][0], half[1][j][0], 2), pair_rows(half[0][j][1], half[1][j][1], 2), 1)


def stream_kernel(layer, units, num_in, *refs):
    num_conv = 1 + max(f for f, _, conv in units if conv)
    v_in, z_in, filt = refs[:3]
    v_out, z_out = refs[num_in:num_in + 2]
    parts = refs[num_in + 2:num_in + 6]
    ring, rows, win, in_sem, out_sem, filt_sem, lane_sem = refs[num_in + 6:]
    k = lax.axis_index("sp")
    first = pl.multiple_of(jnp.maximum(2 - k, 0) * SHARD, SHARD)

    def seqs(u):
        return pl.ds(pl.multiple_of(lax.rem(k + units[u][1], 4) * BLK, BLK), BLK)

    def in_copy(u):
        return pltpu.make_async_copy((v_in, z_in)[units[u][0]].at[layer, seqs(u)], ring.at[u], in_sem.at[u])

    def lane_copy(ct):
        lanes = pl.ds(pl.multiple_of(ct * 128, 128), 128)
        return pltpu.make_async_copy(
            (v_in, z_in)[units[0][0]].at[layer, seqs(0), :, lanes], ring.at[0, :, :, lanes], lane_sem.at[ct])

    def out_copy(u):
        return pltpu.make_async_copy(ring.at[u], (v_out, z_out)[units[u][0]].at[layer, seqs(u)], out_sem.at[u])

    filt_copies = [pltpu.make_async_copy(filt.at[layer, f, pl.ds(first, SHARD + 8)], rows.at[f], filt_sem.at[f])
                   for f in range(num_conv)]
    filt_copies[0].start()
    for ct in range(CH // 128):
        lane_copy(ct).start()
    filt_copies[0].wait()
    for u, (f, d, conv) in enumerate(units):
        new_filter = d == 0 and conv
        if u == 0:
            in_copy(1).start()

            def ready(ct):
                fill_window(win, rows.at[0], ct)
                lane_copy(ct).wait()

            conv_block(ring.at[0], win, parts[0].at[0], ready)
            out_copy(0).start()
            in_copy(2).start()
            for copy in filt_copies[1:]:
                copy.start()
            continue
        in_copy(u).wait()
        out_copy(u).start()
        if u + 2 < len(units):
            in_copy(u + 2).start()
        if new_filter:
            filt_copies[f].wait()
        if conv:
            conv_block(ring.at[u], win, parts[d].at[f],
                       (lambda ct, f=f: fill_window(win, rows.at[f], ct)) if new_filter else (lambda ct: None))
    for u in range(len(units)):
        out_copy(u).wait()


def stream_call(layer, units, v_cache, z_cache, long_filt, earlier=()):
    hbm = pl.BlockSpec(memory_space=pltpu.HBM)
    num_in = 3 + len(earlier)
    num_conv = 1 + max(f for f, _, conv in units if conv)
    part = jax.ShapeDtypeStruct((num_conv, NUM_STEPS, BLK, CH), F32)
    return pl.pallas_call(
        functools.partial(stream_kernel, layer, units, num_in),
        out_shape=(jax.ShapeDtypeStruct(v_cache.shape, BF16), jax.ShapeDtypeStruct(z_cache.shape, BF16)) + (part,) * 4,
        in_specs=[hbm] * num_in,
        out_specs=[hbm] * 2 + [pl.BlockSpec(memory_space=pltpu.VMEM)] * 4,
        scratch_shapes=[
            pltpu.VMEM((SLOTS, BLK, SHARD, CH), BF16),
            pltpu.VMEM((2, SHARD + 8, CH), F32),
            pltpu.VMEM((CH // 128, SHARD + 8, 128), F32),
            pltpu.SemaphoreType.DMA((len(units),)),
            pltpu.SemaphoreType.DMA((len(units),)),
            pltpu.SemaphoreType.DMA((2,)),
            pltpu.SemaphoreType.DMA((CH // 128,)),
        ],
        input_output_aliases={3: 0, 4: 1} if earlier else {},
        cost_estimate=pl.CostEstimate(flops=SEQ * SHARD * CH * 16, bytes_accessed=4 * SEQ * SHARD * CH * 2, transcendentals=0),
        compiler_params=pltpu.CompilerParams(vmem_limit_bytes=30 << 20),
        name=f"stream_{layer}",
    )(v_cache, z_cache, long_filt, *earlier)


def norm_rows(rows_in):
    mean_val = jnp.mean(rows_in, axis=-1, keepdims=True)
    centered = rows_in - mean_val
    var_val = jnp.mean(centered * centered, axis=-1, keepdims=True)
    return centered * lax.rsqrt(var_val + 1e-5)


def round_bf16(x):
    return x.astype(BF16).astype(F32)


def layer_kernel(*refs):
    sums0 = refs[:4]
    parts1 = refs[4:8]
    (emb_ref, b_in_ref, taps_ref, gain_ref, b_out_ref, filt_hbm, state_hbm, w_in_hbm, w_out_hbm, w_up_hbm, w_down_hbm,
     hid_ref, st_ref, rows_ref,
     w_in, w_out, w_up, w_down, emb32, state, lags, rs_buf, st0_buf, x_send, x_recv, hid_buf, st_buf, row_buf,
     w_sem, s_sem, rs_send, rs_recv, x_ssem, x_rsem, st_ssem, st_rsem, row_ssem, row_rsem, g_ssem, g_rsem) = refs[8:]
    k = lax.axis_index("sp")
    t = lax.axis_index("tp")
    others = [lax.rem(k + d, 4) for d in range(1, 4)]
    mate = k + 1 - 2 * lax.rem(k, 2)
    across = lax.rem(k + 2, 4)
    own = pl.ds(pl.multiple_of(k * BLK, BLK), BLK)

    small = [pltpu.make_async_copy(state_hbm.at[:, own], state, s_sem.at[0]),
             pltpu.make_async_copy(filt_hbm.at[:, :, 0:8], lags, s_sem.at[1])]
    for copy in small:
        copy.start()
    w_pairs = ((w_in_hbm, w_in), (w_out_hbm, w_out), (w_up_hbm, w_up), (w_down_hbm, w_down))
    w_copies = [pltpu.make_async_copy(src.at[layer], dst.at[layer], w_sem.at[layer, idx])
                for layer in range(NUM_LAYERS) for idx, (src, dst) in enumerate(w_pairs)]
    for copy in w_copies[:2]:
        copy.start()

    barrier = pltpu.get_barrier_semaphore()
    for dev in others:
        pl.semaphore_signal(barrier, inc=1, device_id={"sp": dev}, device_id_type=MESH)
    pl.semaphore_signal(barrier, inc=1, device_id={"tp": 1 - t}, device_id_type=MESH)
    pl.semaphore_wait(barrier, 4)

    def rs_copy(f, d):
        return pltpu.make_async_remote_copy(
            src_ref=parts1[d].at[f], dst_ref=rs_buf.at[d - 1, f], send_sem=rs_send.at[f, d - 1], recv_sem=rs_recv.at[f, d - 1],
            device_id={"sp": others[d - 1]}, device_id_type=MESH)

    def cached_sum(layer, f, j):
        if layer == 0:
            return (sums0[0][f, j] + sums0[1][f, j]) + (sums0[2][f, j] + sums0[3][f, j])
        return (parts1[0][f, j] + rs_buf[0, f, j]) + (rs_buf[1, f, j] + rs_buf[2, f, j])

    def x_copy(n, h, c):
        return pltpu.make_async_remote_copy(
            src_ref=x_send.at[n, h, c], dst_ref=x_recv.at[n, h, c], send_sem=x_ssem.at[n, h, c], recv_sem=x_rsem.at[n, h, c],
            device_id={"tp": 1 - t}, device_id_type=MESH)

    def row_copy(which, layer, src=None):
        piece = row_buf.at[which, layer, own if src is None else pl.ds(src * BLK, BLK)]
        return pltpu.make_async_remote_copy(
            src_ref=piece, dst_ref=piece, send_sem=row_ssem.at[which, layer],
            recv_sem=row_rsem.at[which, layer, k if src is None else src],
            device_id={"sp": 3}, device_id_type=MESH)

    def block_of(hop):
        return pl.ds(pl.multiple_of((k if hop < 2 else across) * BLK, BLK), BLK)

    def st_copy(hop):
        piece = st_buf.at[block_of(hop)]
        return pltpu.make_async_remote_copy(
            src_ref=piece, dst_ref=piece, send_sem=st_ssem.at[hop], recv_sem=st_rsem.at[hop],
            device_id={"sp": across if hop == 1 else mate}, device_id_type=MESH)

    def keep_rows(which, layer, vals):
        for b in range(BLK):
            for j in range(NUM_STEPS):
                row_buf[which, layer, k * BLK + b, j:j + 1, :] = vals[j][b:b + 1]

        @pl.when(k < 3)
        def _():
            row_copy(which, layer).start()

    def long_conv(layer, f, j, vals):
        acc = cached_sum(layer, f, j)
        for i in range(j + 1):
            acc = acc + lags[layer, f, j - i:j - i + 1] * vals[i]
        return acc + gain_ref[layer, f:f + 1] * vals[j]

    proj_rows = [[None] * 3 for _ in range(NUM_LAYERS)]
    v_rows = [[], []]
    z_rows = [[], []]

    def matmul_exchange(n, h, lhs, w_ref):
        for c in range(NCH):
            x_send[n, h, c] = jnp.dot(lhs, w_ref[:, c * CW:(c + 1) * CW], preferred_element_type=F32)
            x_copy(n, h, c).start()

    def add_exchange(n, h, base):
        outs = []
        for c in range(NCH):
            x_copy(n, h, c).wait_recv()
            outs.append(base[:, c * CW:(c + 1) * CW] + (x_send[n, h, c] + x_recv[n, h, c]))
        return jnp.concatenate(outs, axis=1)

    def front(layer, h, rows_in):
        normed = norm_rows(rows_in).astype(BF16)
        if h == 0:
            w_copies[layer * 4].wait()
            if layer == 0:
                w_copies[2].start()
        mixed = []
        for g in range(3):
            proj = jnp.dot(normed, w_in[layer, g], preferred_element_type=F32) + b_in_ref[g, layer:layer + 1]
            proj = round_bf16(proj)
            if h == 0:
                proj_rows[layer][g] = [
                    jnp.concatenate([state[layer, b, g, s:s + 1].astype(F32) for b in range(BLK)], axis=0) for s in range(2)]
            seq = proj_rows[layer][g]
            seq += [proj[BLK * i:BLK * i + BLK] for i in range(2)]
            tap = [taps_ref[i, g, layer:layer + 1] for i in range(3)]
            mixed.append([tap[0] * seq[j + 2] + tap[1] * seq[j + 1] + tap[2] * seq[j] for j in (2 * h, 2 * h + 1)])
        ys = []
        v_rows[layer] += [round_bf16(x) for x in mixed[2]]
        if layer == 1 and h == 0:
            for f in range(2):
                for d in range(1, 4):
                    rs_copy(f, d).wait_recv()
        for i in range(2):
            a = long_conv(layer, 0, 2 * h + i, v_rows[layer])
            z_rows[layer].append(round_bf16(mixed[0][i] * a))
            ys.append(mixed[1][i] * long_conv(layer, 1, 2 * h + i, z_rows[layer]))
        if h == 0:
            w_copies[layer * 4 + 1].wait()
        matmul_exchange(layer * 2, h, jnp.concatenate(ys, axis=0).astype(BF16), w_out.at[layer])

    def send_kept(layer):
        keep_rows(0, layer, v_rows[layer])
        keep_rows(1, layer, z_rows[layer])
    def middle(layer, h, rows_in):
        out = add_exchange(layer * 2, h, rows_in) + b_out_ref[layer:layer + 1]
        act = norm_rows(out).astype(BF16)
        if h == 0:
            w_copies[layer * 4 + 2].wait()
        inner = jax.nn.gelu(jnp.dot(act, w_up[layer], preferred_element_type=F32)).astype(BF16)
        if h == 0:
            w_copies[layer * 4 + 3].wait()
        matmul_exchange(layer * 2 + 1, h, inner, w_down.at[layer])
        return out

    for copy in small:
        copy.wait()
    rows_in = []
    for h in range(2):
        emb32[...] = emb_ref[2 * h:2 * h + 2].astype(F32)
        rows_in.append(jnp.concatenate([emb32[i, own] for i in range(2)], axis=0))
    front(0, 0, rows_in[0])
    w_copies[3].start()
    front(0, 1, rows_in[1])
    for copy in w_copies[4:6]:
        copy.start()
    for f in range(2):
        for d in range(1, 4):
            rs_copy(f, d).start()
    send_kept(0)
    outs = [middle(0, h, rows_in[h]) for h in range(2)]
    for copy in w_copies[6:8]:
        copy.start()

    normed = norm_rows(emb_ref[2:4].astype(F32).reshape(2 * SEQ, DIM)).astype(BF16)
    for g in range(3):
        proj = jnp.dot(normed, w_in[0, g], preferred_element_type=F32) + b_in_ref[g, 0:1]
        for s in range(2):
            for b in range(SEQ):
                st0_buf[b, g, s:s + 1, :] = proj[s * SEQ + b:s * SEQ + b + 1]
    st_ref[0] = st0_buf[...].astype(BF16)

    rows_in = []
    for h in range(2):
        rows_in.append(add_exchange(1, h, outs[h]))
        front(1, h, rows_in[h])
    for g in range(3):
        for s in range(2):
            for i in range(BLK):
                st_buf[k * BLK + i, g, s:s + 1, :] = proj_rows[1][g][4 + s][i:i + 1]
    st_copy(1).start()
    st_copy(0).start()
    send_kept(1)
    outs = [middle(1, h, rows_in[h]) for h in range(2)]
    st_copy(1).wait_recv()
    st_copy(2).start()

    def g_copy(h, hop):
        piece = hid_buf.at[h, :, block_of(hop)]
        return pltpu.make_async_remote_copy(
            src_ref=piece, dst_ref=piece, send_sem=g_ssem.at[h, hop], recv_sem=g_rsem.at[h, hop],
            device_id={"sp": across if hop == 1 else mate}, device_id_type=MESH)

    for h in range(2):
        done = add_exchange(3, h, outs[h])
        for i in range(2):
            hid_buf[h, i, own] = done[BLK * i:BLK * i + BLK]
        g_copy(h, 1).start()
        g_copy(h, 0).start()
    st_copy(0).wait_recv()
    st_copy(2).wait_recv()
    st_ref[1] = st_buf[...].astype(BF16)

    @pl.when(k == 3)
    def _():
        for layer in range(NUM_LAYERS):
            for which in range(2):
                for src in range(3):
                    row_copy(which, layer, src).wait_recv()
        rows_ref[...] = row_buf[...]

    for h in range(2):
        g_copy(h, 1).wait_recv()
        g_copy(h, 2).start()
    for h in range(2):
        g_copy(h, 0).wait_recv()
        g_copy(h, 2).wait_recv()
        hid_ref[2 * h:2 * h + 2] = hid_buf[h]

    for h in range(2):
        for n in range(4):
            for c in range(NCH):
                x_copy(n, h, c).wait_send()
        for hop in range(3):
            g_copy(h, hop).wait_send()
    for f in range(2):
        for d in range(1, 4):
            rs_copy(f, d).wait_send()
    for hop in range(3):
        st_copy(hop).wait_send()

    @pl.when(k < 3)
    def _():
        for layer in range(NUM_LAYERS):
            for which in range(2):
                row_copy(which, layer).wait_send()


def layer_call(sums0, parts1, step_emb, b_in, taps, gain, b_out, long_filt, state, w_in, w_out, w_up, w_down):
    vm = pl.BlockSpec(memory_space=pltpu.VMEM)
    hbm = pl.BlockSpec(memory_space=pltpu.HBM)
    dma = pltpu.SemaphoreType.DMA
    return pl.pallas_call(
        layer_kernel,
        out_shape=(
            jax.ShapeDtypeStruct((NUM_STEPS, SEQ, DIM), F32),
            jax.ShapeDtypeStruct((NUM_LAYERS, SEQ, 3, 2, CH), BF16),
            jax.ShapeDtypeStruct((2, NUM_LAYERS, SEQ, NUM_STEPS, CH), F32),
        ),
        in_specs=[vm] * 13 + [hbm] * 6,
        out_specs=[vm] * 3,
        scratch_shapes=[
            pltpu.VMEM(w_in.shape, BF16),
            pltpu.VMEM(w_out.shape, BF16),
            pltpu.VMEM(w_up.shape, BF16),
            pltpu.VMEM(w_down.shape, BF16),
            pltpu.VMEM((2, SEQ, DIM), F32),
            pltpu.VMEM((NUM_LAYERS, BLK, 3, 2, CH), BF16),
            pltpu.VMEM((NUM_LAYERS, 2, 8, CH), F32),
            pltpu.VMEM((3, 2, NUM_STEPS, BLK, CH), F32),
            pltpu.VMEM((SEQ, 3, 2, CH), F32),
            pltpu.VMEM((4, 2, NCH, 2 * BLK, CW), F32),
            pltpu.VMEM((4, 2, NCH, 2 * BLK, CW), F32),
            pltpu.VMEM((2, 2, SEQ, DIM), F32),
            pltpu.VMEM((SEQ, 3, 2, CH), F32),
            pltpu.VMEM((2, NUM_LAYERS, SEQ, NUM_STEPS, CH), F32),
            dma((NUM_LAYERS, 4)),
            dma((2,)),
            dma((2, 3)),
            dma((2, 3)),
            dma((4, 2, NCH)),
            dma((4, 2, NCH)),
            dma((3,)),
            dma((3,)),
            dma((2, NUM_LAYERS)),
            dma((2, NUM_LAYERS, 4)),
            dma((2, 3)),
            dma((2, 3)),
        ],
        compiler_params=pltpu.CompilerParams(collective_id=0, has_side_effects=True, vmem_limit_bytes=44 << 20),
        name="layers",
    )(*sums0, *parts1, step_emb, b_in, taps, gain, b_out, long_filt, state, w_in, w_out, w_up, w_down)


def put_kernel(hid_in, st_in, rows_ref, v_in, z_in, hid_out, st_out, v_out, z_out, wide, tile, sems, o_sem):
    copies = [pltpu.make_async_copy(hid_in, hid_out, o_sem.at[0]), pltpu.make_async_copy(st_in, st_out, o_sem.at[1])]
    for copy in copies:
        copy.start()

    @pl.when(lax.axis_index("sp") == 3)
    def _():
        row_copies = []
        for which, dst in enumerate((v_out, z_out)):
            for layer in range(NUM_LAYERS):
                wide[:, 4:8, :] = jnp.zeros((SEQ, 4, CH), F32)
                wide[:, 0:4, :] = rows_ref[which, layer]
                tile[which, layer] = wide[...].astype(BF16)
                copy = pltpu.make_async_copy(tile.at[which, layer], dst.at[layer, :, 0:8, :], sems.at[which, layer])
                copy.start()
                row_copies.append(copy)
        for copy in row_copies:
            copy.wait()

    for copy in copies:
        copy.wait()


def put_call(hidden, states, rows, v_new, z_new):
    hbm = pl.BlockSpec(memory_space=pltpu.HBM)
    vm = pl.BlockSpec(memory_space=pltpu.VMEM)
    return pl.pallas_call(
        put_kernel,
        out_shape=(jax.ShapeDtypeStruct(hidden.shape, F32), jax.ShapeDtypeStruct(states.shape, BF16),
                   jax.ShapeDtypeStruct(v_new.shape, BF16), jax.ShapeDtypeStruct(z_new.shape, BF16)),
        in_specs=[vm] * 3 + [hbm] * 2,
        out_specs=[hbm] * 4,
        scratch_shapes=[
            pltpu.VMEM((SEQ, 8, CH), F32),
            pltpu.VMEM((2, NUM_LAYERS, SEQ, 8, CH), BF16),
            pltpu.SemaphoreType.DMA((2, NUM_LAYERS)),
            pltpu.SemaphoreType.DMA((2,)),
        ],
        input_output_aliases={3: 2, 4: 3},
        compiler_params=pltpu.CompilerParams(vmem_limit_bytes=16 << 20),
        name="put_rows",
    )(hidden, states, rows, v_new, z_new)


def solution(mesh):
    def device_fn(step_emb, v_cache, z_cache, short_state, w_in, b_in, short_taps, long_filt, skip_gain, w_out, b_out, w_up, w_down):
        v_cache, z_cache, long_filt, w_in, w_out, w_up, w_down = [
            pltpu.with_memory_space_constraint(x, pltpu.HBM)
            for x in (v_cache, z_cache, long_filt, jnp.transpose(w_in, (0, 2, 1, 3)), w_out, w_up, w_down)]
        both = tuple((f, d, True) for f in range(2) for d in range(4))
        v_new, z_new, *parts0 = stream_call(0, both, v_cache, z_cache, long_filt)
        sums0 = [parts0[0]] + [lax.ppermute(parts0[d], "sp", [(i, (i + d) % 4) for i in range(4)]) for d in range(1, 4)]
        v_new, z_new, *parts1 = stream_call(1, both, v_cache, z_cache, long_filt, (v_new, z_new))
        hidden, states, rows = layer_call(
            sums0, parts1, step_emb, jnp.transpose(b_in, (1, 0, 2)), jnp.transpose(short_taps, (1, 2, 0, 3)),
            skip_gain, b_out, long_filt, jnp.transpose(short_state, (0, 1, 3, 2, 4)),
            w_in, w_out, w_up, w_down)
        hidden, states, v_new, z_new = put_call(hidden, states, rows, v_new, z_new)
        return hidden, v_new, z_new, jnp.transpose(states, (0, 1, 3, 2, 4))

    specs_in = (
        P(None, "dp", None),
        P(None, "dp", "sp", "tp"),
        P(None, "dp", "sp", "tp"),
        P(None, "dp", None, None, "tp"),
        P(None, None, None, "tp"),
        P(None, None, "tp"),
        P(None, None, None, "tp"),
        P(None, None, None, "tp"),
        P(None, None, "tp"),
        P(None, "tp", None),
        P(None, None),
        P(None, None, "tp"),
        P(None, "tp", None),
    )
    specs_out = (
        P(None, "dp", None),
        P(None, "dp", "sp", "tp"),
        P(None, "dp", "sp", "tp"),
        P(None, "dp", None, None, "tp"),
    )
    return jax.shard_map(device_fn, mesh=mesh, in_specs=specs_in, out_specs=specs_out, check_vma=False)
```

```python
import functools

import jax
import jax.numpy as jnp
from jax import lax
from jax.experimental import pallas as pl
from jax.experimental.pallas import tpu as pltpu
from jax.sharding import PartitionSpec as P

F32 = jnp.float32
BF16 = jnp.bfloat16
NUM_STEPS = 4
NUM_LAYERS = 2
SEQ = 32
BLK = 8
DIM = 1024
CH = 512
UP = 2048
SHARD = 256
NCH = 2
CW = DIM // NCH
SLOTS = 8
MESH = pl.DeviceIdType.MESH


def pair_rows(lo, hi, shift):
    clear = (lax.broadcasted_iota(jnp.int32, (8, 128), 0) // shift) % 2 == 0
    if shift == 4:
        return jnp.where(clear, lo, hi) + pltpu.roll(jnp.where(clear, hi, lo), 4, 0)
    return jnp.where(clear, lo + pltpu.roll(lo, 8 - shift, 0), hi + pltpu.roll(hi, shift, 0))


def fill_window(win, filt_rows, ct):
    flip = 7 - lax.broadcasted_iota(jnp.int32, (8, 128), 0)
    lanes = pl.ds(pl.multiple_of(ct * 128, 128), 128)
    for m in range(SHARD // 8 + 1):
        rows = filt_rows[SHARD - 8 * m:SHARD - 8 * m + 8, lanes]
        win[ct, 8 * m:8 * m + 8] = jnp.take_along_axis(rows, flip, axis=0)


def conv_block(src, win, dst, ready):
    @pl.loop(0, CH // 128)
    def _(ct):
        ready(ct)
        lanes = pl.ds(pl.multiple_of(ct * 128, 128), 128)
        half = []
        for seqs in ((0, 4, 1, 5), (2, 6, 3, 7)):
            accs = [[None] * NUM_STEPS for _ in seqs]
            for pt in range(SHARD // 16):
                w = [[win[ct, 16 * pt + 8 * h + 7 - j:16 * pt + 8 * h + 15 - j] for h in range(2)] for j in range(NUM_STEPS)]
                for i, b in enumerate(seqs):
                    x = src[b, 16 * pt:16 * pt + 16, lanes].astype(F32)
                    for j in range(NUM_STEPS):
                        for h in range(2):
                            term = x[8 * h:8 * h + 8] * w[j][h]
                            accs[i][j] = term if accs[i][j] is None else accs[i][j] + term
            half.append([[pair_rows(accs[0][j], accs[1][j], 4), pair_rows(accs[2][j], accs[3][j], 4)] for j in range(NUM_STEPS)])
        for j in range(NUM_STEPS):
            dst[j, :, lanes] = pair_rows(pair_rows(half[0][j][0], half[1][j][0], 2), pair_rows(half[0][j][1], half[1][j][1], 2), 1)


def stream_kernel(layer, units, num_in, *refs):
    num_conv = 1 + max(f for f, _, conv in units if conv)
    v_in, z_in, filt = refs[:3]
    v_out, z_out = refs[num_in:num_in + 2]
    parts = refs[num_in + 2:num_in + 6]
    ring, rows, win, in_sem, out_sem, filt_sem, lane_sem = refs[num_in + 6:]
    k = lax.axis_index("sp")
    first = pl.multiple_of(jnp.maximum(2 - k, 0) * SHARD, SHARD)

    def seqs(u):
        return pl.ds(pl.multiple_of(lax.rem(k + units[u][1], 4) * BLK, BLK), BLK)

    def in_copy(u):
        return pltpu.make_async_copy((v_in, z_in)[units[u][0]].at[layer, seqs(u)], ring.at[u], in_sem.at[u])

    def lane_copy(ct):
        lanes = pl.ds(pl.multiple_of(ct * 128, 128), 128)
        return pltpu.make_async_copy(
            (v_in, z_in)[units[0][0]].at[layer, seqs(0), :, lanes], ring.at[0, :, :, lanes], lane_sem.at[ct])

    def out_copy(u):
        return pltpu.make_async_copy(ring.at[u], (v_out, z_out)[units[u][0]].at[layer, seqs(u)], out_sem.at[u])

    filt_copies = [pltpu.make_async_copy(filt.at[layer, f, pl.ds(first, SHARD + 8)], rows.at[f], filt_sem.at[f])
                   for f in range(num_conv)]
    reads = {0: (2,), 1: (3, 4), 2: (5, 6), 3: (7,)}
    writes = {3: (0, 1), 4: (2, 3), 5: (4, 5), 6: (6,), 7: (7,)}
    filt_copies[0].start()
    for ct in range(CH // 128):
        lane_copy(ct).start()
    filt_copies[0].wait()
    in_copy(1).start()
    for u, (f, d, conv) in enumerate(units):
        if u > 0:
            in_copy(u).wait()
        for nxt in reads.get(u, ()):
            in_copy(nxt).start()
        for nxt in writes.get(u, ()):
            out_copy(nxt).start()
        if u == 1:
            for copy in filt_copies[1:]:
                copy.start()
        new_filter = d == 0 and conv
        if new_filter and u > 0:
            filt_copies[f].wait()

        def ready(ct, u=u, f=f, new_filter=new_filter):
            if new_filter:
                fill_window(win, rows.at[f], ct)
            if u == 0:
                lane_copy(ct).wait()

        if conv:
            conv_block(ring.at[u], win, parts[d].at[f], ready)
    for u in range(len(units)):
        out_copy(u).wait()


def stream_call(layer, units, v_cache, z_cache, long_filt, earlier=()):
    hbm = pl.BlockSpec(memory_space=pltpu.HBM)
    num_in = 3 + len(earlier)
    num_conv = 1 + max(f for f, _, conv in units if conv)
    part = jax.ShapeDtypeStruct((num_conv, NUM_STEPS, BLK, CH), F32)
    return pl.pallas_call(
        functools.partial(stream_kernel, layer, units, num_in),
        out_shape=(jax.ShapeDtypeStruct(v_cache.shape, BF16), jax.ShapeDtypeStruct(z_cache.shape, BF16)) + (part,) * 4,
        in_specs=[hbm] * num_in,
        out_specs=[hbm] * 2 + [pl.BlockSpec(memory_space=pltpu.VMEM)] * 4,
        scratch_shapes=[
            pltpu.VMEM((SLOTS, BLK, SHARD, CH), BF16),
            pltpu.VMEM((2, SHARD + 8, CH), F32),
            pltpu.VMEM((CH // 128, SHARD + 8, 128), F32),
            pltpu.SemaphoreType.DMA((len(units),)),
            pltpu.SemaphoreType.DMA((len(units),)),
            pltpu.SemaphoreType.DMA((2,)),
            pltpu.SemaphoreType.DMA((CH // 128,)),
        ],
        input_output_aliases={3: 0, 4: 1} if earlier else {},
        cost_estimate=pl.CostEstimate(flops=SEQ * SHARD * CH * 16, bytes_accessed=4 * SEQ * SHARD * CH * 2, transcendentals=0),
        compiler_params=pltpu.CompilerParams(vmem_limit_bytes=30 << 20),
        name=f"stream_{layer}",
    )(v_cache, z_cache, long_filt, *earlier)


def norm_rows(rows_in):
    mean_val = jnp.mean(rows_in, axis=-1, keepdims=True)
    centered = rows_in - mean_val
    var_val = jnp.mean(centered * centered, axis=-1, keepdims=True)
    return centered * lax.rsqrt(var_val + 1e-5)


def round_bf16(x):
    return x.astype(BF16).astype(F32)


def layer_kernel(*refs):
    sums0 = refs[:4]
    parts1 = refs[4:8]
    (emb_ref, b_in_ref, taps_ref, gain_ref, b_out_ref, filt_hbm, state_hbm, w_in_hbm, w_out_hbm, w_up_hbm, w_down_hbm,
     hid_ref, st_ref, rows_ref,
     w_in, w_out, w_up, w_down, emb32, state, lags, rs_buf, st0_buf, x_send, x_recv, hid_buf, st_buf, row_buf,
     w_sem, s_sem, rs_send, rs_recv, x_ssem, x_rsem, st_ssem, st_rsem, row_ssem, row_rsem, g_ssem, g_rsem) = refs[8:]
    k = lax.axis_index("sp")
    t = lax.axis_index("tp")
    others = [lax.rem(k + d, 4) for d in range(1, 4)]
    mate = k + 1 - 2 * lax.rem(k, 2)
    across = lax.rem(k + 2, 4)
    own = pl.ds(pl.multiple_of(k * BLK, BLK), BLK)

    small = [pltpu.make_async_copy(state_hbm.at[:, own], state, s_sem.at[0]),
             pltpu.make_async_copy(filt_hbm.at[:, :, 0:8], lags, s_sem.at[1])]
    for copy in small:
        copy.start()
    w_pairs = ((w_in_hbm, w_in), (w_out_hbm, w_out), (w_up_hbm, w_up), (w_down_hbm, w_down))
    w_copies = [pltpu.make_async_copy(src.at[layer], dst.at[layer], w_sem.at[layer, idx])
                for layer in range(NUM_LAYERS) for idx, (src, dst) in enumerate(w_pairs)]
    for copy in w_copies[:2]:
        copy.start()

    barrier = pltpu.get_barrier_semaphore()
    for dev in others:
        pl.semaphore_signal(barrier, inc=1, device_id={"sp": dev}, device_id_type=MESH)
    pl.semaphore_signal(barrier, inc=1, device_id={"tp": 1 - t}, device_id_type=MESH)
    pl.semaphore_wait(barrier, 4)

    def rs_copy(f, d):
        return pltpu.make_async_remote_copy(
            src_ref=parts1[d].at[f], dst_ref=rs_buf.at[d - 1, f], send_sem=rs_send.at[f, d - 1], recv_sem=rs_recv.at[f, d - 1],
            device_id={"sp": others[d - 1]}, device_id_type=MESH)

    def cached_sum(layer, f, j):
        if layer == 0:
            return (sums0[0][f, j] + sums0[1][f, j]) + (sums0[2][f, j] + sums0[3][f, j])
        return (parts1[0][f, j] + rs_buf[0, f, j]) + (rs_buf[1, f, j] + rs_buf[2, f, j])

    def x_copy(n, h, c):
        return pltpu.make_async_remote_copy(
            src_ref=x_send.at[n, h, c], dst_ref=x_recv.at[n, h, c], send_sem=x_ssem.at[n, h, c], recv_sem=x_rsem.at[n, h, c],
            device_id={"tp": 1 - t}, device_id_type=MESH)

    def row_copy(which, layer, src=None):
        piece = row_buf.at[which, layer, own if src is None else pl.ds(src * BLK, BLK)]
        return pltpu.make_async_remote_copy(
            src_ref=piece, dst_ref=piece, send_sem=row_ssem.at[which, layer],
            recv_sem=row_rsem.at[which, layer, k if src is None else src],
            device_id={"sp": 3}, device_id_type=MESH)

    def block_of(hop):
        return pl.ds(pl.multiple_of((k if hop < 2 else across) * BLK, BLK), BLK)

    def st_copy(hop):
        piece = st_buf.at[block_of(hop)]
        return pltpu.make_async_remote_copy(
            src_ref=piece, dst_ref=piece, send_sem=st_ssem.at[hop], recv_sem=st_rsem.at[hop],
            device_id={"sp": across if hop == 1 else mate}, device_id_type=MESH)

    def keep_rows(which, layer, vals):
        for b in range(BLK):
            for j in range(NUM_STEPS):
                row_buf[which, layer, k * BLK + b, j:j + 1, :] = vals[j][b:b + 1]

        @pl.when(k < 3)
        def _():
            row_copy(which, layer).start()

    def long_conv(layer, f, j, vals):
        acc = cached_sum(layer, f, j)
        for i in range(j + 1):
            acc = acc + lags[layer, f, j - i:j - i + 1] * vals[i]
        return acc + gain_ref[layer, f:f + 1] * vals[j]

    proj_rows = [[None] * 3 for _ in range(NUM_LAYERS)]
    v_rows = [[], []]
    z_rows = [[], []]

    def matmul_exchange(n, h, lhs, w_ref):
        for c in range(NCH):
            x_send[n, h, c] = jnp.dot(lhs, w_ref[:, c * CW:(c + 1) * CW], preferred_element_type=F32)
            x_copy(n, h, c).start()

    def add_exchange(n, h, base):
        outs = []
        for c in range(NCH):
            x_copy(n, h, c).wait_recv()
            outs.append(base[:, c * CW:(c + 1) * CW] + (x_send[n, h, c] + x_recv[n, h, c]))
        return jnp.concatenate(outs, axis=1)

    def front(layer, h, rows_in):
        normed = norm_rows(rows_in).astype(BF16)
        if h == 0:
            w_copies[layer * 4].wait()
            if layer == 0:
                w_copies[2].start()
        mixed = []
        for g in range(3):
            proj = jnp.dot(normed, w_in[layer, g], preferred_element_type=F32) + b_in_ref[g, layer:layer + 1]
            proj = round_bf16(proj)
            if h == 0:
                proj_rows[layer][g] = [
                    jnp.concatenate([state[layer, b, g, s:s + 1].astype(F32) for b in range(BLK)], axis=0) for s in range(2)]
            seq = proj_rows[layer][g]
            seq += [proj[BLK * i:BLK * i + BLK] for i in range(2)]
            tap = [taps_ref[i, g, layer:layer + 1] for i in range(3)]
            mixed.append([tap[0] * seq[j + 2] + tap[1] * seq[j + 1] + tap[2] * seq[j] for j in (2 * h, 2 * h + 1)])
        ys = []
        v_rows[layer] += [round_bf16(x) for x in mixed[2]]
        if layer == 1 and h == 0:
            for f in range(2):
                for d in range(1, 4):
                    rs_copy(f, d).wait_recv()
        for i in range(2):
            a = long_conv(layer, 0, 2 * h + i, v_rows[layer])
            z_rows[layer].append(round_bf16(mixed[0][i] * a))
            ys.append(mixed[1][i] * long_conv(layer, 1, 2 * h + i, z_rows[layer]))
        if h == 0:
            w_copies[layer * 4 + 1].wait()
        matmul_exchange(layer * 2, h, jnp.concatenate(ys, axis=0).astype(BF16), w_out.at[layer])

    def send_kept(layer):
        keep_rows(0, layer, v_rows[layer])
        keep_rows(1, layer, z_rows[layer])
    def middle(layer, h, rows_in):
        out = add_exchange(layer * 2, h, rows_in) + b_out_ref[layer:layer + 1]
        act = norm_rows(out).astype(BF16)
        if h == 0:
            w_copies[layer * 4 + 2].wait()
        inner = jax.nn.gelu(jnp.dot(act, w_up[layer], preferred_element_type=F32)).astype(BF16)
        if h == 0:
            w_copies[layer * 4 + 3].wait()
        matmul_exchange(layer * 2 + 1, h, inner, w_down.at[layer])
        return out

    for copy in small:
        copy.wait()
    rows_in = []
    for h in range(2):
        emb32[...] = emb_ref[2 * h:2 * h + 2].astype(F32)
        rows_in.append(jnp.concatenate([emb32[i, own] for i in range(2)], axis=0))
    front(0, 0, rows_in[0])
    w_copies[3].start()
    front(0, 1, rows_in[1])
    for copy in w_copies[4:6]:
        copy.start()
    for f in range(2):
        for d in range(1, 4):
            rs_copy(f, d).start()
    send_kept(0)
    outs = [middle(0, h, rows_in[h]) for h in range(2)]
    for copy in w_copies[6:8]:
        copy.start()

    normed = norm_rows(emb_ref[2:4].astype(F32).reshape(2 * SEQ, DIM)).astype(BF16)
    for g in range(3):
        proj = jnp.dot(normed, w_in[0, g], preferred_element_type=F32) + b_in_ref[g, 0:1]
        for s in range(2):
            for b in range(SEQ):
                st0_buf[b, g, s:s + 1, :] = proj[s * SEQ + b:s * SEQ + b + 1]
    st_ref[0] = st0_buf[...].astype(BF16)

    rows_in = []
    for h in range(2):
        rows_in.append(add_exchange(1, h, outs[h]))
        front(1, h, rows_in[h])
    for g in range(3):
        for s in range(2):
            for i in range(BLK):
                st_buf[k * BLK + i, g, s:s + 1, :] = proj_rows[1][g][4 + s][i:i + 1]
    st_copy(1).start()
    st_copy(0).start()
    send_kept(1)
    outs = [middle(1, h, rows_in[h]) for h in range(2)]
    st_copy(1).wait_recv()
    st_copy(2).start()

    def g_copy(h, hop):
        piece = hid_buf.at[h, :, block_of(hop)]
        return pltpu.make_async_remote_copy(
            src_ref=piece, dst_ref=piece, send_sem=g_ssem.at[h, hop], recv_sem=g_rsem.at[h, hop],
            device_id={"sp": across if hop == 1 else mate}, device_id_type=MESH)

    for h in range(2):
        done = add_exchange(3, h, outs[h])
        for i in range(2):
            hid_buf[h, i, own] = done[BLK * i:BLK * i + BLK]
        g_copy(h, 1).start()
        g_copy(h, 0).start()
    st_copy(0).wait_recv()
    st_copy(2).wait_recv()
    st_ref[1] = st_buf[...].astype(BF16)

    @pl.when(k == 3)
    def _():
        for layer in range(NUM_LAYERS):
            for which in range(2):
                for src in range(3):
                    row_copy(which, layer, src).wait_recv()
        rows_ref[...] = row_buf[...]

    for h in range(2):
        g_copy(h, 1).wait_recv()
        g_copy(h, 2).start()
    for h in range(2):
        g_copy(h, 0).wait_recv()
        g_copy(h, 2).wait_recv()
        hid_ref[2 * h:2 * h + 2] = hid_buf[h]

    for h in range(2):
        for n in range(4):
            for c in range(NCH):
                x_copy(n, h, c).wait_send()
        for hop in range(3):
            g_copy(h, hop).wait_send()
    for f in range(2):
        for d in range(1, 4):
            rs_copy(f, d).wait_send()
    for hop in range(3):
        st_copy(hop).wait_send()

    @pl.when(k < 3)
    def _():
        for layer in range(NUM_LAYERS):
            for which in range(2):
                row_copy(which, layer).wait_send()


def layer_call(sums0, parts1, step_emb, b_in, taps, gain, b_out, long_filt, state, w_in, w_out, w_up, w_down):
    vm = pl.BlockSpec(memory_space=pltpu.VMEM)
    hbm = pl.BlockSpec(memory_space=pltpu.HBM)
    dma = pltpu.SemaphoreType.DMA
    return pl.pallas_call(
        layer_kernel,
        out_shape=(
            jax.ShapeDtypeStruct((NUM_STEPS, SEQ, DIM), F32),
            jax.ShapeDtypeStruct((NUM_LAYERS, SEQ, 3, 2, CH), BF16),
            jax.ShapeDtypeStruct((2, NUM_LAYERS, SEQ, NUM_STEPS, CH), F32),
        ),
        in_specs=[vm] * 13 + [hbm] * 6,
        out_specs=[vm] * 3,
        scratch_shapes=[
            pltpu.VMEM(w_in.shape, BF16),
            pltpu.VMEM(w_out.shape, BF16),
            pltpu.VMEM(w_up.shape, BF16),
            pltpu.VMEM(w_down.shape, BF16),
            pltpu.VMEM((2, SEQ, DIM), F32),
            pltpu.VMEM((NUM_LAYERS, BLK, 3, 2, CH), BF16),
            pltpu.VMEM((NUM_LAYERS, 2, 8, CH), F32),
            pltpu.VMEM((3, 2, NUM_STEPS, BLK, CH), F32),
            pltpu.VMEM((SEQ, 3, 2, CH), F32),
            pltpu.VMEM((4, 2, NCH, 2 * BLK, CW), F32),
            pltpu.VMEM((4, 2, NCH, 2 * BLK, CW), F32),
            pltpu.VMEM((2, 2, SEQ, DIM), F32),
            pltpu.VMEM((SEQ, 3, 2, CH), F32),
            pltpu.VMEM((2, NUM_LAYERS, SEQ, NUM_STEPS, CH), F32),
            dma((NUM_LAYERS, 4)),
            dma((2,)),
            dma((2, 3)),
            dma((2, 3)),
            dma((4, 2, NCH)),
            dma((4, 2, NCH)),
            dma((3,)),
            dma((3,)),
            dma((2, NUM_LAYERS)),
            dma((2, NUM_LAYERS, 4)),
            dma((2, 3)),
            dma((2, 3)),
        ],
        compiler_params=pltpu.CompilerParams(collective_id=0, has_side_effects=True, vmem_limit_bytes=44 << 20),
        name="layers",
    )(*sums0, *parts1, step_emb, b_in, taps, gain, b_out, long_filt, state, w_in, w_out, w_up, w_down)


def put_kernel(hid_in, st_in, rows_ref, v_in, z_in, hid_out, st_out, v_out, z_out, wide, tile, sems, o_sem):
    copies = [pltpu.make_async_copy(hid_in, hid_out, o_sem.at[0]), pltpu.make_async_copy(st_in, st_out, o_sem.at[1])]
    for copy in copies:
        copy.start()

    @pl.when(lax.axis_index("sp") == 3)
    def _():
        row_copies = []
        for which, dst in enumerate((v_out, z_out)):
            for layer in range(NUM_LAYERS):
                wide[:, 4:8, :] = jnp.zeros((SEQ, 4, CH), F32)
                wide[:, 0:4, :] = rows_ref[which, layer]
                tile[which, layer] = wide[...].astype(BF16)
                copy = pltpu.make_async_copy(tile.at[which, layer], dst.at[layer, :, 0:8, :], sems.at[which, layer])
                copy.start()
                row_copies.append(copy)
        for copy in row_copies:
            copy.wait()

    for copy in copies:
        copy.wait()


def put_call(hidden, states, rows, v_new, z_new):
    hbm = pl.BlockSpec(memory_space=pltpu.HBM)
    vm = pl.BlockSpec(memory_space=pltpu.VMEM)
    return pl.pallas_call(
        put_kernel,
        out_shape=(jax.ShapeDtypeStruct(hidden.shape, F32), jax.ShapeDtypeStruct(states.shape, BF16),
                   jax.ShapeDtypeStruct(v_new.shape, BF16), jax.ShapeDtypeStruct(z_new.shape, BF16)),
        in_specs=[vm] * 3 + [hbm] * 2,
        out_specs=[hbm] * 4,
        scratch_shapes=[
            pltpu.VMEM((SEQ, 8, CH), F32),
            pltpu.VMEM((2, NUM_LAYERS, SEQ, 8, CH), BF16),
            pltpu.SemaphoreType.DMA((2, NUM_LAYERS)),
            pltpu.SemaphoreType.DMA((2,)),
        ],
        input_output_aliases={3: 2, 4: 3},
        compiler_params=pltpu.CompilerParams(vmem_limit_bytes=16 << 20),
        name="put_rows",
    )(hidden, states, rows, v_new, z_new)


def solution(mesh):
    def device_fn(step_emb, v_cache, z_cache, short_state, w_in, b_in, short_taps, long_filt, skip_gain, w_out, b_out, w_up, w_down):
        v_cache, z_cache, long_filt, w_in, w_out, w_up, w_down = [
            pltpu.with_memory_space_constraint(x, pltpu.HBM)
            for x in (v_cache, z_cache, long_filt, jnp.transpose(w_in, (0, 2, 1, 3)), w_out, w_up, w_down)]
        both = tuple((f, d, True) for f in range(2) for d in range(4))
        v_new, z_new, *parts0 = stream_call(0, both, v_cache, z_cache, long_filt)
        sums0 = [parts0[0]] + [lax.ppermute(parts0[d], "sp", [(i, (i + d) % 4) for i in range(4)]) for d in range(1, 4)]
        v_new, z_new, *parts1 = stream_call(1, both, v_cache, z_cache, long_filt, (v_new, z_new))
        hidden, states, rows = layer_call(
            sums0, parts1, step_emb, jnp.transpose(b_in, (1, 0, 2)), jnp.transpose(short_taps, (1, 2, 0, 3)),
            skip_gain, b_out, long_filt, jnp.transpose(short_state, (0, 1, 3, 2, 4)),
            w_in, w_out, w_up, w_down)
        hidden, states, v_new, z_new = put_call(hidden, states, rows, v_new, z_new)
        return hidden, v_new, z_new, jnp.transpose(states, (0, 1, 3, 2, 4))

    specs_in = (
        P(None, "dp", None),
        P(None, "dp", "sp", "tp"),
        P(None, "dp", "sp", "tp"),
        P(None, "dp", None, None, "tp"),
        P(None, None, None, "tp"),
        P(None, None, "tp"),
        P(None, None, None, "tp"),
        P(None, None, None, "tp"),
        P(None, None, "tp"),
        P(None, "tp", None),
        P(None, None),
        P(None, None, "tp"),
        P(None, "tp", None),
    )
    specs_out = (
        P(None, "dp", None),
        P(None, "dp", "sp", "tp"),
        P(None, "dp", "sp", "tp"),
        P(None, "dp", None, None, "tp"),
    )
    return jax.shard_map(device_fn, mesh=mesh, in_specs=specs_in, out_specs=specs_out, check_vma=False)
```

```python
import functools

import jax
import jax.numpy as jnp
from jax import lax
from jax.experimental import pallas as pl
from jax.experimental.pallas import tpu as pltpu
from jax.sharding import PartitionSpec as P

F32 = jnp.float32
BF16 = jnp.bfloat16
NUM_STEPS = 4
NUM_LAYERS = 2
SEQ = 32
BLK = 8
DIM = 1024
CH = 512
UP = 2048
SHARD = 256
NCH = 2
CW = DIM // NCH
SLOTS = 8
MESH = pl.DeviceIdType.MESH


def pair_rows(lo, hi, shift):
    clear = (lax.broadcasted_iota(jnp.int32, (8, 128), 0) // shift) % 2 == 0
    if shift == 4:
        return jnp.where(clear, lo, hi) + pltpu.roll(jnp.where(clear, hi, lo), 4, 0)
    return jnp.where(clear, lo + pltpu.roll(lo, 8 - shift, 0), hi + pltpu.roll(hi, shift, 0))


def fill_window(win, filt_rows, ct):
    flip = 7 - lax.broadcasted_iota(jnp.int32, (8, 128), 0)
    lanes = pl.ds(pl.multiple_of(ct * 128, 128), 128)
    for m in range(SHARD // 8 + 1):
        rows = filt_rows[SHARD - 8 * m:SHARD - 8 * m + 8, lanes]
        win[ct, 8 * m:8 * m + 8] = jnp.take_along_axis(rows, flip, axis=0)


def conv_block(src, win, dst, ready):
    @pl.loop(0, CH // 128)
    def _(ct):
        ready(ct)
        lanes = pl.ds(pl.multiple_of(ct * 128, 128), 128)
        half = []
        for seqs in ((0, 4, 1, 5), (2, 6, 3, 7)):
            accs = [[None] * NUM_STEPS for _ in seqs]
            for pt in range(SHARD // 16):
                w = [[win[ct, 16 * pt + 8 * h + 7 - j:16 * pt + 8 * h + 15 - j] for h in range(2)] for j in range(NUM_STEPS)]
                for i, b in enumerate(seqs):
                    x = src[b, 16 * pt:16 * pt + 16, lanes].astype(F32)
                    for j in range(NUM_STEPS):
                        for h in range(2):
                            term = x[8 * h:8 * h + 8] * w[j][h]
                            accs[i][j] = term if accs[i][j] is None else accs[i][j] + term
            half.append([[pair_rows(accs[0][j], accs[1][j], 4), pair_rows(accs[2][j], accs[3][j], 4)] for j in range(NUM_STEPS)])
        for j in range(NUM_STEPS):
            dst[j, :, lanes] = pair_rows(pair_rows(half[0][j][0], half[1][j][0], 2), pair_rows(half[0][j][1], half[1][j][1], 2), 1)


def stream_kernel(layer, units, num_in, *refs):
    num_conv = 1 + max(f for f, _, conv in units if conv)
    v_in, z_in, filt = refs[:3]
    v_out, z_out = refs[num_in:num_in + 2]
    parts = refs[num_in + 2:num_in + 6]
    if layer == 1:
        emb, w_in_hbm, state_hbm, b_in_ref, taps_ref = refs[5:10]
        mixed_ref, st0_ref = refs[num_in + 6:num_in + 8]
        emb_own, emb_last, w_in, state, st_rows, p_sem = refs[-6:]
    ring, rows, win, in_sem, out_sem, filt_sem, lane_sem = refs[num_in + (8 if layer == 1 else 6):][:7]
    k = lax.axis_index("sp")
    own = pl.ds(pl.multiple_of(k * BLK, BLK), BLK)

    def project_copies():
        return [pltpu.make_async_copy(src, dst, p_sem.at[i]) for i, (src, dst) in enumerate((
            (emb.at[:, own], emb_own), (emb.at[2:4], emb_last), (w_in_hbm.at[0], w_in), (state_hbm.at[0, own], state)))]

    def project():
        for copy in project_copies():
            copy.wait()
        own_rows = NUM_STEPS * BLK
        emb_rows = jnp.concatenate([emb_own[...].astype(F32).reshape(own_rows, DIM), emb_last[...].astype(F32).reshape(2 * SEQ, DIM)], axis=0)
        normed = norm_rows(emb_rows).astype(BF16)
        for g in range(3):
            proj = jnp.dot(normed, w_in[g], preferred_element_type=F32) + b_in_ref[g, 0:1]
            own_proj = round_bf16(proj[:own_rows])
            seq = [jnp.concatenate([state[b, g, s:s + 1].astype(F32) for b in range(BLK)], axis=0) for s in range(2)]
            seq += [own_proj[BLK * j:BLK * j + BLK] for j in range(NUM_STEPS)]
            for j in range(NUM_STEPS):
                mix = taps_ref[0, g, 0:1] * seq[j + 2] + taps_ref[1, g, 0:1] * seq[j + 1] + taps_ref[2, g, 0:1] * seq[j]
                mixed_ref[g, j] = round_bf16(mix) if g == 2 else mix
            for s in range(2):
                for b in range(SEQ):
                    row = own_rows + s * SEQ + b
                    st_rows[b, g, s:s + 1, :] = proj[row:row + 1]
        st0_ref[...] = st_rows[...].astype(BF16)
    first = pl.multiple_of(jnp.maximum(2 - k, 0) * SHARD, SHARD)

    def seqs(u):
        return pl.ds(pl.multiple_of(lax.rem(k + units[u][1], 4) * BLK, BLK), BLK)

    def in_copy(u):
        return pltpu.make_async_copy((v_in, z_in)[units[u][0]].at[layer, seqs(u)], ring.at[u], in_sem.at[u])

    def lane_copy(ct):
        lanes = pl.ds(pl.multiple_of(ct * 128, 128), 128)
        return pltpu.make_async_copy(
            (v_in, z_in)[units[0][0]].at[layer, seqs(0), :, lanes], ring.at[0, :, :, lanes], lane_sem.at[ct])

    def out_copy(u):
        return pltpu.make_async_copy(ring.at[u], (v_out, z_out)[units[u][0]].at[layer, seqs(u)], out_sem.at[u])

    filt_copies = [pltpu.make_async_copy(filt.at[layer, f, pl.ds(first, SHARD + 8)], rows.at[f], filt_sem.at[f])
                   for f in range(num_conv)]
    reads = {0: (2,), 1: (3, 4), 2: (5, 6), 3: (7,)}
    writes = {3: (0, 1), 4: (2, 3), 5: (4, 5), 6: (6, 7)}
    filt_copies[0].start()
    for ct in range(CH // 128):
        lane_copy(ct).start()
    filt_copies[0].wait()
    in_copy(1).start()
    for u, (f, d, conv) in enumerate(units):
        if 0 < u < 7:
            in_copy(u).wait()
        if u == 6:
            in_copy(7).wait()
        for nxt in reads.get(u, ()):
            in_copy(nxt).start()
        for nxt in writes.get(u, ()):
            out_copy(nxt).start()
        if u == 1:
            for copy in filt_copies[1:]:
                copy.start()
        new_filter = d == 0 and conv
        if new_filter and u > 0:
            filt_copies[f].wait()

        def ready(ct, u=u, f=f, new_filter=new_filter):
            if new_filter:
                fill_window(win, rows.at[f], ct)
            if u == 0:
                lane_copy(ct).wait()

        if conv:
            conv_block(ring.at[u], win, parts[d].at[f], ready)
        if layer == 1 and u == 2:
            for copy in project_copies():
                copy.start()
        if layer == 1 and u == 6:
            project()
    for u in range(len(units)):
        out_copy(u).wait()


def stream_call(layer, units, v_cache, z_cache, long_filt, earlier=()):
    hbm = pl.BlockSpec(memory_space=pltpu.HBM)
    vm = pl.BlockSpec(memory_space=pltpu.VMEM)
    num_in = 3 + len(earlier)
    more_out, more_scratch = (), []
    if layer == 1:
        more_out = (jax.ShapeDtypeStruct((3, NUM_STEPS, BLK, CH), F32), jax.ShapeDtypeStruct((SEQ, 3, 2, CH), BF16))
        more_scratch = [
            pltpu.VMEM((NUM_STEPS, BLK, DIM), BF16),
            pltpu.VMEM((2, SEQ, DIM), BF16),
            pltpu.VMEM((3, DIM, CH), BF16),
            pltpu.VMEM((BLK, 3, 2, CH), BF16),
            pltpu.VMEM((SEQ, 3, 2, CH), F32),
            pltpu.SemaphoreType.DMA((4,)),
        ]
    num_conv = 1 + max(f for f, _, conv in units if conv)
    part = jax.ShapeDtypeStruct((num_conv, NUM_STEPS, BLK, CH), F32)
    return pl.pallas_call(
        functools.partial(stream_kernel, layer, units, num_in),
        out_shape=(jax.ShapeDtypeStruct(v_cache.shape, BF16), jax.ShapeDtypeStruct(z_cache.shape, BF16)) + (part,) * 4 + more_out,
        in_specs=[hbm] * 8 + [vm] * 2 if layer == 1 else [hbm] * 3,
        out_specs=[hbm] * 2 + [vm] * (4 + len(more_out)),
        scratch_shapes=[
            pltpu.VMEM((SLOTS, BLK, SHARD, CH), BF16),
            pltpu.VMEM((2, SHARD + 8, CH), F32),
            pltpu.VMEM((CH // 128, SHARD + 8, 128), F32),
            pltpu.SemaphoreType.DMA((len(units),)),
            pltpu.SemaphoreType.DMA((len(units),)),
            pltpu.SemaphoreType.DMA((2,)),
            pltpu.SemaphoreType.DMA((CH // 128,)),
        ] + more_scratch,
        input_output_aliases={3: 0, 4: 1} if earlier else {},
        cost_estimate=pl.CostEstimate(flops=SEQ * SHARD * CH * 16, bytes_accessed=4 * SEQ * SHARD * CH * 2, transcendentals=0),
        compiler_params=pltpu.CompilerParams(vmem_limit_bytes=30 << 20),
        name=f"stream_{layer}",
    )(v_cache, z_cache, long_filt, *earlier)


def norm_rows(rows_in):
    mean_val = jnp.mean(rows_in, axis=-1, keepdims=True)
    centered = rows_in - mean_val
    var_val = jnp.mean(centered * centered, axis=-1, keepdims=True)
    return centered * lax.rsqrt(var_val + 1e-5)


def round_bf16(x):
    return x.astype(BF16).astype(F32)


def layer_kernel(*refs):
    sums0 = refs[:4]
    parts1 = refs[4:8]
    (mixed_ref, emb_ref, b_in_ref, taps_ref, gain_ref, b_out_ref, filt_hbm, state_hbm, w_in_hbm, w_out_hbm, w_up_hbm, w_down_hbm,
     hid_ref, st_ref, rows_ref,
     w_in, w_out, w_up, w_down, emb32, state, lags, rs_buf, x_send, x_recv, hid_buf, st_buf, row_buf,
     w_sem, s_sem, rs_send, rs_recv, x_ssem, x_rsem, st_ssem, st_rsem, row_ssem, row_rsem, g_ssem, g_rsem) = refs[8:]
    k = lax.axis_index("sp")
    t = lax.axis_index("tp")
    others = [lax.rem(k + d, 4) for d in range(1, 4)]
    mate = k + 1 - 2 * lax.rem(k, 2)
    across = lax.rem(k + 2, 4)
    own = pl.ds(pl.multiple_of(k * BLK, BLK), BLK)

    small = [pltpu.make_async_copy(state_hbm.at[1, own], state, s_sem.at[0]),
             pltpu.make_async_copy(filt_hbm.at[:, :, 0:8], lags, s_sem.at[1])]
    for copy in small:
        copy.start()
    w_pairs = ((w_in_hbm, w_in), (w_out_hbm, w_out), (w_up_hbm, w_up), (w_down_hbm, w_down))
    w_copies = [None if (layer, idx) == (0, 0) else
                pltpu.make_async_copy(src.at[layer], dst if idx == 0 else dst.at[layer], w_sem.at[layer, idx])
                for layer in range(NUM_LAYERS) for idx, (src, dst) in enumerate(w_pairs)]
    w_copies[1].start()
    w_copies[2].start()

    barrier = pltpu.get_barrier_semaphore()
    for dev in others:
        pl.semaphore_signal(barrier, inc=1, device_id={"sp": dev}, device_id_type=MESH)
    pl.semaphore_signal(barrier, inc=1, device_id={"tp": 1 - t}, device_id_type=MESH)
    pl.semaphore_wait(barrier, 4)

    def rs_copy(f, d):
        return pltpu.make_async_remote_copy(
            src_ref=parts1[d].at[f], dst_ref=rs_buf.at[d - 1, f], send_sem=rs_send.at[f, d - 1], recv_sem=rs_recv.at[f, d - 1],
            device_id={"sp": others[d - 1]}, device_id_type=MESH)

    def cached_sum(layer, f, j):
        if layer == 0:
            return (sums0[0][f, j] + sums0[1][f, j]) + (sums0[2][f, j] + sums0[3][f, j])
        return (parts1[0][f, j] + rs_buf[0, f, j]) + (rs_buf[1, f, j] + rs_buf[2, f, j])

    def x_copy(n, h, c):
        return pltpu.make_async_remote_copy(
            src_ref=x_send.at[n, h, c], dst_ref=x_recv.at[n, h, c], send_sem=x_ssem.at[n, h, c], recv_sem=x_rsem.at[n, h, c],
            device_id={"tp": 1 - t}, device_id_type=MESH)

    def row_copy(which, layer, src=None):
        piece = row_buf.at[which, layer, own if src is None else pl.ds(src * BLK, BLK)]
        return pltpu.make_async_remote_copy(
            src_ref=piece, dst_ref=piece, send_sem=row_ssem.at[which, layer],
            recv_sem=row_rsem.at[which, layer, k if src is None else src],
            device_id={"sp": 3}, device_id_type=MESH)

    def block_of(hop):
        return pl.ds(pl.multiple_of((k if hop < 2 else across) * BLK, BLK), BLK)

    def st_copy(hop):
        piece = st_buf.at[block_of(hop)]
        return pltpu.make_async_remote_copy(
            src_ref=piece, dst_ref=piece, send_sem=st_ssem.at[hop], recv_sem=st_rsem.at[hop],
            device_id={"sp": across if hop == 1 else mate}, device_id_type=MESH)

    def keep_rows(which, layer, vals):
        for b in range(BLK):
            for j in range(NUM_STEPS):
                row_buf[which, layer, k * BLK + b, j:j + 1, :] = vals[j][b:b + 1]

        @pl.when(k < 3)
        def _():
            row_copy(which, layer).start()

    def long_conv(layer, f, j, vals):
        acc = cached_sum(layer, f, j)
        for i in range(j + 1):
            acc = acc + lags[layer, f, j - i:j - i + 1] * vals[i]
        return acc + gain_ref[layer, f:f + 1] * vals[j]

    proj_rows = [None] * 3
    v_rows = [[], []]
    z_rows = [[], []]

    def matmul_exchange(n, h, lhs, w_ref):
        for c in range(NCH):
            x_send[n, h, c] = jnp.dot(lhs, w_ref[:, c * CW:(c + 1) * CW], preferred_element_type=F32)
            x_copy(n, h, c).start()

    def add_exchange(n, h, base):
        outs = []
        for c in range(NCH):
            x_copy(n, h, c).wait_recv()
            outs.append(base[:, c * CW:(c + 1) * CW] + (x_send[n, h, c] + x_recv[n, h, c]))
        return jnp.concatenate(outs, axis=1)

    def front(layer, h, rows_in):
        if layer == 0:
            mixed = [[mixed_ref[g, j] for j in (2 * h, 2 * h + 1)] for g in range(3)]
            v_rows[0] += mixed[2]
        else:
            normed = norm_rows(rows_in).astype(BF16)
            if h == 0:
                w_copies[4].wait()
            mixed = []
            for g in range(3):
                proj = round_bf16(jnp.dot(normed, w_in[g], preferred_element_type=F32) + b_in_ref[g, 1:2])
                if h == 0:
                    proj_rows[g] = [
                        jnp.concatenate([state[b, g, s:s + 1].astype(F32) for b in range(BLK)], axis=0) for s in range(2)]
                seq = proj_rows[g]
                seq += [proj[BLK * i:BLK * i + BLK] for i in range(2)]
                tap = [taps_ref[i, g, 1:2] for i in range(3)]
                mixed.append([tap[0] * seq[j + 2] + tap[1] * seq[j + 1] + tap[2] * seq[j] for j in (2 * h, 2 * h + 1)])
            v_rows[1] += [round_bf16(x) for x in mixed[2]]
        ys = []
        if layer == 1 and h == 0:
            for f in range(2):
                for d in range(1, 4):
                    rs_copy(f, d).wait_recv()
        for i in range(2):
            a = long_conv(layer, 0, 2 * h + i, v_rows[layer])
            z_rows[layer].append(round_bf16(mixed[0][i] * a))
            ys.append(mixed[1][i] * long_conv(layer, 1, 2 * h + i, z_rows[layer]))
        if h == 0:
            w_copies[layer * 4 + 1].wait()
        matmul_exchange(layer * 2, h, jnp.concatenate(ys, axis=0).astype(BF16), w_out.at[layer])

    def send_kept(layer):
        keep_rows(0, layer, v_rows[layer])
        keep_rows(1, layer, z_rows[layer])
    def middle(layer, h, rows_in):
        out = add_exchange(layer * 2, h, rows_in) + b_out_ref[layer:layer + 1]
        act = norm_rows(out).astype(BF16)
        if h == 0:
            w_copies[layer * 4 + 2].wait()
        inner = jax.nn.gelu(jnp.dot(act, w_up[layer], preferred_element_type=F32)).astype(BF16)
        if h == 0:
            w_copies[layer * 4 + 3].wait()
        matmul_exchange(layer * 2 + 1, h, inner, w_down.at[layer])
        return out

    for copy in small:
        copy.wait()
    rows_in = []
    for h in range(2):
        emb32[...] = emb_ref[2 * h:2 * h + 2].astype(F32)
        rows_in.append(jnp.concatenate([emb32[i, own] for i in range(2)], axis=0))
    front(0, 0, rows_in[0])
    w_copies[3].start()
    front(0, 1, rows_in[1])
    for copy in w_copies[4:6]:
        copy.start()
    for f in range(2):
        for d in range(1, 4):
            rs_copy(f, d).start()
    send_kept(0)
    outs = [middle(0, h, rows_in[h]) for h in range(2)]
    for copy in w_copies[6:8]:
        copy.start()

    rows_in = []
    for h in range(2):
        rows_in.append(add_exchange(1, h, outs[h]))
        front(1, h, rows_in[h])
    for g in range(3):
        for s in range(2):
            for i in range(BLK):
                st_buf[k * BLK + i, g, s:s + 1, :] = proj_rows[g][4 + s][i:i + 1]
    st_copy(1).start()
    st_copy(0).start()
    send_kept(1)
    outs = [middle(1, h, rows_in[h]) for h in range(2)]
    st_copy(1).wait_recv()
    st_copy(2).start()

    def g_copy(h, c, hop):
        piece = hid_buf.at[h, c, :, block_of(hop)]
        return pltpu.make_async_remote_copy(
            src_ref=piece, dst_ref=piece, send_sem=g_ssem.at[h, c, hop], recv_sem=g_rsem.at[h, c, hop],
            device_id={"sp": across if hop == 1 else mate}, device_id_type=MESH)

    chunks = [(h, c) for h in range(2) for c in range(NCH)]
    for h, c in chunks:
        x_copy(3, h, c).wait_recv()
        done = outs[h][:, c * CW:(c + 1) * CW] + (x_send[3, h, c] + x_recv[3, h, c])
        for i in range(2):
            hid_buf[h, c, i, own] = done[BLK * i:BLK * i + BLK]
        g_copy(h, c, 1).start()
        g_copy(h, c, 0).start()
    st_copy(0).wait_recv()
    st_copy(2).wait_recv()
    st_ref[...] = st_buf[...].astype(BF16)

    @pl.when(k == 3)
    def _():
        for layer in range(NUM_LAYERS):
            for which in range(2):
                for src in range(3):
                    row_copy(which, layer, src).wait_recv()
        rows_ref[...] = row_buf[...]

    for h, c in chunks:
        g_copy(h, c, 1).wait_recv()
        g_copy(h, c, 2).start()
    for h, c in chunks:
        g_copy(h, c, 0).wait_recv()
        g_copy(h, c, 2).wait_recv()
        hid_ref[2 * h:2 * h + 2, :, c * CW:(c + 1) * CW] = hid_buf[h, c]

    for h, c in chunks:
        for n in range(4):
            x_copy(n, h, c).wait_send()
        for hop in range(3):
            g_copy(h, c, hop).wait_send()
    for f in range(2):
        for d in range(1, 4):
            rs_copy(f, d).wait_send()
    for hop in range(3):
        st_copy(hop).wait_send()

    @pl.when(k < 3)
    def _():
        for layer in range(NUM_LAYERS):
            for which in range(2):
                row_copy(which, layer).wait_send()


def layer_call(sums0, parts1, mixed, step_emb, b_in, taps, gain, b_out, long_filt, state, w_in, w_out, w_up, w_down):
    vm = pl.BlockSpec(memory_space=pltpu.VMEM)
    hbm = pl.BlockSpec(memory_space=pltpu.HBM)
    dma = pltpu.SemaphoreType.DMA
    return pl.pallas_call(
        layer_kernel,
        out_shape=(
            jax.ShapeDtypeStruct((NUM_STEPS, SEQ, DIM), F32),
            jax.ShapeDtypeStruct((SEQ, 3, 2, CH), BF16),
            jax.ShapeDtypeStruct((2, NUM_LAYERS, SEQ, NUM_STEPS, CH), F32),
        ),
        in_specs=[vm] * 14 + [hbm] * 6,
        out_specs=[vm] * 3,
        scratch_shapes=[
            pltpu.VMEM(w_in.shape[1:], BF16),
            pltpu.VMEM(w_out.shape, BF16),
            pltpu.VMEM(w_up.shape, BF16),
            pltpu.VMEM(w_down.shape, BF16),
            pltpu.VMEM((2, SEQ, DIM), F32),
            pltpu.VMEM((BLK, 3, 2, CH), BF16),
            pltpu.VMEM((NUM_LAYERS, 2, 8, CH), F32),
            pltpu.VMEM((3, 2, NUM_STEPS, BLK, CH), F32),
            pltpu.VMEM((4, 2, NCH, 2 * BLK, CW), F32),
            pltpu.VMEM((4, 2, NCH, 2 * BLK, CW), F32),
            pltpu.VMEM((2, NCH, 2, SEQ, CW), F32),
            pltpu.VMEM((SEQ, 3, 2, CH), F32),
            pltpu.VMEM((2, NUM_LAYERS, SEQ, NUM_STEPS, CH), F32),
            dma((NUM_LAYERS, 4)),
            dma((2,)),
            dma((2, 3)),
            dma((2, 3)),
            dma((4, 2, NCH)),
            dma((4, 2, NCH)),
            dma((3,)),
            dma((3,)),
            dma((2, NUM_LAYERS)),
            dma((2, NUM_LAYERS, 4)),
            dma((2, NCH, 3)),
            dma((2, NCH, 3)),
        ],
        compiler_params=pltpu.CompilerParams(collective_id=0, has_side_effects=True, vmem_limit_bytes=44 << 20),
        name="layers",
    )(*sums0, *parts1, mixed, step_emb, b_in, taps, gain, b_out, long_filt, state, w_in, w_out, w_up, w_down)


def put_kernel(hid_in, st0_in, st1_in, rows_ref, v_in, z_in, hid_out, st_out, v_out, z_out, wide, tile, sems, o_sem):
    copies = [pltpu.make_async_copy(hid_in, hid_out, o_sem.at[0]), pltpu.make_async_copy(st0_in, st_out.at[0], o_sem.at[1]),
              pltpu.make_async_copy(st1_in, st_out.at[1], o_sem.at[2])]
    for copy in copies:
        copy.start()

    @pl.when(lax.axis_index("sp") == 3)
    def _():
        row_copies = []
        for which, dst in enumerate((v_out, z_out)):
            for layer in range(NUM_LAYERS):
                wide[:, 4:8, :] = jnp.zeros((SEQ, 4, CH), F32)
                wide[:, 0:4, :] = rows_ref[which, layer]
                tile[which, layer] = wide[...].astype(BF16)
                copy = pltpu.make_async_copy(tile.at[which, layer], dst.at[layer, :, 0:8, :], sems.at[which, layer])
                copy.start()
                row_copies.append(copy)
        for copy in row_copies:
            copy.wait()

    for copy in copies:
        copy.wait()


def put_call(hidden, st0, st1, rows, v_new, z_new):
    hbm = pl.BlockSpec(memory_space=pltpu.HBM)
    vm = pl.BlockSpec(memory_space=pltpu.VMEM)
    return pl.pallas_call(
        put_kernel,
        out_shape=(jax.ShapeDtypeStruct(hidden.shape, F32), jax.ShapeDtypeStruct((NUM_LAYERS,) + st0.shape, BF16),
                   jax.ShapeDtypeStruct(v_new.shape, BF16), jax.ShapeDtypeStruct(z_new.shape, BF16)),
        in_specs=[vm] * 4 + [hbm] * 2,
        out_specs=[hbm] * 4,
        scratch_shapes=[
            pltpu.VMEM((SEQ, 8, CH), F32),
            pltpu.VMEM((2, NUM_LAYERS, SEQ, 8, CH), BF16),
            pltpu.SemaphoreType.DMA((2, NUM_LAYERS)),
            pltpu.SemaphoreType.DMA((3,)),
        ],
        input_output_aliases={4: 2, 5: 3},
        compiler_params=pltpu.CompilerParams(vmem_limit_bytes=16 << 20),
        name="put_rows",
    )(hidden, st0, st1, rows, v_new, z_new)


def solution(mesh):
    def device_fn(step_emb, v_cache, z_cache, short_state, w_in, b_in, short_taps, long_filt, skip_gain, w_out, b_out, w_up, w_down):
        v_cache, z_cache, long_filt, w_in, w_out, w_up, w_down = [
            pltpu.with_memory_space_constraint(x, pltpu.HBM)
            for x in (v_cache, z_cache, long_filt, jnp.transpose(w_in, (0, 2, 1, 3)), w_out, w_up, w_down)]
        both = tuple((f, d, True) for f in range(2) for d in range(4))
        v_new, z_new, *parts0 = stream_call(0, both, v_cache, z_cache, long_filt)
        sums0 = [parts0[0]] + [lax.ppermute(parts0[d], "sp", [(i, (i + d) % 4) for i in range(4)]) for d in range(1, 4)]
        state = jnp.transpose(short_state, (0, 1, 3, 2, 4))
        b_in = jnp.transpose(b_in, (1, 0, 2))
        taps = jnp.transpose(short_taps, (1, 2, 0, 3))
        v_new, z_new, *parts1, mixed, st0 = stream_call(
            1, both, v_cache, z_cache, long_filt, (v_new, z_new, step_emb, w_in, state, b_in, taps))
        hidden, st1, rows = layer_call(
            sums0, parts1, mixed, step_emb, b_in, taps, skip_gain, b_out, long_filt, state, w_in, w_out, w_up, w_down)
        hidden, states, v_new, z_new = put_call(hidden, st0, st1, rows, v_new, z_new)
        return hidden, v_new, z_new, jnp.transpose(states, (0, 1, 3, 2, 4))

    specs_in = (
        P(None, "dp", None),
        P(None, "dp", "sp", "tp"),
        P(None, "dp", "sp", "tp"),
        P(None, "dp", None, None, "tp"),
        P(None, None, None, "tp"),
        P(None, None, "tp"),
        P(None, None, None, "tp"),
        P(None, None, None, "tp"),
        P(None, None, "tp"),
        P(None, "tp", None),
        P(None, None),
        P(None, None, "tp"),
        P(None, "tp", None),
    )
    specs_out = (
        P(None, "dp", None),
        P(None, "dp", "sp", "tp"),
        P(None, "dp", "sp", "tp"),
        P(None, "dp", None, None, "tp"),
    )
    return jax.shard_map(device_fn, mesh=mesh, in_specs=specs_in, out_specs=specs_out, check_vma=False)
```

```python
import functools

import jax
import jax.numpy as jnp
from jax import lax
from jax.experimental import pallas as pl
from jax.experimental.pallas import tpu as pltpu
from jax.sharding import PartitionSpec as P

F32 = jnp.float32
BF16 = jnp.bfloat16
NUM_STEPS = 4
NUM_LAYERS = 2
SEQ = 32
BLK = 8
DIM = 1024
CH = 512
UP = 2048
SHARD = 256
NCH = 2
CW = DIM // NCH
SLOTS = 8
MESH = pl.DeviceIdType.MESH


def pair_rows(lo, hi, shift):
    clear = (lax.broadcasted_iota(jnp.int32, (8, 128), 0) // shift) % 2 == 0
    if shift == 4:
        return jnp.where(clear, lo, hi) + pltpu.roll(jnp.where(clear, hi, lo), 4, 0)
    return jnp.where(clear, lo + pltpu.roll(lo, 8 - shift, 0), hi + pltpu.roll(hi, shift, 0))


def fill_window(win, filt_rows, ct):
    flip = 7 - lax.broadcasted_iota(jnp.int32, (8, 128), 0)
    lanes = pl.ds(pl.multiple_of(ct * 128, 128), 128)
    for m in range(SHARD // 8 + 1):
        rows = filt_rows[SHARD - 8 * m:SHARD - 8 * m + 8, lanes]
        win[ct, 8 * m:8 * m + 8] = jnp.take_along_axis(rows, flip, axis=0)


def conv_block(src, win, dst, ready):
    @pl.loop(0, CH // 128)
    def _(ct):
        ready(ct)
        lanes = pl.ds(pl.multiple_of(ct * 128, 128), 128)
        half = []
        for seqs in ((0, 4, 1, 5), (2, 6, 3, 7)):
            accs = [[None] * NUM_STEPS for _ in seqs]
            for pt in range(SHARD // 16):
                w = [[win[ct, 16 * pt + 8 * h + 7 - j:16 * pt + 8 * h + 15 - j] for h in range(2)] for j in range(NUM_STEPS)]
                for i, b in enumerate(seqs):
                    x = src[b, 16 * pt:16 * pt + 16, lanes].astype(F32)
                    for j in range(NUM_STEPS):
                        for h in range(2):
                            term = x[8 * h:8 * h + 8] * w[j][h]
                            accs[i][j] = term if accs[i][j] is None else accs[i][j] + term
            half.append([[pair_rows(accs[0][j], accs[1][j], 4), pair_rows(accs[2][j], accs[3][j], 4)] for j in range(NUM_STEPS)])
        for j in range(NUM_STEPS):
            dst[j, :, lanes] = pair_rows(pair_rows(half[0][j][0], half[1][j][0], 2), pair_rows(half[0][j][1], half[1][j][1], 2), 1)


def stream_kernel(layer, units, num_in, *refs):
    num_conv = 1 + max(f for f, _, conv in units if conv)
    v_in, z_in, filt = refs[:3]
    v_out, z_out = refs[num_in:num_in + 2]
    parts = refs[num_in + 2:num_in + 6]
    ring, rows, win, in_sem, out_sem, filt_sem, lane_sem = refs[num_in + 6:]
    k = lax.axis_index("sp")
    first = pl.multiple_of(jnp.maximum(2 - k, 0) * SHARD, SHARD)

    def seqs(u):
        return pl.ds(pl.multiple_of(lax.rem(k + units[u][1], 4) * BLK, BLK), BLK)

    def in_copy(u):
        return pltpu.make_async_copy((v_in, z_in)[units[u][0]].at[layer, seqs(u)], ring.at[u], in_sem.at[u])

    def lane_copy(ct):
        lanes = pl.ds(pl.multiple_of(ct * 128, 128), 128)
        return pltpu.make_async_copy(
            (v_in, z_in)[units[0][0]].at[layer, seqs(0), :, lanes], ring.at[0, :, :, lanes], lane_sem.at[ct])

    def out_copy(u):
        return pltpu.make_async_copy(ring.at[u], (v_out, z_out)[units[u][0]].at[layer, seqs(u)], out_sem.at[u])

    filt_copies = [pltpu.make_async_copy(filt.at[layer, f, pl.ds(first, SHARD + 8)], rows.at[f], filt_sem.at[f])
                   for f in range(num_conv)]
    reads = {0: (2,), 1: (3, 4), 2: (5, 6), 3: (7,)}
    writes = {3: (0, 1), 4: (2, 3), 5: (4, 5), 6: (6,), 7: (7,)}
    filt_copies[0].start()
    lane_copy(0).start()
    filt_copies[0].wait()
    for ct in range(1, CH // 128):
        lane_copy(ct).start()
    in_copy(1).start()
    for u, (f, d, conv) in enumerate(units):
        if u > 0:
            in_copy(u).wait()
        for nxt in reads.get(u, ()):
            in_copy(nxt).start()
        for nxt in writes.get(u, ()):
            out_copy(nxt).start()
        if u == 1:
            for copy in filt_copies[1:]:
                copy.start()
        new_filter = d == 0 and conv
        if new_filter and u > 0:
            filt_copies[f].wait()

        def ready(ct, u=u, f=f, new_filter=new_filter):
            if new_filter:
                fill_window(win, rows.at[f], ct)
            if u == 0:
                lane_copy(ct).wait()

        if conv:
            conv_block(ring.at[u], win, parts[d].at[f], ready)
    for u in range(len(units)):
        out_copy(u).wait()


def stream_call(layer, units, v_cache, z_cache, long_filt, earlier=()):
    hbm = pl.BlockSpec(memory_space=pltpu.HBM)
    num_in = 3 + len(earlier)
    num_conv = 1 + max(f for f, _, conv in units if conv)
    part = jax.ShapeDtypeStruct((num_conv, NUM_STEPS, BLK, CH), F32)
    return pl.pallas_call(
        functools.partial(stream_kernel, layer, units, num_in),
        out_shape=(jax.ShapeDtypeStruct(v_cache.shape, BF16), jax.ShapeDtypeStruct(z_cache.shape, BF16)) + (part,) * 4,
        in_specs=[hbm] * num_in,
        out_specs=[hbm] * 2 + [pl.BlockSpec(memory_space=pltpu.VMEM)] * 4,
        scratch_shapes=[
            pltpu.VMEM((SLOTS, BLK, SHARD, CH), BF16),
            pltpu.VMEM((2, SHARD + 8, CH), F32),
            pltpu.VMEM((CH // 128, SHARD + 8, 128), F32),
            pltpu.SemaphoreType.DMA((len(units),)),
            pltpu.SemaphoreType.DMA((len(units),)),
            pltpu.SemaphoreType.DMA((2,)),
            pltpu.SemaphoreType.DMA((CH // 128,)),
        ],
        input_output_aliases={3: 0, 4: 1} if earlier else {},
        cost_estimate=pl.CostEstimate(flops=SEQ * SHARD * CH * 16, bytes_accessed=4 * SEQ * SHARD * CH * 2, transcendentals=0),
        compiler_params=pltpu.CompilerParams(vmem_limit_bytes=30 << 20),
        name=f"stream_{layer}",
    )(v_cache, z_cache, long_filt, *earlier)


def norm_rows(rows_in):
    mean_val = jnp.mean(rows_in, axis=-1, keepdims=True)
    centered = rows_in - mean_val
    var_val = jnp.mean(centered * centered, axis=-1, keepdims=True)
    return centered * lax.rsqrt(var_val + 1e-5)


def round_bf16(x):
    return x.astype(BF16).astype(F32)


def layer_kernel(*refs):
    sums0 = refs[:4]
    parts1 = refs[4:8]
    (emb_ref, b_in_ref, taps_ref, gain_ref, b_out_ref, filt_hbm, state_hbm, w_in_hbm, w_out_hbm, w_up_hbm, w_down_hbm,
     hid_ref, st_ref, rows_ref,
     w_in, w_out, w_up, w_down, emb32, state, lags, rs_buf, st0_buf, x_send, x_recv, hid_buf, st_buf, row_buf,
     w_sem, s_sem, rs_send, rs_recv, x_ssem, x_rsem, st_ssem, st_rsem, row_ssem, row_rsem, g_ssem, g_rsem) = refs[8:]
    k = lax.axis_index("sp")
    t = lax.axis_index("tp")
    others = [lax.rem(k + d, 4) for d in range(1, 4)]
    mate = k + 1 - 2 * lax.rem(k, 2)
    across = lax.rem(k + 2, 4)
    own = pl.ds(pl.multiple_of(k * BLK, BLK), BLK)

    small = [pltpu.make_async_copy(state_hbm.at[:, own], state, s_sem.at[0]),
             pltpu.make_async_copy(filt_hbm.at[:, :, 0:8], lags, s_sem.at[1])]
    for copy in small:
        copy.start()
    w_pairs = ((w_in_hbm, w_in), (w_out_hbm, w_out), (w_up_hbm, w_up), (w_down_hbm, w_down))
    w_copies = [pltpu.make_async_copy(src.at[layer], dst.at[layer], w_sem.at[layer, idx])
                for layer in range(NUM_LAYERS) for idx, (src, dst) in enumerate(w_pairs)]
    for copy in w_copies[:2]:
        copy.start()

    barrier = pltpu.get_barrier_semaphore()
    for dev in others:
        pl.semaphore_signal(barrier, inc=1, device_id={"sp": dev}, device_id_type=MESH)
    pl.semaphore_signal(barrier, inc=1, device_id={"tp": 1 - t}, device_id_type=MESH)
    pl.semaphore_wait(barrier, 4)

    def rs_copy(f, d):
        return pltpu.make_async_remote_copy(
            src_ref=parts1[d].at[f], dst_ref=rs_buf.at[d - 1, f], send_sem=rs_send.at[f, d - 1], recv_sem=rs_recv.at[f, d - 1],
            device_id={"sp": others[d - 1]}, device_id_type=MESH)

    def cached_sum(layer, f, j):
        if layer == 0:
            return (sums0[0][f, j] + sums0[1][f, j]) + (sums0[2][f, j] + sums0[3][f, j])
        return (parts1[0][f, j] + rs_buf[0, f, j]) + (rs_buf[1, f, j] + rs_buf[2, f, j])

    def x_copy(n, h, c):
        return pltpu.make_async_remote_copy(
            src_ref=x_send.at[n, h, c], dst_ref=x_recv.at[n, h, c], send_sem=x_ssem.at[n, h, c], recv_sem=x_rsem.at[n, h, c],
            device_id={"tp": 1 - t}, device_id_type=MESH)

    def row_copy(which, layer, src=None):
        piece = row_buf.at[which, layer, own if src is None else pl.ds(src * BLK, BLK)]
        return pltpu.make_async_remote_copy(
            src_ref=piece, dst_ref=piece, send_sem=row_ssem.at[which, layer],
            recv_sem=row_rsem.at[which, layer, k if src is None else src],
            device_id={"sp": 3}, device_id_type=MESH)

    def block_of(hop):
        return pl.ds(pl.multiple_of((k if hop < 2 else across) * BLK, BLK), BLK)

    def st_copy(hop):
        piece = st_buf.at[block_of(hop)]
        return pltpu.make_async_remote_copy(
            src_ref=piece, dst_ref=piece, send_sem=st_ssem.at[hop], recv_sem=st_rsem.at[hop],
            device_id={"sp": across if hop == 1 else mate}, device_id_type=MESH)

    def keep_rows(which, layer, vals):
        for b in range(BLK):
            for j in range(NUM_STEPS):
                row_buf[which, layer, k * BLK + b, j:j + 1, :] = vals[j][b:b + 1]

        @pl.when(k < 3)
        def _():
            row_copy(which, layer).start()

    def long_conv(layer, f, j, vals):
        acc = cached_sum(layer, f, j)
        for i in range(j + 1):
            acc = acc + lags[layer, f, j - i:j - i + 1] * vals[i]
        return acc + gain_ref[layer, f:f + 1] * vals[j]

    proj_rows = [[None] * 3 for _ in range(NUM_LAYERS)]
    v_rows = [[], []]
    z_rows = [[], []]

    def matmul_exchange(n, h, lhs, w_ref):
        for c in range(NCH):
            x_send[n, h, c] = jnp.dot(lhs, w_ref[:, c * CW:(c + 1) * CW], preferred_element_type=F32)
            x_copy(n, h, c).start()

    def add_exchange(n, h, base):
        outs = []
        for c in range(NCH):
            x_copy(n, h, c).wait_recv()
            outs.append(base[:, c * CW:(c + 1) * CW] + (x_send[n, h, c] + x_recv[n, h, c]))
        return jnp.concatenate(outs, axis=1)

    def front(layer, h, rows_in):
        normed = norm_rows(rows_in).astype(BF16)
        if h == 0:
            w_copies[layer * 4].wait()
            if layer == 0:
                w_copies[2].start()
        mixed = []
        for g in range(3):
            proj = jnp.dot(normed, w_in[layer, g], preferred_element_type=F32) + b_in_ref[g, layer:layer + 1]
            proj = round_bf16(proj)
            if h == 0:
                proj_rows[layer][g] = [
                    jnp.concatenate([state[layer, b, g, s:s + 1].astype(F32) for b in range(BLK)], axis=0) for s in range(2)]
            seq = proj_rows[layer][g]
            seq += [proj[BLK * i:BLK * i + BLK] for i in range(2)]
            tap = [taps_ref[i, g, layer:layer + 1] for i in range(3)]
            mixed.append([tap[0] * seq[j + 2] + tap[1] * seq[j + 1] + tap[2] * seq[j] for j in (2 * h, 2 * h + 1)])
        ys = []
        v_rows[layer] += [round_bf16(x) for x in mixed[2]]
        if layer == 1 and h == 0:
            for f in range(2):
                for d in range(1, 4):
                    rs_copy(f, d).wait_recv()
        for i in range(2):
            a = long_conv(layer, 0, 2 * h + i, v_rows[layer])
            z_rows[layer].append(round_bf16(mixed[0][i] * a))
            ys.append(mixed[1][i] * long_conv(layer, 1, 2 * h + i, z_rows[layer]))
        if h == 0:
            w_copies[layer * 4 + 1].wait()
        matmul_exchange(layer * 2, h, jnp.concatenate(ys, axis=0).astype(BF16), w_out.at[layer])

    def send_kept(layer):
        keep_rows(0, layer, v_rows[layer])
        keep_rows(1, layer, z_rows[layer])
    def middle(layer, h, rows_in):
        out = add_exchange(layer * 2, h, rows_in) + b_out_ref[layer:layer + 1]
        act = norm_rows(out).astype(BF16)
        if h == 0:
            w_copies[layer * 4 + 2].wait()
        inner = jax.nn.gelu(jnp.dot(act, w_up[layer], preferred_element_type=F32)).astype(BF16)
        if h == 0:
            w_copies[layer * 4 + 3].wait()
        matmul_exchange(layer * 2 + 1, h, inner, w_down.at[layer])
        return out

    for copy in small:
        copy.wait()
    rows_in = []
    for h in range(2):
        emb32[...] = emb_ref[2 * h:2 * h + 2].astype(F32)
        rows_in.append(jnp.concatenate([emb32[i, own] for i in range(2)], axis=0))
    front(0, 0, rows_in[0])
    w_copies[3].start()
    front(0, 1, rows_in[1])
    for copy in w_copies[4:6]:
        copy.start()
    for f in range(2):
        for d in range(1, 4):
            rs_copy(f, d).start()
    send_kept(0)
    outs = [middle(0, h, rows_in[h]) for h in range(2)]
    for copy in w_copies[6:8]:
        copy.start()

    normed = norm_rows(emb_ref[2:4].astype(F32).reshape(2 * SEQ, DIM)).astype(BF16)
    for g in range(3):
        proj = jnp.dot(normed, w_in[0, g], preferred_element_type=F32) + b_in_ref[g, 0:1]
        for s in range(2):
            for b in range(SEQ):
                st0_buf[b, g, s:s + 1, :] = proj[s * SEQ + b:s * SEQ + b + 1]
    st_ref[0] = st0_buf[...].astype(BF16)

    rows_in = []
    for h in range(2):
        rows_in.append(add_exchange(1, h, outs[h]))
        front(1, h, rows_in[h])
    for g in range(3):
        for s in range(2):
            for i in range(BLK):
                st_buf[k * BLK + i, g, s:s + 1, :] = proj_rows[1][g][4 + s][i:i + 1]
    st_copy(1).start()
    st_copy(0).start()
    send_kept(1)
    outs = [middle(1, h, rows_in[h]) for h in range(2)]
    st_copy(1).wait_recv()
    st_copy(2).start()

    def g_copy(h, c, hop):
        piece = hid_buf.at[h, c, :, block_of(hop)]
        return pltpu.make_async_remote_copy(
            src_ref=piece, dst_ref=piece, send_sem=g_ssem.at[h, c, hop], recv_sem=g_rsem.at[h, c, hop],
            device_id={"sp": across if hop == 1 else mate}, device_id_type=MESH)

    chunks = [(h, c) for h in range(2) for c in range(NCH)]
    for h, c in chunks:
        x_copy(3, h, c).wait_recv()
        done = outs[h][:, c * CW:(c + 1) * CW] + (x_send[3, h, c] + x_recv[3, h, c])
        for i in range(2):
            hid_buf[h, c, i, own] = done[BLK * i:BLK * i + BLK]
        g_copy(h, c, 1).start()
        g_copy(h, c, 0).start()
    st_copy(0).wait_recv()
    st_copy(2).wait_recv()
    st_ref[1] = st_buf[...].astype(BF16)

    @pl.when(k == 3)
    def _():
        for layer in range(NUM_LAYERS):
            for which in range(2):
                for src in range(3):
                    row_copy(which, layer, src).wait_recv()
        rows_ref[...] = row_buf[...]

    for h, c in chunks:
        g_copy(h, c, 1).wait_recv()
        g_copy(h, c, 2).start()
    for h, c in chunks:
        g_copy(h, c, 0).wait_recv()
        g_copy(h, c, 2).wait_recv()
        hid_ref[2 * h:2 * h + 2, :, c * CW:(c + 1) * CW] = hid_buf[h, c]

    for h, c in chunks:
        for n in range(4):
            x_copy(n, h, c).wait_send()
        for hop in range(3):
            g_copy(h, c, hop).wait_send()
    for f in range(2):
        for d in range(1, 4):
            rs_copy(f, d).wait_send()
    for hop in range(3):
        st_copy(hop).wait_send()

    @pl.when(k < 3)
    def _():
        for layer in range(NUM_LAYERS):
            for which in range(2):
                row_copy(which, layer).wait_send()


def layer_call(sums0, parts1, step_emb, b_in, taps, gain, b_out, long_filt, state, w_in, w_out, w_up, w_down):
    vm = pl.BlockSpec(memory_space=pltpu.VMEM)
    hbm = pl.BlockSpec(memory_space=pltpu.HBM)
    dma = pltpu.SemaphoreType.DMA
    return pl.pallas_call(
        layer_kernel,
        out_shape=(
            jax.ShapeDtypeStruct((NUM_STEPS, SEQ, DIM), F32),
            jax.ShapeDtypeStruct((NUM_LAYERS, SEQ, 3, 2, CH), BF16),
            jax.ShapeDtypeStruct((2, NUM_LAYERS, SEQ, NUM_STEPS, CH), F32),
        ),
        in_specs=[vm] * 13 + [hbm] * 6,
        out_specs=[vm] * 3,
        scratch_shapes=[
            pltpu.VMEM(w_in.shape, BF16),
            pltpu.VMEM(w_out.shape, BF16),
            pltpu.VMEM(w_up.shape, BF16),
            pltpu.VMEM(w_down.shape, BF16),
            pltpu.VMEM((2, SEQ, DIM), F32),
            pltpu.VMEM((NUM_LAYERS, BLK, 3, 2, CH), BF16),
            pltpu.VMEM((NUM_LAYERS, 2, 8, CH), F32),
            pltpu.VMEM((3, 2, NUM_STEPS, BLK, CH), F32),
            pltpu.VMEM((SEQ, 3, 2, CH), F32),
            pltpu.VMEM((4, 2, NCH, 2 * BLK, CW), F32),
            pltpu.VMEM((4, 2, NCH, 2 * BLK, CW), F32),
            pltpu.VMEM((2, NCH, 2, SEQ, CW), F32),
            pltpu.VMEM((SEQ, 3, 2, CH), F32),
            pltpu.VMEM((2, NUM_LAYERS, SEQ, NUM_STEPS, CH), F32),
            dma((NUM_LAYERS, 4)),
            dma((2,)),
            dma((2, 3)),
            dma((2, 3)),
            dma((4, 2, NCH)),
            dma((4, 2, NCH)),
            dma((3,)),
            dma((3,)),
            dma((2, NUM_LAYERS)),
            dma((2, NUM_LAYERS, 4)),
            dma((2, NCH, 3)),
            dma((2, NCH, 3)),
        ],
        compiler_params=pltpu.CompilerParams(collective_id=0, has_side_effects=True, vmem_limit_bytes=44 << 20),
        name="layers",
    )(*sums0, *parts1, step_emb, b_in, taps, gain, b_out, long_filt, state, w_in, w_out, w_up, w_down)


def put_kernel(hid_in, st_in, rows_ref, v_in, z_in, hid_out, st_out, v_out, z_out, wide, tile, sems, o_sem):
    copies = [pltpu.make_async_copy(hid_in, hid_out, o_sem.at[0]), pltpu.make_async_copy(st_in, st_out, o_sem.at[1])]
    for copy in copies:
        copy.start()

    @pl.when(lax.axis_index("sp") == 3)
    def _():
        row_copies = []
        for which, dst in enumerate((v_out, z_out)):
            for layer in range(NUM_LAYERS):
                wide[:, 4:8, :] = jnp.zeros((SEQ, 4, CH), F32)
                wide[:, 0:4, :] = rows_ref[which, layer]
                tile[which, layer] = wide[...].astype(BF16)
                copy = pltpu.make_async_copy(tile.at[which, layer], dst.at[layer, :, 0:8, :], sems.at[which, layer])
                copy.start()
                row_copies.append(copy)
        for copy in row_copies:
            copy.wait()

    for copy in copies:
        copy.wait()


def put_call(hidden, states, rows, v_new, z_new):
    hbm = pl.BlockSpec(memory_space=pltpu.HBM)
    vm = pl.BlockSpec(memory_space=pltpu.VMEM)
    return pl.pallas_call(
        put_kernel,
        out_shape=(jax.ShapeDtypeStruct(hidden.shape, F32), jax.ShapeDtypeStruct(states.shape, BF16),
                   jax.ShapeDtypeStruct(v_new.shape, BF16), jax.ShapeDtypeStruct(z_new.shape, BF16)),
        in_specs=[vm] * 3 + [hbm] * 2,
        out_specs=[hbm] * 4,
        scratch_shapes=[
            pltpu.VMEM((SEQ, 8, CH), F32),
            pltpu.VMEM((2, NUM_LAYERS, SEQ, 8, CH), BF16),
            pltpu.SemaphoreType.DMA((2, NUM_LAYERS)),
            pltpu.SemaphoreType.DMA((2,)),
        ],
        input_output_aliases={3: 2, 4: 3},
        compiler_params=pltpu.CompilerParams(vmem_limit_bytes=16 << 20),
        name="put_rows",
    )(hidden, states, rows, v_new, z_new)


def solution(mesh):
    def device_fn(step_emb, v_cache, z_cache, short_state, w_in, b_in, short_taps, long_filt, skip_gain, w_out, b_out, w_up, w_down):
        v_cache, z_cache, long_filt, w_in, w_out, w_up, w_down = [
            pltpu.with_memory_space_constraint(x, pltpu.HBM)
            for x in (v_cache, z_cache, long_filt, jnp.transpose(w_in, (0, 2, 1, 3)), w_out, w_up, w_down)]
        both = tuple((f, d, True) for f in range(2) for d in range(4))
        v_new, z_new, *parts0 = stream_call(0, both, v_cache, z_cache, long_filt)
        sums0 = [parts0[0]] + [lax.ppermute(parts0[d], "sp", [(i, (i + d) % 4) for i in range(4)]) for d in range(1, 4)]
        v_new, z_new, *parts1 = stream_call(1, both, v_cache, z_cache, long_filt, (v_new, z_new))
        hidden, states, rows = layer_call(
            sums0, parts1, step_emb, jnp.transpose(b_in, (1, 0, 2)), jnp.transpose(short_taps, (1, 2, 0, 3)),
            skip_gain, b_out, long_filt, jnp.transpose(short_state, (0, 1, 3, 2, 4)),
            w_in, w_out, w_up, w_down)
        hidden, states, v_new, z_new = put_call(hidden, states, rows, v_new, z_new)
        return hidden, v_new, z_new, jnp.transpose(states, (0, 1, 3, 2, 4))

    specs_in = (
        P(None, "dp", None),
        P(None, "dp", "sp", "tp"),
        P(None, "dp", "sp", "tp"),
        P(None, "dp", None, None, "tp"),
        P(None, None, None, "tp"),
        P(None, None, "tp"),
        P(None, None, None, "tp"),
        P(None, None, None, "tp"),
        P(None, None, "tp"),
        P(None, "tp", None),
        P(None, None),
        P(None, None, "tp"),
        P(None, "tp", None),
    )
    specs_out = (
        P(None, "dp", None),
        P(None, "dp", "sp", "tp"),
        P(None, "dp", "sp", "tp"),
        P(None, "dp", None, None, "tp"),
    )
    return jax.shard_map(device_fn, mesh=mesh, in_specs=specs_in, out_specs=specs_out, check_vma=False)
```

```python
import functools

import jax
import jax.numpy as jnp
from jax import lax
from jax.experimental import pallas as pl
from jax.experimental.pallas import tpu as pltpu
from jax.sharding import PartitionSpec as P

F32 = jnp.float32
BF16 = jnp.bfloat16
NUM_STEPS = 4
NUM_LAYERS = 2
SEQ = 32
BLK = 8
DIM = 1024
CH = 512
UP = 2048
SHARD = 256
NCH = 4
CW = DIM // NCH
SLOTS = 8
GROUPS = 1
GSTEPS = NUM_STEPS // GROUPS
MESH = pl.DeviceIdType.MESH


def pair_rows(lo, hi, shift):
    clear = (lax.broadcasted_iota(jnp.int32, (8, 128), 0) // shift) % 2 == 0
    if shift == 4:
        return jnp.where(clear, lo, hi) + pltpu.roll(jnp.where(clear, hi, lo), 4, 0)
    return jnp.where(clear, lo + pltpu.roll(lo, 8 - shift, 0), hi + pltpu.roll(hi, shift, 0))


def fill_window(win, filt_rows, ct):
    flip = 7 - lax.broadcasted_iota(jnp.int32, (8, 128), 0)
    lanes = pl.ds(pl.multiple_of(ct * 128, 128), 128)
    for m in range(SHARD // 8 + 1):
        rows = filt_rows[SHARD - 8 * m:SHARD - 8 * m + 8, lanes]
        win[ct, 8 * m:8 * m + 8] = jnp.take_along_axis(rows, flip, axis=0)


def conv_block(src, win, dst, ready):
    @pl.loop(0, CH // 128)
    def _(ct):
        ready(ct)
        lanes = pl.ds(pl.multiple_of(ct * 128, 128), 128)
        half = []
        for seqs in ((0, 4, 1, 5), (2, 6, 3, 7)):
            accs = [[None] * NUM_STEPS for _ in seqs]
            for pt in range(SHARD // 16):
                w = [[win[ct, 16 * pt + 8 * h + 7 - j:16 * pt + 8 * h + 15 - j] for h in range(2)] for j in range(NUM_STEPS)]
                for i, b in enumerate(seqs):
                    x = src[b, 16 * pt:16 * pt + 16, lanes].astype(F32)
                    for j in range(NUM_STEPS):
                        for h in range(2):
                            term = x[8 * h:8 * h + 8] * w[j][h]
                            accs[i][j] = term if accs[i][j] is None else accs[i][j] + term
            half.append([[pair_rows(accs[0][j], accs[1][j], 4), pair_rows(accs[2][j], accs[3][j], 4)] for j in range(NUM_STEPS)])
        for j in range(NUM_STEPS):
            dst[j, :, lanes] = pair_rows(pair_rows(half[0][j][0], half[1][j][0], 2), pair_rows(half[0][j][1], half[1][j][1], 2), 1)


def stream_kernel(layer, units, num_in, *refs):
    num_conv = 1 + max(f for f, _, conv in units if conv)
    v_in, z_in, filt = refs[:3]
    v_out, z_out = refs[num_in:num_in + 2]
    parts = refs[num_in + 2:num_in + 6]
    ring, rows, win, in_sem, out_sem, filt_sem, lane_sem = refs[num_in + 6:]
    k = lax.axis_index("sp")
    first = pl.multiple_of(jnp.maximum(2 - k, 0) * SHARD, SHARD)

    def seqs(u):
        return pl.ds(pl.multiple_of(lax.rem(k + units[u][1], 4) * BLK, BLK), BLK)

    def in_copy(u):
        return pltpu.make_async_copy((v_in, z_in)[units[u][0]].at[layer, seqs(u)], ring.at[u], in_sem.at[u])

    def lane_copy(ct):
        lanes = pl.ds(pl.multiple_of(ct * 128, 128), 128)
        return pltpu.make_async_copy(
            (v_in, z_in)[units[0][0]].at[layer, seqs(0), :, lanes], ring.at[0, :, :, lanes], lane_sem.at[ct])

    def out_copy(u):
        return pltpu.make_async_copy(ring.at[u], (v_out, z_out)[units[u][0]].at[layer, seqs(u)], out_sem.at[u])

    filt_copies = [pltpu.make_async_copy(filt.at[layer, f, pl.ds(first, SHARD + 8)], rows.at[f], filt_sem.at[f])
                   for f in range(num_conv)]
    reads = {0: (2,), 1: (3, 4), 2: (5, 6), 3: (7,)}
    writes = {3: (0, 1), 4: (2, 3), 5: (4, 5), 6: (6,), 7: (7,)}
    filt_copies[0].start()
    lane_copy(0).start()
    filt_copies[0].wait()
    for ct in range(1, CH // 128):
        lane_copy(ct).start()
    in_copy(1).start()
    for u, (f, d, conv) in enumerate(units):
        if u > 0:
            in_copy(u).wait()
        for nxt in reads.get(u, ()):
            in_copy(nxt).start()
        for nxt in writes.get(u, ()):
            out_copy(nxt).start()
        if u == 1:
            for copy in filt_copies[1:]:
                copy.start()
        new_filter = d == 0 and conv
        if new_filter and u > 0:
            filt_copies[f].wait()

        def ready(ct, u=u, f=f, new_filter=new_filter):
            if new_filter:
                fill_window(win, rows.at[f], ct)
            if u == 0:
                lane_copy(ct).wait()

        if conv:
            conv_block(ring.at[u], win, parts[d].at[f], ready)
    for u in range(len(units)):
        out_copy(u).wait()


def stream_call(layer, units, v_cache, z_cache, long_filt, earlier=()):
    hbm = pl.BlockSpec(memory_space=pltpu.HBM)
    num_in = 3 + len(earlier)
    num_conv = 1 + max(f for f, _, conv in units if conv)
    part = jax.ShapeDtypeStruct((num_conv, NUM_STEPS, BLK, CH), F32)
    return pl.pallas_call(
        functools.partial(stream_kernel, layer, units, num_in),
        out_shape=(jax.ShapeDtypeStruct(v_cache.shape, BF16), jax.ShapeDtypeStruct(z_cache.shape, BF16)) + (part,) * 4,
        in_specs=[hbm] * num_in,
        out_specs=[hbm] * 2 + [pl.BlockSpec(memory_space=pltpu.VMEM)] * 4,
        scratch_shapes=[
            pltpu.VMEM((SLOTS, BLK, SHARD, CH), BF16),
            pltpu.VMEM((2, SHARD + 8, CH), F32),
            pltpu.VMEM((CH // 128, SHARD + 8, 128), F32),
            pltpu.SemaphoreType.DMA((len(units),)),
            pltpu.SemaphoreType.DMA((len(units),)),
            pltpu.SemaphoreType.DMA((2,)),
            pltpu.SemaphoreType.DMA((CH // 128,)),
        ],
        input_output_aliases={3: 0, 4: 1} if earlier else {},
        cost_estimate=pl.CostEstimate(flops=SEQ * SHARD * CH * 16, bytes_accessed=4 * SEQ * SHARD * CH * 2, transcendentals=0),
        compiler_params=pltpu.CompilerParams(vmem_limit_bytes=30 << 20),
        name=f"stream_{layer}",
    )(v_cache, z_cache, long_filt, *earlier)


def norm_rows(rows_in):
    mean_val = jnp.mean(rows_in, axis=-1, keepdims=True)
    centered = rows_in - mean_val
    var_val = jnp.mean(centered * centered, axis=-1, keepdims=True)
    return centered * lax.rsqrt(var_val + 1e-5)


def round_bf16(x):
    return x.astype(BF16).astype(F32)


def layer_kernel(*refs):
    sums0 = refs[:4]
    parts1 = refs[4:8]
    (emb_ref, b_in_ref, taps_ref, gain_ref, b_out_ref, filt_hbm, state_hbm, w_in_hbm, w_out_hbm, w_up_hbm, w_down_hbm,
     hid_ref, st_ref, rows_ref,
     w_in, w_out, w_up, w_down, emb32, state, lags, rs_buf, st0_buf, x_send, x_recv, hid_buf, st_buf, row_buf,
     w_sem, s_sem, rs_send, rs_recv, x_ssem, x_rsem, st_ssem, st_rsem, row_ssem, row_rsem, g_ssem, g_rsem) = refs[8:]
    k = lax.axis_index("sp")
    t = lax.axis_index("tp")
    others = [lax.rem(k + d, 4) for d in range(1, 4)]
    mate = k + 1 - 2 * lax.rem(k, 2)
    across = lax.rem(k + 2, 4)
    own = pl.ds(pl.multiple_of(k * BLK, BLK), BLK)

    small = [pltpu.make_async_copy(state_hbm.at[:, own], state, s_sem.at[0]),
             pltpu.make_async_copy(filt_hbm.at[:, :, 0:8], lags, s_sem.at[1])]
    for copy in small:
        copy.start()
    w_pairs = ((w_in_hbm, w_in), (w_out_hbm, w_out), (w_up_hbm, w_up), (w_down_hbm, w_down))
    w_copies = [pltpu.make_async_copy(src.at[layer], dst.at[layer], w_sem.at[layer, idx])
                for layer in range(NUM_LAYERS) for idx, (src, dst) in enumerate(w_pairs)]
    for copy in w_copies[:2]:
        copy.start()

    barrier = pltpu.get_barrier_semaphore()
    for dev in others:
        pl.semaphore_signal(barrier, inc=1, device_id={"sp": dev}, device_id_type=MESH)
    pl.semaphore_signal(barrier, inc=1, device_id={"tp": 1 - t}, device_id_type=MESH)
    pl.semaphore_wait(barrier, 4)

    def rs_copy(f, d):
        return pltpu.make_async_remote_copy(
            src_ref=parts1[d].at[f], dst_ref=rs_buf.at[d - 1, f], send_sem=rs_send.at[f, d - 1], recv_sem=rs_recv.at[f, d - 1],
            device_id={"sp": others[d - 1]}, device_id_type=MESH)

    def cached_sum(layer, f, j):
        if layer == 0:
            return (sums0[0][f, j] + sums0[1][f, j]) + (sums0[2][f, j] + sums0[3][f, j])
        return (parts1[0][f, j] + rs_buf[0, f, j]) + (rs_buf[1, f, j] + rs_buf[2, f, j])

    def x_copy(n, h, c):
        return pltpu.make_async_remote_copy(
            src_ref=x_send.at[n, h, c], dst_ref=x_recv.at[n, h, c], send_sem=x_ssem.at[n, h, c], recv_sem=x_rsem.at[n, h, c],
            device_id={"tp": 1 - t}, device_id_type=MESH)

    def row_copy(which, layer, src=None):
        piece = row_buf.at[which, layer, own if src is None else pl.ds(src * BLK, BLK)]
        return pltpu.make_async_remote_copy(
            src_ref=piece, dst_ref=piece, send_sem=row_ssem.at[which, layer],
            recv_sem=row_rsem.at[which, layer, k if src is None else src],
            device_id={"sp": 3}, device_id_type=MESH)

    def block_of(hop):
        return pl.ds(pl.multiple_of((k if hop < 2 else across) * BLK, BLK), BLK)

    def st_copy(hop):
        piece = st_buf.at[block_of(hop)]
        return pltpu.make_async_remote_copy(
            src_ref=piece, dst_ref=piece, send_sem=st_ssem.at[hop], recv_sem=st_rsem.at[hop],
            device_id={"sp": across if hop == 1 else mate}, device_id_type=MESH)

    def keep_rows(which, layer, vals):
        for b in range(BLK):
            for j in range(NUM_STEPS):
                row_buf[which, layer, k * BLK + b, j:j + 1, :] = vals[j][b:b + 1]

        @pl.when(k < 3)
        def _():
            row_copy(which, layer).start()

    def long_conv(layer, f, j, vals):
        acc = cached_sum(layer, f, j)
        for i in range(j + 1):
            acc = acc + lags[layer, f, j - i:j - i + 1] * vals[i]
        return acc + gain_ref[layer, f:f + 1] * vals[j]

    proj_rows = [[None] * 3 for _ in range(NUM_LAYERS)]
    v_rows = [[], []]
    z_rows = [[], []]

    def matmul_exchange(n, h, lhs, w_ref):
        for c in range(NCH):
            x_send[n, h, c] = jnp.dot(lhs, w_ref[:, c * CW:(c + 1) * CW], preferred_element_type=F32)
            x_copy(n, h, c).start()

    def add_exchange(n, h, base):
        outs = []
        for c in range(NCH):
            x_copy(n, h, c).wait_recv()
            outs.append(base[:, c * CW:(c + 1) * CW] + (x_send[n, h, c] + x_recv[n, h, c]))
        return jnp.concatenate(outs, axis=1)

    def front(layer, h, rows_in):
        normed = norm_rows(rows_in).astype(BF16)
        if h == 0:
            w_copies[layer * 4].wait()
            if layer == 0:
                w_copies[2].start()
        mixed = []
        for g in range(3):
            proj = jnp.dot(normed, w_in[layer, g], preferred_element_type=F32) + b_in_ref[g, layer:layer + 1]
            proj = round_bf16(proj)
            if h == 0:
                proj_rows[layer][g] = [
                    jnp.concatenate([state[layer, b, g, s:s + 1].astype(F32) for b in range(BLK)], axis=0) for s in range(2)]
            seq = proj_rows[layer][g]
            seq += [proj[BLK * i:BLK * i + BLK] for i in range(GSTEPS)]
            tap = [taps_ref[i, g, layer:layer + 1] for i in range(3)]
            mixed.append([tap[0] * seq[j + 2] + tap[1] * seq[j + 1] + tap[2] * seq[j] for j in range(GSTEPS * h, GSTEPS * h + GSTEPS)])
        ys = []
        v_rows[layer] += [round_bf16(x) for x in mixed[2]]
        if layer == 1 and h == 0:
            for f in range(2):
                for d in range(1, 4):
                    rs_copy(f, d).wait_recv()
        for i in range(GSTEPS):
            a = long_conv(layer, 0, GSTEPS * h + i, v_rows[layer])
            z_rows[layer].append(round_bf16(mixed[0][i] * a))
            ys.append(mixed[1][i] * long_conv(layer, 1, GSTEPS * h + i, z_rows[layer]))
        if h == 0:
            w_copies[layer * 4 + 1].wait()
        matmul_exchange(layer * 2, h, jnp.concatenate(ys, axis=0).astype(BF16), w_out.at[layer])

    def send_kept(layer):
        keep_rows(0, layer, v_rows[layer])
        keep_rows(1, layer, z_rows[layer])
    def middle(layer, h, rows_in):
        out = add_exchange(layer * 2, h, rows_in) + b_out_ref[layer:layer + 1]
        act = norm_rows(out).astype(BF16)
        if h == 0:
            w_copies[layer * 4 + 2].wait()
        inner = jax.nn.gelu(jnp.dot(act, w_up[layer], preferred_element_type=F32)).astype(BF16)
        if h == 0:
            w_copies[layer * 4 + 3].wait()
        matmul_exchange(layer * 2 + 1, h, inner, w_down.at[layer])
        return out

    for copy in small:
        copy.wait()
    rows_in = []
    for h in range(GROUPS):
        emb32[...] = emb_ref[GSTEPS * h:GSTEPS * h + GSTEPS].astype(F32)
        rows_in.append(jnp.concatenate([emb32[i, own] for i in range(GSTEPS)], axis=0))
    for h in range(GROUPS):
        front(0, h, rows_in[h])
        if h == 0:
            w_copies[3].start()
    for copy in w_copies[4:6]:
        copy.start()
    for f in range(2):
        for d in range(1, 4):
            rs_copy(f, d).start()
    send_kept(0)
    outs = [middle(0, h, rows_in[h]) for h in range(GROUPS)]
    for copy in w_copies[6:8]:
        copy.start()

    normed = norm_rows(emb_ref[2:4].astype(F32).reshape(2 * SEQ, DIM)).astype(BF16)
    for g in range(3):
        proj = jnp.dot(normed, w_in[0, g], preferred_element_type=F32) + b_in_ref[g, 0:1]
        for s in range(2):
            for b in range(SEQ):
                st0_buf[b, g, s:s + 1, :] = proj[s * SEQ + b:s * SEQ + b + 1]
    st_ref[0] = st0_buf[...].astype(BF16)

    rows_in = []
    for h in range(GROUPS):
        rows_in.append(add_exchange(1, h, outs[h]))
        front(1, h, rows_in[h])
    for g in range(3):
        for s in range(2):
            for i in range(BLK):
                st_buf[k * BLK + i, g, s:s + 1, :] = proj_rows[1][g][4 + s][i:i + 1]
    st_copy(1).start()
    st_copy(0).start()
    send_kept(1)
    outs = [middle(1, h, rows_in[h]) for h in range(GROUPS)]
    st_copy(1).wait_recv()
    st_copy(2).start()

    def g_copy(h, c, hop):
        piece = hid_buf.at[h, c, :, block_of(hop)]
        return pltpu.make_async_remote_copy(
            src_ref=piece, dst_ref=piece, send_sem=g_ssem.at[h, c, hop], recv_sem=g_rsem.at[h, c, hop],
            device_id={"sp": across if hop == 1 else mate}, device_id_type=MESH)

    chunks = [(h, c) for h in range(GROUPS) for c in range(NCH)]
    for h, c in chunks:
        x_copy(3, h, c).wait_recv()
        done = outs[h][:, c * CW:(c + 1) * CW] + (x_send[3, h, c] + x_recv[3, h, c])
        for i in range(GSTEPS):
            hid_buf[h, c, i, own] = done[BLK * i:BLK * i + BLK]
        g_copy(h, c, 1).start()
        g_copy(h, c, 0).start()
    st_copy(0).wait_recv()
    st_copy(2).wait_recv()
    st_ref[1] = st_buf[...].astype(BF16)

    @pl.when(k == 3)
    def _():
        for layer in range(NUM_LAYERS):
            for which in range(2):
                for src in range(3):
                    row_copy(which, layer, src).wait_recv()
        rows_ref[...] = row_buf[...]

    for h, c in chunks:
        g_copy(h, c, 1).wait_recv()
        g_copy(h, c, 2).start()
    for h, c in chunks:
        g_copy(h, c, 0).wait_recv()
        g_copy(h, c, 2).wait_recv()
        hid_ref[GSTEPS * h:GSTEPS * h + GSTEPS, :, c * CW:(c + 1) * CW] = hid_buf[h, c]

    for h, c in chunks:
        for n in range(4):
            x_copy(n, h, c).wait_send()
        for hop in range(3):
            g_copy(h, c, hop).wait_send()
    for f in range(2):
        for d in range(1, 4):
            rs_copy(f, d).wait_send()
    for hop in range(3):
        st_copy(hop).wait_send()

    @pl.when(k < 3)
    def _():
        for layer in range(NUM_LAYERS):
            for which in range(2):
                row_copy(which, layer).wait_send()


def layer_call(sums0, parts1, step_emb, b_in, taps, gain, b_out, long_filt, state, w_in, w_out, w_up, w_down):
    vm = pl.BlockSpec(memory_space=pltpu.VMEM)
    hbm = pl.BlockSpec(memory_space=pltpu.HBM)
    dma = pltpu.SemaphoreType.DMA
    return pl.pallas_call(
        layer_kernel,
        out_shape=(
            jax.ShapeDtypeStruct((NUM_STEPS, SEQ, DIM), F32),
            jax.ShapeDtypeStruct((NUM_LAYERS, SEQ, 3, 2, CH), BF16),
            jax.ShapeDtypeStruct((2, NUM_LAYERS, SEQ, NUM_STEPS, CH), F32),
        ),
        in_specs=[vm] * 13 + [hbm] * 6,
        out_specs=[vm] * 3,
        scratch_shapes=[
            pltpu.VMEM(w_in.shape, BF16),
            pltpu.VMEM(w_out.shape, BF16),
            pltpu.VMEM(w_up.shape, BF16),
            pltpu.VMEM(w_down.shape, BF16),
            pltpu.VMEM((GSTEPS, SEQ, DIM), F32),
            pltpu.VMEM((NUM_LAYERS, BLK, 3, 2, CH), BF16),
            pltpu.VMEM((NUM_LAYERS, 2, 8, CH), F32),
            pltpu.VMEM((3, 2, NUM_STEPS, BLK, CH), F32),
            pltpu.VMEM((SEQ, 3, 2, CH), F32),
            pltpu.VMEM((4, GROUPS, NCH, GSTEPS * BLK, CW), F32),
            pltpu.VMEM((4, GROUPS, NCH, GSTEPS * BLK, CW), F32),
            pltpu.VMEM((GROUPS, NCH, GSTEPS, SEQ, CW), F32),
            pltpu.VMEM((SEQ, 3, 2, CH), F32),
            pltpu.VMEM((2, NUM_LAYERS, SEQ, NUM_STEPS, CH), F32),
            dma((NUM_LAYERS, 4)),
            dma((2,)),
            dma((2, 3)),
            dma((2, 3)),
            dma((4, GROUPS, NCH)),
            dma((4, GROUPS, NCH)),
            dma((3,)),
            dma((3,)),
            dma((2, NUM_LAYERS)),
            dma((2, NUM_LAYERS, 4)),
            dma((GROUPS, NCH, 3)),
            dma((GROUPS, NCH, 3)),
        ],
        compiler_params=pltpu.CompilerParams(collective_id=0, has_side_effects=True, vmem_limit_bytes=44 << 20),
        name="layers",
    )(*sums0, *parts1, step_emb, b_in, taps, gain, b_out, long_filt, state, w_in, w_out, w_up, w_down)


def put_kernel(hid_in, st_in, rows_ref, v_in, z_in, hid_out, st_out, v_out, z_out, wide, tile, sems, o_sem):
    copies = [pltpu.make_async_copy(hid_in, hid_out, o_sem.at[0]), pltpu.make_async_copy(st_in, st_out, o_sem.at[1])]
    for copy in copies:
        copy.start()

    @pl.when(lax.axis_index("sp") == 3)
    def _():
        row_copies = []
        for which, dst in enumerate((v_out, z_out)):
            for layer in range(NUM_LAYERS):
                wide[:, 4:8, :] = jnp.zeros((SEQ, 4, CH), F32)
                wide[:, 0:4, :] = rows_ref[which, layer]
                tile[which, layer] = wide[...].astype(BF16)
                copy = pltpu.make_async_copy(tile.at[which, layer], dst.at[layer, :, 0:8, :], sems.at[which, layer])
                copy.start()
                row_copies.append(copy)
        for copy in row_copies:
            copy.wait()

    for copy in copies:
        copy.wait()


def put_call(hidden, states, rows, v_new, z_new):
    hbm = pl.BlockSpec(memory_space=pltpu.HBM)
    vm = pl.BlockSpec(memory_space=pltpu.VMEM)
    return pl.pallas_call(
        put_kernel,
        out_shape=(jax.ShapeDtypeStruct(hidden.shape, F32), jax.ShapeDtypeStruct(states.shape, BF16),
                   jax.ShapeDtypeStruct(v_new.shape, BF16), jax.ShapeDtypeStruct(z_new.shape, BF16)),
        in_specs=[vm] * 3 + [hbm] * 2,
        out_specs=[hbm] * 4,
        scratch_shapes=[
            pltpu.VMEM((SEQ, 8, CH), F32),
            pltpu.VMEM((2, NUM_LAYERS, SEQ, 8, CH), BF16),
            pltpu.SemaphoreType.DMA((2, NUM_LAYERS)),
            pltpu.SemaphoreType.DMA((2,)),
        ],
        input_output_aliases={3: 2, 4: 3},
        compiler_params=pltpu.CompilerParams(vmem_limit_bytes=16 << 20),
        name="put_rows",
    )(hidden, states, rows, v_new, z_new)


def solution(mesh):
    def device_fn(step_emb, v_cache, z_cache, short_state, w_in, b_in, short_taps, long_filt, skip_gain, w_out, b_out, w_up, w_down):
        v_cache, z_cache, long_filt, w_in, w_out, w_up, w_down = [
            pltpu.with_memory_space_constraint(x, pltpu.HBM)
            for x in (v_cache, z_cache, long_filt, jnp.transpose(w_in, (0, 2, 1, 3)), w_out, w_up, w_down)]
        both = tuple((f, d, True) for f in range(2) for d in range(4))
        v_new, z_new, *parts0 = stream_call(0, both, v_cache, z_cache, long_filt)
        sums0 = [parts0[0]] + [lax.ppermute(parts0[d], "sp", [(i, (i + d) % 4) for i in range(4)]) for d in range(1, 4)]
        v_new, z_new, *parts1 = stream_call(1, both, v_cache, z_cache, long_filt, (v_new, z_new))
        hidden, states, rows = layer_call(
            sums0, parts1, step_emb, jnp.transpose(b_in, (1, 0, 2)), jnp.transpose(short_taps, (1, 2, 0, 3)),
            skip_gain, b_out, long_filt, jnp.transpose(short_state, (0, 1, 3, 2, 4)),
            w_in, w_out, w_up, w_down)
        hidden, states, v_new, z_new = put_call(hidden, states, rows, v_new, z_new)
        return hidden, v_new, z_new, jnp.transpose(states, (0, 1, 3, 2, 4))

    specs_in = (
        P(None, "dp", None),
        P(None, "dp", "sp", "tp"),
        P(None, "dp", "sp", "tp"),
        P(None, "dp", None, None, "tp"),
        P(None, None, None, "tp"),
        P(None, None, "tp"),
        P(None, None, None, "tp"),
        P(None, None, None, "tp"),
        P(None, None, "tp"),
        P(None, "tp", None),
        P(None, None),
        P(None, None, "tp"),
        P(None, "tp", None),
    )
    specs_out = (
        P(None, "dp", None),
        P(None, "dp", "sp", "tp"),
        P(None, "dp", "sp", "tp"),
        P(None, "dp", None, None, "tp"),
    )
    return jax.shard_map(device_fn, mesh=mesh, in_specs=specs_in, out_specs=specs_out, check_vma=False)
```

```python
import functools

import jax
import jax.numpy as jnp
from jax import lax
from jax.experimental import pallas as pl
from jax.experimental.pallas import tpu as pltpu
from jax.sharding import PartitionSpec as P

F32 = jnp.float32
BF16 = jnp.bfloat16
NUM_STEPS = 4
NUM_LAYERS = 2
SEQ = 32
BLK = 8
DIM = 1024
CH = 512
UP = 2048
SHARD = 256
NCH = 2
CW = DIM // NCH
SLOTS = 8
GROUPS = 2
GSTEPS = NUM_STEPS // GROUPS
MESH = pl.DeviceIdType.MESH


def pair_rows(lo, hi, shift):
    clear = (lax.broadcasted_iota(jnp.int32, (8, 128), 0) // shift) % 2 == 0
    if shift == 4:
        return jnp.where(clear, lo, hi) + pltpu.roll(jnp.where(clear, hi, lo), 4, 0)
    return jnp.where(clear, lo + pltpu.roll(lo, 8 - shift, 0), hi + pltpu.roll(hi, shift, 0))


def fill_window(win, filt_rows, ct):
    flip = 7 - lax.broadcasted_iota(jnp.int32, (8, 128), 0)
    lanes = pl.ds(pl.multiple_of(ct * 128, 128), 128)
    for m in range(SHARD // 8 + 1):
        rows = filt_rows[SHARD - 8 * m:SHARD - 8 * m + 8, lanes]
        win[ct, 8 * m:8 * m + 8] = jnp.take_along_axis(rows, flip, axis=0)


def conv_block(src, win, dst, ready):
    @pl.loop(0, CH // 128)
    def _(ct):
        ready(ct)
        lanes = pl.ds(pl.multiple_of(ct * 128, 128), 128)
        half = []
        for seqs in ((0, 4, 1, 5), (2, 6, 3, 7)):
            accs = [[None] * NUM_STEPS for _ in seqs]
            for pt in range(SHARD // 16):
                w = [[win[ct, 16 * pt + 8 * h + 7 - j:16 * pt + 8 * h + 15 - j] for h in range(2)] for j in range(NUM_STEPS)]
                for i, b in enumerate(seqs):
                    x = src[b, 16 * pt:16 * pt + 16, lanes].astype(F32)
                    for j in range(NUM_STEPS):
                        for h in range(2):
                            term = x[8 * h:8 * h + 8] * w[j][h]
                            accs[i][j] = term if accs[i][j] is None else accs[i][j] + term
            half.append([[pair_rows(accs[0][j], accs[1][j], 4), pair_rows(accs[2][j], accs[3][j], 4)] for j in range(NUM_STEPS)])
        for j in range(NUM_STEPS):
            dst[j, :, lanes] = pair_rows(pair_rows(half[0][j][0], half[1][j][0], 2), pair_rows(half[0][j][1], half[1][j][1], 2), 1)


def stream_kernel(layer, units, num_in, *refs):
    num_conv = 1 + max(f for f, _, conv in units if conv)
    v_in, z_in, filt = refs[:3]
    v_out, z_out = refs[num_in:num_in + 2]
    parts = refs[num_in + 2:num_in + 6]
    ring, rows, win, in_sem, out_sem, filt_sem, lane_sem = refs[num_in + 6:]
    k = lax.axis_index("sp")
    first = pl.multiple_of(jnp.maximum(2 - k, 0) * SHARD, SHARD)

    def seqs(u):
        return pl.ds(pl.multiple_of(lax.rem(k + units[u][1], 4) * BLK, BLK), BLK)

    def in_copy(u):
        return pltpu.make_async_copy((v_in, z_in)[units[u][0]].at[layer, seqs(u)], ring.at[u], in_sem.at[u])

    def lane_copy(ct):
        lanes = pl.ds(pl.multiple_of(ct * 128, 128), 128)
        return pltpu.make_async_copy(
            (v_in, z_in)[units[0][0]].at[layer, seqs(0), :, lanes], ring.at[0, :, :, lanes], lane_sem.at[ct])

    def out_copy(u):
        return pltpu.make_async_copy(ring.at[u], (v_out, z_out)[units[u][0]].at[layer, seqs(u)], out_sem.at[u])

    filt_copies = [pltpu.make_async_copy(filt.at[layer, f, pl.ds(first, SHARD + 8)], rows.at[f], filt_sem.at[f])
                   for f in range(num_conv)]
    reads = {0: (2,), 1: (3, 4), 2: (5, 6), 3: (7,)}
    writes = {3: (0, 1), 4: (2, 3), 5: (4, 5), 6: (6,), 7: (7,)}
    filt_copies[0].start()
    lane_copy(0).start()
    filt_copies[0].wait()
    for ct in range(1, CH // 128):
        lane_copy(ct).start()
    in_copy(1).start()
    for u, (f, d, conv) in enumerate(units):
        if u > 0:
            in_copy(u).wait()
        for nxt in reads.get(u, ()):
            in_copy(nxt).start()
        for nxt in writes.get(u, ()):
            out_copy(nxt).start()
        if u == 1:
            for copy in filt_copies[1:]:
                copy.start()
        new_filter = d == 0 and conv
        if new_filter and u > 0:
            filt_copies[f].wait()

        def ready(ct, u=u, f=f, new_filter=new_filter):
            if new_filter:
                fill_window(win, rows.at[f], ct)
            if u == 0:
                lane_copy(ct).wait()

        if conv:
            conv_block(ring.at[u], win, parts[d].at[f], ready)
    for u in range(len(units)):
        out_copy(u).wait()


def stream_call(layer, units, v_cache, z_cache, long_filt, earlier=()):
    hbm = pl.BlockSpec(memory_space=pltpu.HBM)
    num_in = 3 + len(earlier)
    num_conv = 1 + max(f for f, _, conv in units if conv)
    part = jax.ShapeDtypeStruct((num_conv, NUM_STEPS, BLK, CH), F32)
    return pl.pallas_call(
        functools.partial(stream_kernel, layer, units, num_in),
        out_shape=(jax.ShapeDtypeStruct(v_cache.shape, BF16), jax.ShapeDtypeStruct(z_cache.shape, BF16)) + (part,) * 4,
        in_specs=[hbm] * num_in,
        out_specs=[hbm] * 2 + [pl.BlockSpec(memory_space=pltpu.VMEM)] * 4,
        scratch_shapes=[
            pltpu.VMEM((SLOTS, BLK, SHARD, CH), BF16),
            pltpu.VMEM((2, SHARD + 8, CH), F32),
            pltpu.VMEM((CH // 128, SHARD + 8, 128), F32),
            pltpu.SemaphoreType.DMA((len(units),)),
            pltpu.SemaphoreType.DMA((len(units),)),
            pltpu.SemaphoreType.DMA((2,)),
            pltpu.SemaphoreType.DMA((CH // 128,)),
        ],
        input_output_aliases={3: 0, 4: 1} if earlier else {},
        cost_estimate=pl.CostEstimate(flops=SEQ * SHARD * CH * 16, bytes_accessed=4 * SEQ * SHARD * CH * 2, transcendentals=0),
        compiler_params=pltpu.CompilerParams(vmem_limit_bytes=30 << 20),
        name=f"stream_{layer}",
    )(v_cache, z_cache, long_filt, *earlier)


def norm_rows(rows_in):
    mean_val = jnp.mean(rows_in, axis=-1, keepdims=True)
    centered = rows_in - mean_val
    var_val = jnp.mean(centered * centered, axis=-1, keepdims=True)
    return centered * lax.rsqrt(var_val + 1e-5)


def round_bf16(x):
    return x.astype(BF16).astype(F32)


def layer_kernel(*refs):
    sums0 = refs[:4]
    parts1 = refs[4:8]
    (emb_ref, b_in_ref, taps_ref, gain_ref, b_out_ref, filt_hbm, state_hbm, w_in_hbm, w_out_hbm, w_up_hbm, w_down_hbm,
     hid_ref, st_ref, rows_ref,
     w_in, w_out, w_up, w_down, emb32, state, lags, rs_buf, st0_buf, x_send, x_recv, y_recv, hid_buf, st_buf, row_buf,
     w_sem, s_sem, rs_send, rs_recv, x_ssem, x_rsem, y_ssem, y_rsem, st_ssem, st_rsem, row_ssem, row_rsem, g_ssem, g_rsem) = refs[8:]
    k = lax.axis_index("sp")
    t = lax.axis_index("tp")
    others = [lax.rem(k + d, 4) for d in range(1, 4)]
    mate = k + 1 - 2 * lax.rem(k, 2)
    across = lax.rem(k + 2, 4)
    own = pl.ds(pl.multiple_of(k * BLK, BLK), BLK)

    small = [pltpu.make_async_copy(state_hbm.at[:, own], state, s_sem.at[0]),
             pltpu.make_async_copy(filt_hbm.at[:, :, 0:8], lags, s_sem.at[1])]
    for copy in small:
        copy.start()
    w_pairs = ((w_in_hbm, w_in), (w_out_hbm, w_out), (w_up_hbm, w_up), (w_down_hbm, w_down))
    w_copies = [pltpu.make_async_copy(src.at[layer], dst.at[layer], w_sem.at[layer, idx])
                for layer in range(NUM_LAYERS) for idx, (src, dst) in enumerate(w_pairs)]
    for copy in w_copies[:2]:
        copy.start()

    barrier = pltpu.get_barrier_semaphore()
    for dev in others:
        pl.semaphore_signal(barrier, inc=1, device_id={"sp": dev}, device_id_type=MESH)
    pl.semaphore_signal(barrier, inc=1, device_id={"tp": 1 - t}, device_id_type=MESH)
    pl.semaphore_signal(barrier, inc=1, device_id={"sp": across, "tp": 1 - t}, device_id_type=MESH)
    pl.semaphore_wait(barrier, 5)

    def rs_copy(f, d):
        return pltpu.make_async_remote_copy(
            src_ref=parts1[d].at[f], dst_ref=rs_buf.at[d - 1, f], send_sem=rs_send.at[f, d - 1], recv_sem=rs_recv.at[f, d - 1],
            device_id={"sp": others[d - 1]}, device_id_type=MESH)

    def cached_sum(layer, f, j):
        if layer == 0:
            return (sums0[0][f, j] + sums0[1][f, j]) + (sums0[2][f, j] + sums0[3][f, j])
        return (parts1[0][f, j] + rs_buf[0, f, j]) + (rs_buf[1, f, j] + rs_buf[2, f, j])

    def x_copy(n, h, c):
        return pltpu.make_async_remote_copy(
            src_ref=x_send.at[n, h, c], dst_ref=x_recv.at[n, h, c], send_sem=x_ssem.at[n, h, c], recv_sem=x_rsem.at[n, h, c],
            device_id={"tp": 1 - t}, device_id_type=MESH)

    def row_copy(which, layer, src=None):
        piece = row_buf.at[which, layer, own if src is None else pl.ds(src * BLK, BLK)]
        return pltpu.make_async_remote_copy(
            src_ref=piece, dst_ref=piece, send_sem=row_ssem.at[which, layer],
            recv_sem=row_rsem.at[which, layer, k if src is None else src],
            device_id={"sp": 3}, device_id_type=MESH)

    def block_of(hop):
        return pl.ds(pl.multiple_of((k if hop < 2 else across) * BLK, BLK), BLK)

    def st_copy(hop):
        piece = st_buf.at[block_of(hop)]
        return pltpu.make_async_remote_copy(
            src_ref=piece, dst_ref=piece, send_sem=st_ssem.at[hop], recv_sem=st_rsem.at[hop],
            device_id={"sp": across if hop == 1 else mate}, device_id_type=MESH)

    def keep_rows(which, layer, vals):
        for b in range(BLK):
            for j in range(NUM_STEPS):
                row_buf[which, layer, k * BLK + b, j:j + 1, :] = vals[j][b:b + 1]

        @pl.when(k < 3)
        def _():
            row_copy(which, layer).start()

    def long_conv(layer, f, j, vals):
        acc = cached_sum(layer, f, j)
        for i in range(j + 1):
            acc = acc + lags[layer, f, j - i:j - i + 1] * vals[i]
        return acc + gain_ref[layer, f:f + 1] * vals[j]

    proj_rows = [[None] * 3 for _ in range(NUM_LAYERS)]
    v_rows = [[], []]
    z_rows = [[], []]

    def y_copy(h, c, other):
        return pltpu.make_async_remote_copy(
            src_ref=x_send.at[3, h, c], dst_ref=y_recv.at[other, h, c], send_sem=y_ssem.at[other, h, c], recv_sem=y_rsem.at[other, h, c],
            device_id={"sp": across, "tp": (1 - t) if other else t}, device_id_type=MESH)

    def matmul_exchange(n, h, lhs, w_ref, base=None):
        for c in range(NCH):
            part = jnp.dot(lhs, w_ref[:, c * CW:(c + 1) * CW], preferred_element_type=F32)
            if base is not None:
                part = part + jnp.where(t == 0, base[:, c * CW:(c + 1) * CW], 0.0)
            x_send[n, h, c] = part
            if base is not None:
                y_copy(h, c, 1).start()
                y_copy(h, c, 0).start()
            x_copy(n, h, c).start()

    def add_exchange(n, h, base):
        outs = []
        for c in range(NCH):
            x_copy(n, h, c).wait_recv()
            outs.append(base[:, c * CW:(c + 1) * CW] + (x_send[n, h, c] + x_recv[n, h, c]))
        return jnp.concatenate(outs, axis=1)

    def front(layer, h, rows_in):
        normed = norm_rows(rows_in).astype(BF16)
        if h == 0:
            w_copies[layer * 4].wait()
            if layer == 0:
                w_copies[2].start()
        mixed = []
        for g in range(3):
            proj = jnp.dot(normed, w_in[layer, g], preferred_element_type=F32) + b_in_ref[g, layer:layer + 1]
            proj = round_bf16(proj)
            if h == 0:
                proj_rows[layer][g] = [
                    jnp.concatenate([state[layer, b, g, s:s + 1].astype(F32) for b in range(BLK)], axis=0) for s in range(2)]
            seq = proj_rows[layer][g]
            seq += [proj[BLK * i:BLK * i + BLK] for i in range(GSTEPS)]
            tap = [taps_ref[i, g, layer:layer + 1] for i in range(3)]
            mixed.append([tap[0] * seq[j + 2] + tap[1] * seq[j + 1] + tap[2] * seq[j] for j in range(GSTEPS * h, GSTEPS * h + GSTEPS)])
        ys = []
        v_rows[layer] += [round_bf16(x) for x in mixed[2]]
        if layer == 1 and h == 0:
            for f in range(2):
                for d in range(1, 4):
                    rs_copy(f, d).wait_recv()
        for i in range(GSTEPS):
            a = long_conv(layer, 0, GSTEPS * h + i, v_rows[layer])
            z_rows[layer].append(round_bf16(mixed[0][i] * a))
            ys.append(mixed[1][i] * long_conv(layer, 1, GSTEPS * h + i, z_rows[layer]))
        if h == 0:
            w_copies[layer * 4 + 1].wait()
        matmul_exchange(layer * 2, h, jnp.concatenate(ys, axis=0).astype(BF16), w_out.at[layer])

    def send_kept(layer):
        keep_rows(0, layer, v_rows[layer])
        keep_rows(1, layer, z_rows[layer])
    def middle(layer, h, rows_in):
        out = add_exchange(layer * 2, h, rows_in) + b_out_ref[layer:layer + 1]
        act = norm_rows(out).astype(BF16)
        if h == 0:
            w_copies[layer * 4 + 2].wait()
        inner = jax.nn.gelu(jnp.dot(act, w_up[layer], preferred_element_type=F32)).astype(BF16)
        if h == 0:
            w_copies[layer * 4 + 3].wait()
        matmul_exchange(layer * 2 + 1, h, inner, w_down.at[layer], out if layer == 1 else None)
        return out

    for copy in small:
        copy.wait()
    rows_in = []
    for h in range(GROUPS):
        emb32[...] = emb_ref[GSTEPS * h:GSTEPS * h + GSTEPS].astype(F32)
        rows_in.append(jnp.concatenate([emb32[i, own] for i in range(GSTEPS)], axis=0))
    for h in range(GROUPS):
        front(0, h, rows_in[h])
        if h == 0:
            w_copies[3].start()
    for copy in w_copies[4:6]:
        copy.start()
    for f in range(2):
        for d in range(1, 4):
            rs_copy(f, d).start()
    send_kept(0)
    outs = [middle(0, h, rows_in[h]) for h in range(GROUPS)]
    for copy in w_copies[6:8]:
        copy.start()

    normed = norm_rows(emb_ref[2:4].astype(F32).reshape(2 * SEQ, DIM)).astype(BF16)
    for g in range(3):
        proj = jnp.dot(normed, w_in[0, g], preferred_element_type=F32) + b_in_ref[g, 0:1]
        for s in range(2):
            for b in range(SEQ):
                st0_buf[b, g, s:s + 1, :] = proj[s * SEQ + b:s * SEQ + b + 1]
    st_ref[0] = st0_buf[...].astype(BF16)

    rows_in = []
    for h in range(GROUPS):
        rows_in.append(add_exchange(1, h, outs[h]))
        front(1, h, rows_in[h])
    for g in range(3):
        for s in range(2):
            for i in range(BLK):
                st_buf[k * BLK + i, g, s:s + 1, :] = proj_rows[1][g][4 + s][i:i + 1]
    st_copy(1).start()
    st_copy(0).start()
    send_kept(1)
    outs = [middle(1, h, rows_in[h]) for h in range(GROUPS)]
    st_copy(1).wait_recv()
    st_copy(2).start()

    def g_copy(h, c, hop):
        piece = hid_buf.at[h, c, :, block_of(hop)]
        return pltpu.make_async_remote_copy(
            src_ref=piece, dst_ref=piece, send_sem=g_ssem.at[h, c, hop], recv_sem=g_rsem.at[h, c, hop],
            device_id={"sp": across if hop == 1 else mate}, device_id_type=MESH)

    chunks = [(h, c) for h in range(GROUPS) for c in range(NCH)]
    def keep_sum(h, c, total, hop):
        for i in range(GSTEPS):
            hid_buf[h, c, i, block_of(hop)] = total[BLK * i:BLK * i + BLK]
        g_copy(h, c, hop).start()

    for h in range(GROUPS):
        for c in range(NCH):
            x_copy(3, h, c).wait_recv()
            keep_sum(h, c, x_send[3, h, c] + x_recv[3, h, c], 0)
        for c in range(NCH):
            y_copy(h, c, 0).wait_recv()
            y_copy(h, c, 1).wait_recv()
            keep_sum(h, c, y_recv[0, h, c] + y_recv[1, h, c], 2)
    st_copy(0).wait_recv()
    st_copy(2).wait_recv()
    st_ref[1] = st_buf[...].astype(BF16)

    @pl.when(k == 3)
    def _():
        for layer in range(NUM_LAYERS):
            for which in range(2):
                for src in range(3):
                    row_copy(which, layer, src).wait_recv()
        rows_ref[...] = row_buf[...]

    for h, c in chunks:
        g_copy(h, c, 0).wait_recv()
        g_copy(h, c, 2).wait_recv()
        hid_ref[GSTEPS * h:GSTEPS * h + GSTEPS, :, c * CW:(c + 1) * CW] = hid_buf[h, c]

    for h, c in chunks:
        for n in range(4):
            x_copy(n, h, c).wait_send()
        for hop in (0, 2):
            g_copy(h, c, hop).wait_send()
        for other in range(2):
            y_copy(h, c, other).wait_send()
    for f in range(2):
        for d in range(1, 4):
            rs_copy(f, d).wait_send()
    for hop in range(3):
        st_copy(hop).wait_send()

    @pl.when(k < 3)
    def _():
        for layer in range(NUM_LAYERS):
            for which in range(2):
                row_copy(which, layer).wait_send()


def layer_call(sums0, parts1, step_emb, b_in, taps, gain, b_out, long_filt, state, w_in, w_out, w_up, w_down):
    vm = pl.BlockSpec(memory_space=pltpu.VMEM)
    hbm = pl.BlockSpec(memory_space=pltpu.HBM)
    dma = pltpu.SemaphoreType.DMA
    return pl.pallas_call(
        layer_kernel,
        out_shape=(
            jax.ShapeDtypeStruct((NUM_STEPS, SEQ, DIM), F32),
            jax.ShapeDtypeStruct((NUM_LAYERS, SEQ, 3, 2, CH), BF16),
            jax.ShapeDtypeStruct((2, NUM_LAYERS, SEQ, NUM_STEPS, CH), F32),
        ),
        in_specs=[vm] * 13 + [hbm] * 6,
        out_specs=[vm] * 3,
        scratch_shapes=[
            pltpu.VMEM(w_in.shape, BF16),
            pltpu.VMEM(w_out.shape, BF16),
            pltpu.VMEM(w_up.shape, BF16),
            pltpu.VMEM(w_down.shape, BF16),
            pltpu.VMEM((GSTEPS, SEQ, DIM), F32),
            pltpu.VMEM((NUM_LAYERS, BLK, 3, 2, CH), BF16),
            pltpu.VMEM((NUM_LAYERS, 2, 8, CH), F32),
            pltpu.VMEM((3, 2, NUM_STEPS, BLK, CH), F32),
            pltpu.VMEM((SEQ, 3, 2, CH), F32),
            pltpu.VMEM((4, GROUPS, NCH, GSTEPS * BLK, CW), F32),
            pltpu.VMEM((4, GROUPS, NCH, GSTEPS * BLK, CW), F32),
            pltpu.VMEM((2, GROUPS, NCH, GSTEPS * BLK, CW), F32),
            pltpu.VMEM((GROUPS, NCH, GSTEPS, SEQ, CW), F32),
            pltpu.VMEM((SEQ, 3, 2, CH), F32),
            pltpu.VMEM((2, NUM_LAYERS, SEQ, NUM_STEPS, CH), F32),
            dma((NUM_LAYERS, 4)),
            dma((2,)),
            dma((2, 3)),
            dma((2, 3)),
            dma((4, GROUPS, NCH)),
            dma((4, GROUPS, NCH)),
            dma((2, GROUPS, NCH)),
            dma((2, GROUPS, NCH)),
            dma((3,)),
            dma((3,)),
            dma((2, NUM_LAYERS)),
            dma((2, NUM_LAYERS, 4)),
            dma((GROUPS, NCH, 3)),
            dma((GROUPS, NCH, 3)),
        ],
        compiler_params=pltpu.CompilerParams(collective_id=0, has_side_effects=True, vmem_limit_bytes=44 << 20),
        name="layers",
    )(*sums0, *parts1, step_emb, b_in, taps, gain, b_out, long_filt, state, w_in, w_out, w_up, w_down)


def put_kernel(hid_in, st_in, rows_ref, v_in, z_in, hid_out, st_out, v_out, z_out, wide, tile, sems, o_sem):
    copies = [pltpu.make_async_copy(hid_in, hid_out, o_sem.at[0]), pltpu.make_async_copy(st_in, st_out, o_sem.at[1])]
    for copy in copies:
        copy.start()

    @pl.when(lax.axis_index("sp") == 3)
    def _():
        row_copies = []
        for which, dst in enumerate((v_out, z_out)):
            for layer in range(NUM_LAYERS):
                wide[:, 4:8, :] = jnp.zeros((SEQ, 4, CH), F32)
                wide[:, 0:4, :] = rows_ref[which, layer]
                tile[which, layer] = wide[...].astype(BF16)
                copy = pltpu.make_async_copy(tile.at[which, layer], dst.at[layer, :, 0:8, :], sems.at[which, layer])
                copy.start()
                row_copies.append(copy)
        for copy in row_copies:
            copy.wait()

    for copy in copies:
        copy.wait()


def put_call(hidden, states, rows, v_new, z_new):
    hbm = pl.BlockSpec(memory_space=pltpu.HBM)
    vm = pl.BlockSpec(memory_space=pltpu.VMEM)
    return pl.pallas_call(
        put_kernel,
        out_shape=(jax.ShapeDtypeStruct(hidden.shape, F32), jax.ShapeDtypeStruct(states.shape, BF16),
                   jax.ShapeDtypeStruct(v_new.shape, BF16), jax.ShapeDtypeStruct(z_new.shape, BF16)),
        in_specs=[vm] * 3 + [hbm] * 2,
        out_specs=[hbm] * 4,
        scratch_shapes=[
            pltpu.VMEM((SEQ, 8, CH), F32),
            pltpu.VMEM((2, NUM_LAYERS, SEQ, 8, CH), BF16),
            pltpu.SemaphoreType.DMA((2, NUM_LAYERS)),
            pltpu.SemaphoreType.DMA((2,)),
        ],
        input_output_aliases={3: 2, 4: 3},
        compiler_params=pltpu.CompilerParams(vmem_limit_bytes=16 << 20),
        name="put_rows",
    )(hidden, states, rows, v_new, z_new)


def solution(mesh):
    def device_fn(step_emb, v_cache, z_cache, short_state, w_in, b_in, short_taps, long_filt, skip_gain, w_out, b_out, w_up, w_down):
        v_cache, z_cache, long_filt, w_in, w_out, w_up, w_down = [
            pltpu.with_memory_space_constraint(x, pltpu.HBM)
            for x in (v_cache, z_cache, long_filt, jnp.transpose(w_in, (0, 2, 1, 3)), w_out, w_up, w_down)]
        both = tuple((f, d, True) for f in range(2) for d in range(4))
        v_new, z_new, *parts0 = stream_call(0, both, v_cache, z_cache, long_filt)
        sums0 = [parts0[0]] + [lax.ppermute(parts0[d], "sp", [(i, (i + d) % 4) for i in range(4)]) for d in range(1, 4)]
        v_new, z_new, *parts1 = stream_call(1, both, v_cache, z_cache, long_filt, (v_new, z_new))
        hidden, states, rows = layer_call(
            sums0, parts1, step_emb, jnp.transpose(b_in, (1, 0, 2)), jnp.transpose(short_taps, (1, 2, 0, 3)),
            skip_gain, b_out, long_filt, jnp.transpose(short_state, (0, 1, 3, 2, 4)),
            w_in, w_out, w_up, w_down)
        hidden, states, v_new, z_new = put_call(hidden, states, rows, v_new, z_new)
        return hidden, v_new, z_new, jnp.transpose(states, (0, 1, 3, 2, 4))

    specs_in = (
        P(None, "dp", None),
        P(None, "dp", "sp", "tp"),
        P(None, "dp", "sp", "tp"),
        P(None, "dp", None, None, "tp"),
        P(None, None, None, "tp"),
        P(None, None, "tp"),
        P(None, None, None, "tp"),
        P(None, None, None, "tp"),
        P(None, None, "tp"),
        P(None, "tp", None),
        P(None, None),
        P(None, None, "tp"),
        P(None, "tp", None),
    )
    specs_out = (
        P(None, "dp", None),
        P(None, "dp", "sp", "tp"),
        P(None, "dp", "sp", "tp"),
        P(None, "dp", None, None, "tp"),
    )
    return jax.shard_map(device_fn, mesh=mesh, in_specs=specs_in, out_specs=specs_out, check_vma=False)
```

```python
import functools

import jax
import jax.numpy as jnp
from jax import lax
from jax.experimental import pallas as pl
from jax.experimental.pallas import tpu as pltpu
from jax.sharding import PartitionSpec as P

F32 = jnp.float32
BF16 = jnp.bfloat16
NUM_STEPS = 4
NUM_LAYERS = 2
SEQ = 32
BLK = 8
DIM = 1024
CH = 512
UP = 2048
SHARD = 256
NCH = 2
CW = DIM // NCH
GROUPS = 2
GSTEPS = NUM_STEPS // GROUPS
MESH = pl.DeviceIdType.MESH


def pair_rows(lo, hi, shift):
    clear = (lax.broadcasted_iota(jnp.int32, (8, 128), 0) // shift) % 2 == 0
    if shift == 4:
        return jnp.where(clear, lo, hi) + pltpu.roll(jnp.where(clear, hi, lo), 4, 0)
    return jnp.where(clear, lo + pltpu.roll(lo, 8 - shift, 0), hi + pltpu.roll(hi, shift, 0))


def fill_window(win, filt_rows, ct):
    flip = 7 - lax.broadcasted_iota(jnp.int32, (8, 128), 0)
    lanes = pl.ds(pl.multiple_of(ct * 128, 128), 128)
    for m in range(SHARD // 8 + 1):
        rows = filt_rows[SHARD - 8 * m:SHARD - 8 * m + 8, lanes]
        win[ct, 8 * m:8 * m + 8] = jnp.take_along_axis(rows, flip, axis=0)


def conv_block(src, win, dst, ready):
    @pl.loop(0, CH // 128)
    def _(ct):
        ready(ct)
        lanes = pl.ds(pl.multiple_of(ct * 128, 128), 128)
        half = []
        for seqs in ((0, 4, 1, 5), (2, 6, 3, 7)):
            accs = [[None] * NUM_STEPS for _ in seqs]
            for pt in range(SHARD // 16):
                w = [[win[ct, 16 * pt + 8 * h + 7 - j:16 * pt + 8 * h + 15 - j] for h in range(2)] for j in range(NUM_STEPS)]
                for i, b in enumerate(seqs):
                    x = src[b, 16 * pt:16 * pt + 16, lanes].astype(F32)
                    for j in range(NUM_STEPS):
                        for h in range(2):
                            term = x[8 * h:8 * h + 8] * w[j][h]
                            accs[i][j] = term if accs[i][j] is None else accs[i][j] + term
            half.append([[pair_rows(accs[0][j], accs[1][j], 4), pair_rows(accs[2][j], accs[3][j], 4)] for j in range(NUM_STEPS)])
        for j in range(NUM_STEPS):
            dst[j, :, lanes] = pair_rows(pair_rows(half[0][j][0], half[1][j][0], 2), pair_rows(half[0][j][1], half[1][j][1], 2), 1)


def stream_kernel(layer, num_in, *refs):
    v_in, z_in = refs[:2]
    if layer == 0:
        filt = refs[2]
        v_out, z_out, *parts, carry, rows_next = refs[num_in:num_in + 8]
        ring, win, in_sem, out_sem, rows, filt_sem, lane_sem, carry_sem = refs[num_in + 8:]
    else:
        carry, rows = refs[4:6]
        v_out, z_out, *parts = refs[num_in:num_in + 6]
        ring, win, in_sem, out_sem = refs[num_in + 6:]
    units = [(f, d) for f in range(2) for d in range(4)]
    k = lax.axis_index("sp")
    first = pl.multiple_of(jnp.maximum(2 - k, 0) * SHARD, SHARD)

    def seqs(u):
        return pl.ds(pl.multiple_of(lax.rem(k + units[u][1], 4) * BLK, BLK), BLK)

    def slot(u):
        return carry if layer == 1 and u == 0 else ring.at[u]

    def in_copy(u):
        return pltpu.make_async_copy((v_in, z_in)[units[u][0]].at[layer, seqs(u)], ring.at[u], in_sem.at[u])

    def lane_copy(ct):
        lanes = pl.ds(pl.multiple_of(ct * 128, 128), 128)
        return pltpu.make_async_copy(v_in.at[0, seqs(0), :, lanes], ring.at[0, :, :, lanes], lane_sem.at[ct])

    def out_copy(u):
        return pltpu.make_async_copy(slot(u), (v_out, z_out)[units[u][0]].at[layer, seqs(u)], out_sem.at[u])

    def filt_copy(f):
        return pltpu.make_async_copy(filt.at[0, f, pl.ds(first, SHARD + 8)], rows.at[f], filt_sem.at[f])

    def carry_copies():
        return [pltpu.make_async_copy(v_in.at[1, seqs(0)], carry, carry_sem.at[2])] + [
            pltpu.make_async_copy(filt.at[1, f, pl.ds(first, SHARD + 8)], rows_next.at[f], carry_sem.at[f]) for f in range(2)]

    reads = {0: (2,), 1: (3, 4), 2: (5, 6), 3: (7,)}
    writes = {3: (0, 1), 4: (2, 3), 5: (4, 5), 6: (6, 7)}
    if layer == 0:
        filt_copy(0).start()
        for ct in range(CH // 128):
            lane_copy(ct).start()
        filt_copy(0).wait()
    in_copy(1).start()
    for u, (f, d) in enumerate(units):
        if 0 < u < 7:
            in_copy(u).wait()
        if u == 6:
            in_copy(7).wait()
        for nxt in reads.get(u, ()):
            in_copy(nxt).start()
        for nxt in writes.get(u, ()):
            out_copy(nxt).start()
        if layer == 0 and u == 1:
            filt_copy(1).start()
        if layer == 0 and u == 4:
            filt_copy(1).wait()
        if layer == 0 and u == 5:
            for copy in carry_copies():
                copy.start()

        def ready(ct, u=u, f=f, d=d):
            if d == 0:
                fill_window(win, rows.at[f], ct)
            if layer == 0 and u == 0:
                lane_copy(ct).wait()

        conv_block(slot(u), win, parts[d].at[f], ready)
    for u in range(len(units)):
        out_copy(u).wait()
    if layer == 0:
        for copy in carry_copies():
            copy.wait()


def stream_call(layer, *operands):
    hbm = pl.BlockSpec(memory_space=pltpu.HBM)
    vm = pl.BlockSpec(memory_space=pltpu.VMEM)
    cache = jax.ShapeDtypeStruct(operands[0].shape, BF16)
    outs = (cache, cache) + (jax.ShapeDtypeStruct((2, NUM_STEPS, BLK, CH), F32),) * 4
    scratch = [
        pltpu.VMEM((8, BLK, SHARD, CH), BF16),
        pltpu.VMEM((CH // 128, SHARD + 8, 128), F32),
        pltpu.SemaphoreType.DMA((8,)),
        pltpu.SemaphoreType.DMA((8,)),
    ]
    if layer == 0:
        in_specs = [hbm] * 3
        outs += (jax.ShapeDtypeStruct((BLK, SHARD, CH), BF16), jax.ShapeDtypeStruct((2, SHARD + 8, CH), F32))
        scratch += [
            pltpu.VMEM((2, SHARD + 8, CH), F32),
            pltpu.SemaphoreType.DMA((2,)),
            pltpu.SemaphoreType.DMA((CH // 128,)),
            pltpu.SemaphoreType.DMA((3,)),
        ]
    else:
        in_specs = [hbm] * 4 + [vm] * 2
    return pl.pallas_call(
        functools.partial(stream_kernel, layer, len(operands)),
        out_shape=outs,
        in_specs=in_specs,
        out_specs=[hbm] * 2 + [vm] * (len(outs) - 2),
        scratch_shapes=scratch,
        input_output_aliases={} if layer == 0 else {2: 0, 3: 1},
        cost_estimate=pl.CostEstimate(flops=SEQ * SHARD * CH * 16, bytes_accessed=4 * SEQ * SHARD * CH * 2, transcendentals=0),
        compiler_params=pltpu.CompilerParams(vmem_limit_bytes=30 << 20),
        name=f"stream_{layer}",
    )(*operands)


def norm_rows(rows_in):
    mean_val = jnp.mean(rows_in, axis=-1, keepdims=True)
    centered = rows_in - mean_val
    var_val = jnp.mean(centered * centered, axis=-1, keepdims=True)
    return centered * lax.rsqrt(var_val + 1e-5)


def round_bf16(x):
    return x.astype(BF16).astype(F32)


def layer_kernel(*refs):
    sums0 = refs[:4]
    parts1 = refs[4:8]
    (emb_ref, b_in_ref, taps_ref, gain_ref, b_out_ref, state, filt_hbm, w_in_hbm, w_out_hbm, w_up_hbm, w_down_hbm,
     hid_ref, st_ref, rows_ref,
     w_in, w_out, w_up, w_down, emb32, lags, rs_buf, st0_buf, x_send, x_recv, y_recv, hid_buf, st_buf, row_buf,
     w_sem, s_sem, rs_send, rs_recv, x_ssem, x_rsem, y_ssem, y_rsem, st_ssem, st_rsem, row_ssem, row_rsem, g_ssem, g_rsem) = refs[8:]
    k = lax.axis_index("sp")
    t = lax.axis_index("tp")
    others = [lax.rem(k + d, 4) for d in range(1, 4)]
    mate = k + 1 - 2 * lax.rem(k, 2)
    across = lax.rem(k + 2, 4)
    own = pl.ds(pl.multiple_of(k * BLK, BLK), BLK)

    small = [pltpu.make_async_copy(filt_hbm.at[:, :, 0:8], lags, s_sem.at[0])]
    for copy in small:
        copy.start()
    w_pairs = ((w_in_hbm, w_in), (w_out_hbm, w_out), (w_up_hbm, w_up), (w_down_hbm, w_down))
    w_copies = [pltpu.make_async_copy(src.at[layer], dst.at[layer], w_sem.at[layer, idx])
                for layer in range(NUM_LAYERS) for idx, (src, dst) in enumerate(w_pairs)]
    for copy in w_copies[:2]:
        copy.start()

    barrier = pltpu.get_barrier_semaphore()
    for dev in others:
        pl.semaphore_signal(barrier, inc=1, device_id={"sp": dev}, device_id_type=MESH)
    pl.semaphore_signal(barrier, inc=1, device_id={"tp": 1 - t}, device_id_type=MESH)
    pl.semaphore_signal(barrier, inc=1, device_id={"sp": across, "tp": 1 - t}, device_id_type=MESH)
    pl.semaphore_wait(barrier, 5)

    def rs_copy(f, d):
        return pltpu.make_async_remote_copy(
            src_ref=parts1[d].at[f], dst_ref=rs_buf.at[d - 1, f], send_sem=rs_send.at[f, d - 1], recv_sem=rs_recv.at[f, d - 1],
            device_id={"sp": others[d - 1]}, device_id_type=MESH)

    def cached_sum(layer, f, j):
        if layer == 0:
            return (sums0[0][f, j] + sums0[1][f, j]) + (sums0[2][f, j] + sums0[3][f, j])
        return (parts1[0][f, j] + rs_buf[0, f, j]) + (rs_buf[1, f, j] + rs_buf[2, f, j])

    def x_copy(n, h, c):
        return pltpu.make_async_remote_copy(
            src_ref=x_send.at[n, h, c], dst_ref=x_recv.at[n, h, c], send_sem=x_ssem.at[n, h, c], recv_sem=x_rsem.at[n, h, c],
            device_id={"tp": 1 - t}, device_id_type=MESH)

    def row_copy(which, layer, src=None):
        piece = row_buf.at[which, layer, own if src is None else pl.ds(src * BLK, BLK)]
        return pltpu.make_async_remote_copy(
            src_ref=piece, dst_ref=piece, send_sem=row_ssem.at[which, layer],
            recv_sem=row_rsem.at[which, layer, k if src is None else src],
            device_id={"sp": 3}, device_id_type=MESH)

    def block_of(hop):
        return pl.ds(pl.multiple_of((k if hop < 2 else across) * BLK, BLK), BLK)

    def st_copy(hop):
        piece = st_buf.at[block_of(hop)]
        return pltpu.make_async_remote_copy(
            src_ref=piece, dst_ref=piece, send_sem=st_ssem.at[hop], recv_sem=st_rsem.at[hop],
            device_id={"sp": across if hop == 1 else mate}, device_id_type=MESH)

    def keep_rows(which, layer, vals):
        for b in range(BLK):
            for j in range(NUM_STEPS):
                row_buf[which, layer, k * BLK + b, j:j + 1, :] = vals[j][b:b + 1]

        @pl.when(k < 3)
        def _():
            row_copy(which, layer).start()

    def long_conv(layer, f, j, vals):
        acc = cached_sum(layer, f, j)
        for i in range(j + 1):
            acc = acc + lags[layer, f, j - i:j - i + 1] * vals[i]
        return acc + gain_ref[layer, f:f + 1] * vals[j]

    proj_rows = [[None] * 3 for _ in range(NUM_LAYERS)]
    v_rows = [[], []]
    z_rows = [[], []]

    def y_copy(h, c, other):
        return pltpu.make_async_remote_copy(
            src_ref=x_send.at[3, h, c], dst_ref=y_recv.at[other, h, c], send_sem=y_ssem.at[other, h, c], recv_sem=y_rsem.at[other, h, c],
            device_id={"sp": across, "tp": (1 - t) if other else t}, device_id_type=MESH)

    def matmul_exchange(n, h, lhs, w_ref, base=None):
        for c in range(NCH):
            part = jnp.dot(lhs, w_ref[:, c * CW:(c + 1) * CW], preferred_element_type=F32)
            if base is not None:
                part = part + jnp.where(t == 0, base[:, c * CW:(c + 1) * CW], 0.0)
            x_send[n, h, c] = part
            if base is not None:
                y_copy(h, c, 1).start()
                y_copy(h, c, 0).start()
            x_copy(n, h, c).start()

    def add_exchange(n, h, base):
        outs = []
        for c in range(NCH):
            x_copy(n, h, c).wait_recv()
            outs.append(base[:, c * CW:(c + 1) * CW] + (x_send[n, h, c] + x_recv[n, h, c]))
        return jnp.concatenate(outs, axis=1)

    def front(layer, h, rows_in):
        normed = norm_rows(rows_in).astype(BF16)
        if h == 0:
            w_copies[layer * 4].wait()
            if layer == 0:
                w_copies[2].start()
        mixed = []
        for g in range(3):
            proj = jnp.dot(normed, w_in[layer, g], preferred_element_type=F32) + b_in_ref[g, layer:layer + 1]
            proj = round_bf16(proj)
            if h == 0:
                proj_rows[layer][g] = [
                    jnp.concatenate([state[layer, k * BLK + b, g, s:s + 1].astype(F32) for b in range(BLK)], axis=0) for s in range(2)]
            seq = proj_rows[layer][g]
            seq += [proj[BLK * i:BLK * i + BLK] for i in range(GSTEPS)]
            tap = [taps_ref[i, g, layer:layer + 1] for i in range(3)]
            mixed.append([tap[0] * seq[j + 2] + tap[1] * seq[j + 1] + tap[2] * seq[j] for j in range(GSTEPS * h, GSTEPS * h + GSTEPS)])
        ys = []
        v_rows[layer] += [round_bf16(x) for x in mixed[2]]
        if layer == 1 and h == 0:
            for f in range(2):
                for d in range(1, 4):
                    rs_copy(f, d).wait_recv()
        for i in range(GSTEPS):
            a = long_conv(layer, 0, GSTEPS * h + i, v_rows[layer])
            z_rows[layer].append(round_bf16(mixed[0][i] * a))
            ys.append(mixed[1][i] * long_conv(layer, 1, GSTEPS * h + i, z_rows[layer]))
        if h == 0:
            w_copies[layer * 4 + 1].wait()
        matmul_exchange(layer * 2, h, jnp.concatenate(ys, axis=0).astype(BF16), w_out.at[layer])

    def send_kept(layer):
        keep_rows(0, layer, v_rows[layer])
        keep_rows(1, layer, z_rows[layer])
    def middle(layer, h, rows_in):
        out = add_exchange(layer * 2, h, rows_in) + b_out_ref[layer:layer + 1]
        act = norm_rows(out).astype(BF16)
        if h == 0:
            w_copies[layer * 4 + 2].wait()
        inner = jax.nn.gelu(jnp.dot(act, w_up[layer], preferred_element_type=F32)).astype(BF16)
        if h == 0:
            w_copies[layer * 4 + 3].wait()
        matmul_exchange(layer * 2 + 1, h, inner, w_down.at[layer], out if layer == 1 else None)
        return out

    for copy in small:
        copy.wait()
    rows_in = []
    for h in range(GROUPS):
        emb32[...] = emb_ref[GSTEPS * h:GSTEPS * h + GSTEPS].astype(F32)
        rows_in.append(jnp.concatenate([emb32[i, own] for i in range(GSTEPS)], axis=0))
    for h in range(GROUPS):
        front(0, h, rows_in[h])
        if h == 0:
            w_copies[3].start()
    for copy in w_copies[4:6]:
        copy.start()
    for f in range(2):
        for d in range(1, 4):
            rs_copy(f, d).start()
    send_kept(0)
    outs = [middle(0, h, rows_in[h]) for h in range(GROUPS)]
    for copy in w_copies[6:8]:
        copy.start()

    normed = norm_rows(emb_ref[2:4].astype(F32).reshape(2 * SEQ, DIM)).astype(BF16)
    for g in range(3):
        proj = jnp.dot(normed, w_in[0, g], preferred_element_type=F32) + b_in_ref[g, 0:1]
        for s in range(2):
            for b in range(SEQ):
                st0_buf[b, g, s:s + 1, :] = proj[s * SEQ + b:s * SEQ + b + 1]
    st_ref[0] = st0_buf[...].astype(BF16)

    rows_in = []
    for h in range(GROUPS):
        rows_in.append(add_exchange(1, h, outs[h]))
        front(1, h, rows_in[h])
    for g in range(3):
        for s in range(2):
            for i in range(BLK):
                st_buf[k * BLK + i, g, s:s + 1, :] = proj_rows[1][g][4 + s][i:i + 1]
    st_copy(1).start()
    st_copy(0).start()
    send_kept(1)
    outs = [middle(1, h, rows_in[h]) for h in range(GROUPS)]
    st_copy(1).wait_recv()
    st_copy(2).start()

    def g_copy(h, c, hop):
        piece = hid_buf.at[h, c, :, block_of(hop)]
        return pltpu.make_async_remote_copy(
            src_ref=piece, dst_ref=piece, send_sem=g_ssem.at[h, c, hop], recv_sem=g_rsem.at[h, c, hop],
            device_id={"sp": across if hop == 1 else mate}, device_id_type=MESH)

    chunks = [(h, c) for h in range(GROUPS) for c in range(NCH)]
    def keep_sum(h, c, total, hop):
        for i in range(GSTEPS):
            hid_buf[h, c, i, block_of(hop)] = total[BLK * i:BLK * i + BLK]
        g_copy(h, c, hop).start()

    for h in range(GROUPS):
        for c in range(NCH):
            x_copy(3, h, c).wait_recv()
            keep_sum(h, c, x_send[3, h, c] + x_recv[3, h, c], 0)
        for c in range(NCH):
            y_copy(h, c, 0).wait_recv()
            y_copy(h, c, 1).wait_recv()
            keep_sum(h, c, y_recv[0, h, c] + y_recv[1, h, c], 2)
    st_copy(0).wait_recv()
    st_copy(2).wait_recv()
    st_ref[1] = st_buf[...].astype(BF16)

    @pl.when(k == 3)
    def _():
        for layer in range(NUM_LAYERS):
            for which in range(2):
                for src in range(3):
                    row_copy(which, layer, src).wait_recv()
        rows_ref[...] = row_buf[...]

    for h, c in chunks:
        g_copy(h, c, 0).wait_recv()
        g_copy(h, c, 2).wait_recv()
        hid_ref[GSTEPS * h:GSTEPS * h + GSTEPS, :, c * CW:(c + 1) * CW] = hid_buf[h, c]

    for h, c in chunks:
        for n in range(4):
            x_copy(n, h, c).wait_send()
        for hop in (0, 2):
            g_copy(h, c, hop).wait_send()
        for other in range(2):
            y_copy(h, c, other).wait_send()
    for f in range(2):
        for d in range(1, 4):
            rs_copy(f, d).wait_send()
    for hop in range(3):
        st_copy(hop).wait_send()

    @pl.when(k < 3)
    def _():
        for layer in range(NUM_LAYERS):
            for which in range(2):
                row_copy(which, layer).wait_send()


def layer_call(sums0, parts1, step_emb, b_in, taps, gain, b_out, state, long_filt, w_in, w_out, w_up, w_down):
    vm = pl.BlockSpec(memory_space=pltpu.VMEM)
    hbm = pl.BlockSpec(memory_space=pltpu.HBM)
    dma = pltpu.SemaphoreType.DMA
    return pl.pallas_call(
        layer_kernel,
        out_shape=(
            jax.ShapeDtypeStruct((NUM_STEPS, SEQ, DIM), F32),
            jax.ShapeDtypeStruct((NUM_LAYERS, SEQ, 3, 2, CH), BF16),
            jax.ShapeDtypeStruct((2, NUM_LAYERS, SEQ, NUM_STEPS, CH), F32),
        ),
        in_specs=[vm] * 14 + [hbm] * 5,
        out_specs=[vm] * 3,
        scratch_shapes=[
            pltpu.VMEM(w_in.shape, BF16),
            pltpu.VMEM(w_out.shape, BF16),
            pltpu.VMEM(w_up.shape, BF16),
            pltpu.VMEM(w_down.shape, BF16),
            pltpu.VMEM((GSTEPS, SEQ, DIM), F32),
            pltpu.VMEM((NUM_LAYERS, 2, 8, CH), F32),
            pltpu.VMEM((3, 2, NUM_STEPS, BLK, CH), F32),
            pltpu.VMEM((SEQ, 3, 2, CH), F32),
            pltpu.VMEM((4, GROUPS, NCH, GSTEPS * BLK, CW), F32),
            pltpu.VMEM((4, GROUPS, NCH, GSTEPS * BLK, CW), F32),
            pltpu.VMEM((2, GROUPS, NCH, GSTEPS * BLK, CW), F32),
            pltpu.VMEM((GROUPS, NCH, GSTEPS, SEQ, CW), F32),
            pltpu.VMEM((SEQ, 3, 2, CH), F32),
            pltpu.VMEM((2, NUM_LAYERS, SEQ, NUM_STEPS, CH), F32),
            dma((NUM_LAYERS, 4)),
            dma((1,)),
            dma((2, 3)),
            dma((2, 3)),
            dma((4, GROUPS, NCH)),
            dma((4, GROUPS, NCH)),
            dma((2, GROUPS, NCH)),
            dma((2, GROUPS, NCH)),
            dma((3,)),
            dma((3,)),
            dma((2, NUM_LAYERS)),
            dma((2, NUM_LAYERS, 4)),
            dma((GROUPS, NCH, 3)),
            dma((GROUPS, NCH, 3)),
        ],
        compiler_params=pltpu.CompilerParams(collective_id=0, has_side_effects=True, vmem_limit_bytes=44 << 20),
        name="layers",
    )(*sums0, *parts1, step_emb, b_in, taps, gain, b_out, state, long_filt, w_in, w_out, w_up, w_down)


def put_kernel(hid_in, st_in, rows_ref, v_in, z_in, hid_out, st_out, v_out, z_out, wide, tile, sems, o_sem):
    copies = [pltpu.make_async_copy(hid_in, hid_out, o_sem.at[0]), pltpu.make_async_copy(st_in, st_out, o_sem.at[1])]
    for copy in copies:
        copy.start()

    @pl.when(lax.axis_index("sp") == 3)
    def _():
        row_copies = []
        for which, dst in enumerate((v_out, z_out)):
            for layer in range(NUM_LAYERS):
                wide[:, 4:8, :] = jnp.zeros((SEQ, 4, CH), F32)
                wide[:, 0:4, :] = rows_ref[which, layer]
                tile[which, layer] = wide[...].astype(BF16)
                copy = pltpu.make_async_copy(tile.at[which, layer], dst.at[layer, :, 0:8, :], sems.at[which, layer])
                copy.start()
                row_copies.append(copy)
        for copy in row_copies:
            copy.wait()

    for copy in copies:
        copy.wait()


def put_call(hidden, states, rows, v_new, z_new):
    hbm = pl.BlockSpec(memory_space=pltpu.HBM)
    vm = pl.BlockSpec(memory_space=pltpu.VMEM)
    return pl.pallas_call(
        put_kernel,
        out_shape=(jax.ShapeDtypeStruct(hidden.shape, F32), jax.ShapeDtypeStruct(states.shape, BF16),
                   jax.ShapeDtypeStruct(v_new.shape, BF16), jax.ShapeDtypeStruct(z_new.shape, BF16)),
        in_specs=[vm] * 3 + [hbm] * 2,
        out_specs=[hbm] * 4,
        scratch_shapes=[
            pltpu.VMEM((SEQ, 8, CH), F32),
            pltpu.VMEM((2, NUM_LAYERS, SEQ, 8, CH), BF16),
            pltpu.SemaphoreType.DMA((2, NUM_LAYERS)),
            pltpu.SemaphoreType.DMA((2,)),
        ],
        input_output_aliases={3: 2, 4: 3},
        compiler_params=pltpu.CompilerParams(vmem_limit_bytes=16 << 20),
        name="put_rows",
    )(hidden, states, rows, v_new, z_new)


def solution(mesh):
    def device_fn(step_emb, v_cache, z_cache, short_state, w_in, b_in, short_taps, long_filt, skip_gain, w_out, b_out, w_up, w_down):
        v_cache, z_cache, long_filt, w_in, w_out, w_up, w_down = [
            pltpu.with_memory_space_constraint(x, pltpu.HBM)
            for x in (v_cache, z_cache, long_filt, jnp.transpose(w_in, (0, 2, 1, 3)), w_out, w_up, w_down)]
        v_new, z_new, *parts0, carry, rows_next = stream_call(0, v_cache, z_cache, long_filt)
        sums0 = [parts0[0]] + [lax.ppermute(parts0[d], "sp", [(i, (i + d) % 4) for i in range(4)]) for d in range(1, 4)]
        v_new, z_new, *parts1 = stream_call(1, v_cache, z_cache, v_new, z_new, carry, rows_next)
        hidden, states, rows = layer_call(
            sums0, parts1, step_emb, jnp.transpose(b_in, (1, 0, 2)), jnp.transpose(short_taps, (1, 2, 0, 3)),
            skip_gain, b_out, jnp.transpose(short_state, (0, 1, 3, 2, 4)), long_filt,
            w_in, w_out, w_up, w_down)
        hidden, states, v_new, z_new = put_call(hidden, states, rows, v_new, z_new)
        return hidden, v_new, z_new, jnp.transpose(states, (0, 1, 3, 2, 4))

    specs_in = (
        P(None, "dp", None),
        P(None, "dp", "sp", "tp"),
        P(None, "dp", "sp", "tp"),
        P(None, "dp", None, None, "tp"),
        P(None, None, None, "tp"),
        P(None, None, "tp"),
        P(None, None, None, "tp"),
        P(None, None, None, "tp"),
        P(None, None, "tp"),
        P(None, "tp", None),
        P(None, None),
        P(None, None, "tp"),
        P(None, "tp", None),
    )
    specs_out = (
        P(None, "dp", None),
        P(None, "dp", "sp", "tp"),
        P(None, "dp", "sp", "tp"),
        P(None, "dp", None, None, "tp"),
    )
    return jax.shard_map(device_fn, mesh=mesh, in_specs=specs_in, out_specs=specs_out, check_vma=False)
```

```python
import functools

import jax
import jax.numpy as jnp
from jax import lax
from jax.experimental import pallas as pl
from jax.experimental.pallas import tpu as pltpu
from jax.sharding import PartitionSpec as P

F32 = jnp.float32
BF16 = jnp.bfloat16
NUM_STEPS = 4
NUM_LAYERS = 2
SEQ = 32
BLK = 8
DIM = 1024
CH = 512
UP = 2048
SHARD = 256
NCH = 2
CW = DIM // NCH
GROUPS = 2
GSTEPS = NUM_STEPS // GROUPS
MESH = pl.DeviceIdType.MESH


def pair_rows(lo, hi, shift):
    clear = (lax.broadcasted_iota(jnp.int32, (8, 128), 0) // shift) % 2 == 0
    if shift == 4:
        return jnp.where(clear, lo, hi) + pltpu.roll(jnp.where(clear, hi, lo), 4, 0)
    return jnp.where(clear, lo + pltpu.roll(lo, 8 - shift, 0), hi + pltpu.roll(hi, shift, 0))


def fill_window(win, filt_rows, ct):
    flip = 7 - lax.broadcasted_iota(jnp.int32, (8, 128), 0)
    lanes = pl.ds(pl.multiple_of(ct * 128, 128), 128)
    for m in range(SHARD // 8 + 1):
        rows = filt_rows[SHARD - 8 * m:SHARD - 8 * m + 8, lanes]
        win[ct, 8 * m:8 * m + 8] = jnp.take_along_axis(rows, flip, axis=0)


def conv_block(src, win, dst, ready):
    @pl.loop(0, CH // 128)
    def _(ct):
        ready(ct)
        lanes = pl.ds(pl.multiple_of(ct * 128, 128), 128)
        half = []
        for seqs in ((0, 4, 1, 5), (2, 6, 3, 7)):
            accs = [[None] * NUM_STEPS for _ in seqs]
            for pt in range(SHARD // 16):
                w = [[win[ct, 16 * pt + 8 * h + 7 - j:16 * pt + 8 * h + 15 - j] for h in range(2)] for j in range(NUM_STEPS)]
                for i, b in enumerate(seqs):
                    x = src[b, 16 * pt:16 * pt + 16, lanes].astype(F32)
                    for j in range(NUM_STEPS):
                        for h in range(2):
                            term = x[8 * h:8 * h + 8] * w[j][h]
                            accs[i][j] = term if accs[i][j] is None else accs[i][j] + term
            half.append([[pair_rows(accs[0][j], accs[1][j], 4), pair_rows(accs[2][j], accs[3][j], 4)] for j in range(NUM_STEPS)])
        for j in range(NUM_STEPS):
            dst[j, :, lanes] = pair_rows(pair_rows(half[0][j][0], half[1][j][0], 2), pair_rows(half[0][j][1], half[1][j][1], 2), 1)


def stream_kernel(layer, num_in, *refs):
    v_in, z_in = refs[:2]
    if layer == 0:
        filt = refs[2]
        v_out, z_out, *parts, carry, rows_next = refs[num_in:num_in + 8]
        ring, win, in_sem, out_sem, rows, filt_sem, lane_sem, carry_sem = refs[num_in + 8:]
    else:
        carry, rows, w_in_hbm, w_out_hbm, filt = refs[4:9]
        v_out, z_out, *parts, w_in0, w_out0, lags = refs[num_in:num_in + 9]
        ring, win, in_sem, out_sem, carry_sem = refs[num_in + 9:]
    units = [(f, d) for f in range(2) for d in range(4)]
    k = lax.axis_index("sp")
    first = pl.multiple_of(jnp.maximum(2 - k, 0) * SHARD, SHARD)

    def seqs(u):
        return pl.ds(pl.multiple_of(lax.rem(k + units[u][1], 4) * BLK, BLK), BLK)

    def slot(u):
        return carry if layer == 1 and u == 0 else ring.at[u]

    def in_copy(u):
        return pltpu.make_async_copy((v_in, z_in)[units[u][0]].at[layer, seqs(u)], ring.at[u], in_sem.at[u])

    def lane_copy(ct):
        lanes = pl.ds(pl.multiple_of(ct * 128, 128), 128)
        return pltpu.make_async_copy(v_in.at[0, seqs(0), :, lanes], ring.at[0, :, :, lanes], lane_sem.at[ct])

    def out_copy(u):
        return pltpu.make_async_copy(slot(u), (v_out, z_out)[units[u][0]].at[layer, seqs(u)], out_sem.at[u])

    def filt_copy(f):
        return pltpu.make_async_copy(filt.at[0, f, pl.ds(first, SHARD + 8)], rows.at[f], filt_sem.at[f])

    def carry_copies():
        if layer == 1:
            return [pltpu.make_async_copy(w_in_hbm.at[0], w_in0, carry_sem.at[0]),
                    pltpu.make_async_copy(w_out_hbm.at[0], w_out0, carry_sem.at[1]),
                    pltpu.make_async_copy(filt.at[:, :, 0:8], lags, carry_sem.at[2])]
        return [pltpu.make_async_copy(v_in.at[1, seqs(0)], carry, carry_sem.at[2])] + [
            pltpu.make_async_copy(filt.at[1, f, pl.ds(first, SHARD + 8)], rows_next.at[f], carry_sem.at[f]) for f in range(2)]

    reads = {0: (2,), 1: (3, 4), 2: (5, 6), 3: (7,)}
    writes = {3: (0, 1), 4: (2, 3), 5: (4, 5), 6: (6, 7)}
    if layer == 0:
        filt_copy(0).start()
        for ct in range(CH // 128):
            lane_copy(ct).start()
        filt_copy(0).wait()
    in_copy(1).start()
    for u, (f, d) in enumerate(units):
        if 0 < u < 7:
            in_copy(u).wait()
        if u == 6:
            in_copy(7).wait()
        for nxt in reads.get(u, ()):
            in_copy(nxt).start()
        for nxt in writes.get(u, ()):
            out_copy(nxt).start()
        if layer == 0 and u == 1:
            filt_copy(1).start()
        if layer == 0 and u == 4:
            filt_copy(1).wait()
        if u == (5 if layer == 0 else 4):
            for copy in carry_copies():
                copy.start()

        def ready(ct, u=u, f=f, d=d):
            if d == 0:
                fill_window(win, rows.at[f], ct)
            if layer == 0 and u == 0:
                lane_copy(ct).wait()

        conv_block(slot(u), win, parts[d].at[f], ready)
    for u in range(len(units)):
        out_copy(u).wait()
    for copy in carry_copies():
        copy.wait()


def stream_call(layer, *operands):
    hbm = pl.BlockSpec(memory_space=pltpu.HBM)
    vm = pl.BlockSpec(memory_space=pltpu.VMEM)
    cache = jax.ShapeDtypeStruct(operands[0].shape, BF16)
    outs = (cache, cache) + (jax.ShapeDtypeStruct((2, NUM_STEPS, BLK, CH), F32),) * 4
    scratch = [
        pltpu.VMEM((8, BLK, SHARD, CH), BF16),
        pltpu.VMEM((CH // 128, SHARD + 8, 128), F32),
        pltpu.SemaphoreType.DMA((8,)),
        pltpu.SemaphoreType.DMA((8,)),
    ]
    if layer == 0:
        in_specs = [hbm] * 3
        outs += (jax.ShapeDtypeStruct((BLK, SHARD, CH), BF16), jax.ShapeDtypeStruct((2, SHARD + 8, CH), F32))
        scratch += [
            pltpu.VMEM((2, SHARD + 8, CH), F32),
            pltpu.SemaphoreType.DMA((2,)),
            pltpu.SemaphoreType.DMA((CH // 128,)),
            pltpu.SemaphoreType.DMA((3,)),
        ]
    else:
        in_specs = [hbm] * 4 + [vm] * 2 + [hbm] * 3
        outs += (jax.ShapeDtypeStruct((3, DIM, CH), BF16), jax.ShapeDtypeStruct((CH, DIM), BF16),
                 jax.ShapeDtypeStruct((NUM_LAYERS, 2, 8, CH), F32))
        scratch += [pltpu.SemaphoreType.DMA((3,))]
    return pl.pallas_call(
        functools.partial(stream_kernel, layer, len(operands)),
        out_shape=outs,
        in_specs=in_specs,
        out_specs=[hbm] * 2 + [vm] * (len(outs) - 2),
        scratch_shapes=scratch,
        input_output_aliases={} if layer == 0 else {2: 0, 3: 1},
        cost_estimate=pl.CostEstimate(flops=SEQ * SHARD * CH * 16, bytes_accessed=4 * SEQ * SHARD * CH * 2, transcendentals=0),
        compiler_params=pltpu.CompilerParams(vmem_limit_bytes=30 << 20),
        name=f"stream_{layer}",
    )(*operands)


def norm_rows(rows_in):
    mean_val = jnp.mean(rows_in, axis=-1, keepdims=True)
    centered = rows_in - mean_val
    var_val = jnp.mean(centered * centered, axis=-1, keepdims=True)
    return centered * lax.rsqrt(var_val + 1e-5)


def round_bf16(x):
    return x.astype(BF16).astype(F32)


def layer_kernel(*refs):
    sums0 = refs[:4]
    parts1 = refs[4:8]
    (emb_ref, b_in_ref, taps_ref, gain_ref, b_out_ref, state, w_in0, w_out0, lags, w_in_hbm, w_out_hbm, w_up_hbm, w_down_hbm,
     hid_ref, st_ref, rows_ref,
     w_in, w_out, w_up, w_down, emb32, rs_buf, st0_buf, x_send, x_recv, y_recv, hid_buf, st_buf, row_buf,
     w_sem, rs_send, rs_recv, x_ssem, x_rsem, y_ssem, y_rsem, st_ssem, st_rsem, row_ssem, row_rsem, g_ssem, g_rsem) = refs[8:]
    k = lax.axis_index("sp")
    t = lax.axis_index("tp")
    others = [lax.rem(k + d, 4) for d in range(1, 4)]
    mate = k + 1 - 2 * lax.rem(k, 2)
    across = lax.rem(k + 2, 4)
    own = pl.ds(pl.multiple_of(k * BLK, BLK), BLK)

    w_pairs = ((w_in_hbm, w_in), (w_out_hbm, w_out), (w_up_hbm, w_up), (w_down_hbm, w_down))
    w_copies = [None if layer == 0 and idx < 2 else
                pltpu.make_async_copy(src.at[layer], dst if idx < 2 else dst.at[layer], w_sem.at[layer, idx])
                for layer in range(NUM_LAYERS) for idx, (src, dst) in enumerate(w_pairs)]
    w_copies[2].start()

    barrier = pltpu.get_barrier_semaphore()
    for dev in others:
        pl.semaphore_signal(barrier, inc=1, device_id={"sp": dev}, device_id_type=MESH)
    pl.semaphore_signal(barrier, inc=1, device_id={"tp": 1 - t}, device_id_type=MESH)
    pl.semaphore_signal(barrier, inc=1, device_id={"sp": across, "tp": 1 - t}, device_id_type=MESH)
    pl.semaphore_wait(barrier, 5)

    def rs_copy(f, d):
        return pltpu.make_async_remote_copy(
            src_ref=parts1[d].at[f], dst_ref=rs_buf.at[d - 1, f], send_sem=rs_send.at[f, d - 1], recv_sem=rs_recv.at[f, d - 1],
            device_id={"sp": others[d - 1]}, device_id_type=MESH)

    def cached_sum(layer, f, j):
        if layer == 0:
            return (sums0[0][f, j] + sums0[1][f, j]) + (sums0[2][f, j] + sums0[3][f, j])
        return (parts1[0][f, j] + rs_buf[0, f, j]) + (rs_buf[1, f, j] + rs_buf[2, f, j])

    def x_copy(n, h, c):
        return pltpu.make_async_remote_copy(
            src_ref=x_send.at[n, h, c], dst_ref=x_recv.at[n, h, c], send_sem=x_ssem.at[n, h, c], recv_sem=x_rsem.at[n, h, c],
            device_id={"tp": 1 - t}, device_id_type=MESH)

    def row_copy(which, layer, src=None):
        piece = row_buf.at[which, layer, own if src is None else pl.ds(src * BLK, BLK)]
        return pltpu.make_async_remote_copy(
            src_ref=piece, dst_ref=piece, send_sem=row_ssem.at[which, layer],
            recv_sem=row_rsem.at[which, layer, k if src is None else src],
            device_id={"sp": 3}, device_id_type=MESH)

    def block_of(hop):
        return pl.ds(pl.multiple_of((k if hop < 2 else across) * BLK, BLK), BLK)

    def st_copy(hop):
        piece = st_buf.at[block_of(hop)]
        return pltpu.make_async_remote_copy(
            src_ref=piece, dst_ref=piece, send_sem=st_ssem.at[hop], recv_sem=st_rsem.at[hop],
            device_id={"sp": across if hop == 1 else mate}, device_id_type=MESH)

    def keep_rows(which, layer, vals):
        for b in range(BLK):
            for j in range(NUM_STEPS):
                row_buf[which, layer, k * BLK + b, j:j + 1, :] = vals[j][b:b + 1]

        @pl.when(k < 3)
        def _():
            row_copy(which, layer).start()

    def long_conv(layer, f, j, vals):
        acc = cached_sum(layer, f, j)
        for i in range(j + 1):
            acc = acc + lags[layer, f, j - i:j - i + 1] * vals[i]
        return acc + gain_ref[layer, f:f + 1] * vals[j]

    proj_rows = [[None] * 3 for _ in range(NUM_LAYERS)]
    v_rows = [[], []]
    z_rows = [[], []]

    def y_copy(h, c, other):
        return pltpu.make_async_remote_copy(
            src_ref=x_send.at[3, h, c], dst_ref=y_recv.at[other, h, c], send_sem=y_ssem.at[other, h, c], recv_sem=y_rsem.at[other, h, c],
            device_id={"sp": across, "tp": (1 - t) if other else t}, device_id_type=MESH)

    def matmul_exchange(n, h, lhs, w_ref, base=None):
        for c in range(NCH):
            part = jnp.dot(lhs, w_ref[:, c * CW:(c + 1) * CW], preferred_element_type=F32)
            if base is not None:
                part = part + jnp.where(t == 0, base[:, c * CW:(c + 1) * CW], 0.0)
            x_send[n, h, c] = part
            if base is not None:
                y_copy(h, c, 1).start()
                y_copy(h, c, 0).start()
            x_copy(n, h, c).start()

    def add_exchange(n, h, base):
        outs = []
        for c in range(NCH):
            x_copy(n, h, c).wait_recv()
            outs.append(base[:, c * CW:(c + 1) * CW] + (x_send[n, h, c] + x_recv[n, h, c]))
        return jnp.concatenate(outs, axis=1)

    def front(layer, h, rows_in):
        normed = norm_rows(rows_in).astype(BF16)
        if layer == 1 and h == 0:
            w_copies[4].wait()
        mixed = []
        for g in range(3):
            proj = jnp.dot(normed, (w_in0 if layer == 0 else w_in)[g], preferred_element_type=F32) + b_in_ref[g, layer:layer + 1]
            proj = round_bf16(proj)
            if h == 0:
                proj_rows[layer][g] = [
                    jnp.concatenate([state[layer, k * BLK + b, g, s:s + 1].astype(F32) for b in range(BLK)], axis=0) for s in range(2)]
            seq = proj_rows[layer][g]
            seq += [proj[BLK * i:BLK * i + BLK] for i in range(GSTEPS)]
            tap = [taps_ref[i, g, layer:layer + 1] for i in range(3)]
            mixed.append([tap[0] * seq[j + 2] + tap[1] * seq[j + 1] + tap[2] * seq[j] for j in range(GSTEPS * h, GSTEPS * h + GSTEPS)])
        ys = []
        v_rows[layer] += [round_bf16(x) for x in mixed[2]]
        if layer == 1 and h == 0:
            for f in range(2):
                for d in range(1, 4):
                    rs_copy(f, d).wait_recv()
        for i in range(GSTEPS):
            a = long_conv(layer, 0, GSTEPS * h + i, v_rows[layer])
            z_rows[layer].append(round_bf16(mixed[0][i] * a))
            ys.append(mixed[1][i] * long_conv(layer, 1, GSTEPS * h + i, z_rows[layer]))
        if layer == 1 and h == 0:
            w_copies[5].wait()
        matmul_exchange(layer * 2, h, jnp.concatenate(ys, axis=0).astype(BF16), w_out0 if layer == 0 else w_out)

    def send_kept(layer):
        keep_rows(0, layer, v_rows[layer])
        keep_rows(1, layer, z_rows[layer])
    def middle(layer, h, rows_in):
        out = add_exchange(layer * 2, h, rows_in) + b_out_ref[layer:layer + 1]
        act = norm_rows(out).astype(BF16)
        if h == 0:
            w_copies[layer * 4 + 2].wait()
        inner = jax.nn.gelu(jnp.dot(act, w_up[layer], preferred_element_type=F32)).astype(BF16)
        if h == 0:
            w_copies[layer * 4 + 3].wait()
        matmul_exchange(layer * 2 + 1, h, inner, w_down.at[layer], out if layer == 1 else None)
        return out

    rows_in = []
    for h in range(GROUPS):
        emb32[...] = emb_ref[GSTEPS * h:GSTEPS * h + GSTEPS].astype(F32)
        rows_in.append(jnp.concatenate([emb32[i, own] for i in range(GSTEPS)], axis=0))
    for h in range(GROUPS):
        front(0, h, rows_in[h])
        if h == 0:
            w_copies[3].start()
    for copy in w_copies[4:6]:
        copy.start()
    for f in range(2):
        for d in range(1, 4):
            rs_copy(f, d).start()
    send_kept(0)
    outs = [middle(0, h, rows_in[h]) for h in range(GROUPS)]
    for copy in w_copies[6:8]:
        copy.start()

    normed = norm_rows(emb_ref[2:4].astype(F32).reshape(2 * SEQ, DIM)).astype(BF16)
    for g in range(3):
        proj = jnp.dot(normed, w_in0[g], preferred_element_type=F32) + b_in_ref[g, 0:1]
        for s in range(2):
            for b in range(SEQ):
                st0_buf[b, g, s:s + 1, :] = proj[s * SEQ + b:s * SEQ + b + 1]
    st_ref[0] = st0_buf[...].astype(BF16)

    rows_in = []
    for h in range(GROUPS):
        rows_in.append(add_exchange(1, h, outs[h]))
        front(1, h, rows_in[h])
    for g in range(3):
        for s in range(2):
            for i in range(BLK):
                st_buf[k * BLK + i, g, s:s + 1, :] = proj_rows[1][g][4 + s][i:i + 1]
    st_copy(1).start()
    st_copy(0).start()
    send_kept(1)
    outs = [middle(1, h, rows_in[h]) for h in range(GROUPS)]
    st_copy(1).wait_recv()
    st_copy(2).start()

    def g_copy(h, c, hop):
        piece = hid_buf.at[h, c, :, block_of(hop)]
        return pltpu.make_async_remote_copy(
            src_ref=piece, dst_ref=piece, send_sem=g_ssem.at[h, c, hop], recv_sem=g_rsem.at[h, c, hop],
            device_id={"sp": across if hop == 1 else mate}, device_id_type=MESH)

    chunks = [(h, c) for h in range(GROUPS) for c in range(NCH)]
    def keep_sum(h, c, total, hop):
        for i in range(GSTEPS):
            hid_buf[h, c, i, block_of(hop)] = total[BLK * i:BLK * i + BLK]
        g_copy(h, c, hop).start()

    for h in range(GROUPS):
        for c in range(NCH):
            x_copy(3, h, c).wait_recv()
            keep_sum(h, c, x_send[3, h, c] + x_recv[3, h, c], 0)
        for c in range(NCH):
            y_copy(h, c, 0).wait_recv()
            y_copy(h, c, 1).wait_recv()
            keep_sum(h, c, y_recv[0, h, c] + y_recv[1, h, c], 2)
    st_copy(0).wait_recv()
    st_copy(2).wait_recv()
    st_ref[1] = st_buf[...].astype(BF16)

    @pl.when(k == 3)
    def _():
        for layer in range(NUM_LAYERS):
            for which in range(2):
                for src in range(3):
                    row_copy(which, layer, src).wait_recv()
        rows_ref[...] = row_buf[...]

    for h, c in chunks:
        g_copy(h, c, 0).wait_recv()
        g_copy(h, c, 2).wait_recv()
        hid_ref[GSTEPS * h:GSTEPS * h + GSTEPS, :, c * CW:(c + 1) * CW] = hid_buf[h, c]

    for h, c in chunks:
        for n in range(4):
            x_copy(n, h, c).wait_send()
        for hop in (0, 2):
            g_copy(h, c, hop).wait_send()
        for other in range(2):
            y_copy(h, c, other).wait_send()
    for f in range(2):
        for d in range(1, 4):
            rs_copy(f, d).wait_send()
    for hop in range(3):
        st_copy(hop).wait_send()

    @pl.when(k < 3)
    def _():
        for layer in range(NUM_LAYERS):
            for which in range(2):
                row_copy(which, layer).wait_send()


def layer_call(sums0, parts1, step_emb, b_in, taps, gain, b_out, state, w_in0, w_out0, lags, w_in, w_out, w_up, w_down):
    vm = pl.BlockSpec(memory_space=pltpu.VMEM)
    hbm = pl.BlockSpec(memory_space=pltpu.HBM)
    dma = pltpu.SemaphoreType.DMA
    return pl.pallas_call(
        layer_kernel,
        out_shape=(
            jax.ShapeDtypeStruct((NUM_STEPS, SEQ, DIM), F32),
            jax.ShapeDtypeStruct((NUM_LAYERS, SEQ, 3, 2, CH), BF16),
            jax.ShapeDtypeStruct((2, NUM_LAYERS, SEQ, NUM_STEPS, CH), F32),
        ),
        in_specs=[vm] * 17 + [hbm] * 4,
        out_specs=[vm] * 3,
        scratch_shapes=[
            pltpu.VMEM(w_in.shape[1:], BF16),
            pltpu.VMEM(w_out.shape[1:], BF16),
            pltpu.VMEM(w_up.shape, BF16),
            pltpu.VMEM(w_down.shape, BF16),
            pltpu.VMEM((GSTEPS, SEQ, DIM), F32),
            pltpu.VMEM((3, 2, NUM_STEPS, BLK, CH), F32),
            pltpu.VMEM((SEQ, 3, 2, CH), F32),
            pltpu.VMEM((4, GROUPS, NCH, GSTEPS * BLK, CW), F32),
            pltpu.VMEM((4, GROUPS, NCH, GSTEPS * BLK, CW), F32),
            pltpu.VMEM((2, GROUPS, NCH, GSTEPS * BLK, CW), F32),
            pltpu.VMEM((GROUPS, NCH, GSTEPS, SEQ, CW), F32),
            pltpu.VMEM((SEQ, 3, 2, CH), F32),
            pltpu.VMEM((2, NUM_LAYERS, SEQ, NUM_STEPS, CH), F32),
            dma((NUM_LAYERS, 4)),
            dma((2, 3)),
            dma((2, 3)),
            dma((4, GROUPS, NCH)),
            dma((4, GROUPS, NCH)),
            dma((2, GROUPS, NCH)),
            dma((2, GROUPS, NCH)),
            dma((3,)),
            dma((3,)),
            dma((2, NUM_LAYERS)),
            dma((2, NUM_LAYERS, 4)),
            dma((GROUPS, NCH, 3)),
            dma((GROUPS, NCH, 3)),
        ],
        compiler_params=pltpu.CompilerParams(collective_id=0, has_side_effects=True, vmem_limit_bytes=44 << 20),
        name="layers",
    )(*sums0, *parts1, step_emb, b_in, taps, gain, b_out, state, w_in0, w_out0, lags, w_in, w_out, w_up, w_down)


def put_kernel(hid_in, st_in, rows_ref, v_in, z_in, hid_out, st_out, v_out, z_out, wide, tile, sems, o_sem):
    copies = [pltpu.make_async_copy(hid_in, hid_out, o_sem.at[0]), pltpu.make_async_copy(st_in, st_out, o_sem.at[1])]
    for copy in copies:
        copy.start()

    @pl.when(lax.axis_index("sp") == 3)
    def _():
        row_copies = []
        for which, dst in enumerate((v_out, z_out)):
            for layer in range(NUM_LAYERS):
                wide[:, 4:8, :] = jnp.zeros((SEQ, 4, CH), F32)
                wide[:, 0:4, :] = rows_ref[which, layer]
                tile[which, layer] = wide[...].astype(BF16)
                copy = pltpu.make_async_copy(tile.at[which, layer], dst.at[layer, :, 0:8, :], sems.at[which, layer])
                copy.start()
                row_copies.append(copy)
        for copy in row_copies:
            copy.wait()

    for copy in copies:
        copy.wait()


def put_call(hidden, states, rows, v_new, z_new):
    hbm = pl.BlockSpec(memory_space=pltpu.HBM)
    vm = pl.BlockSpec(memory_space=pltpu.VMEM)
    return pl.pallas_call(
        put_kernel,
        out_shape=(jax.ShapeDtypeStruct(hidden.shape, F32), jax.ShapeDtypeStruct(states.shape, BF16),
                   jax.ShapeDtypeStruct(v_new.shape, BF16), jax.ShapeDtypeStruct(z_new.shape, BF16)),
        in_specs=[vm] * 3 + [hbm] * 2,
        out_specs=[hbm] * 4,
        scratch_shapes=[
            pltpu.VMEM((SEQ, 8, CH), F32),
            pltpu.VMEM((2, NUM_LAYERS, SEQ, 8, CH), BF16),
            pltpu.SemaphoreType.DMA((2, NUM_LAYERS)),
            pltpu.SemaphoreType.DMA((2,)),
        ],
        input_output_aliases={3: 2, 4: 3},
        compiler_params=pltpu.CompilerParams(vmem_limit_bytes=16 << 20),
        name="put_rows",
    )(hidden, states, rows, v_new, z_new)


def solution(mesh):
    def device_fn(step_emb, v_cache, z_cache, short_state, w_in, b_in, short_taps, long_filt, skip_gain, w_out, b_out, w_up, w_down):
        v_cache, z_cache, long_filt, w_in, w_out, w_up, w_down = [
            pltpu.with_memory_space_constraint(x, pltpu.HBM)
            for x in (v_cache, z_cache, long_filt, jnp.transpose(w_in, (0, 2, 1, 3)), w_out, w_up, w_down)]
        v_new, z_new, *parts0, carry, rows_next = stream_call(0, v_cache, z_cache, long_filt)
        sums0 = [parts0[0]] + [lax.ppermute(parts0[d], "sp", [(i, (i + d) % 4) for i in range(4)]) for d in range(1, 4)]
        v_new, z_new, *parts1, w_in0, w_out0, lags = stream_call(1, v_cache, z_cache, v_new, z_new, carry, rows_next, w_in, w_out, long_filt)
        hidden, states, rows = layer_call(
            sums0, parts1, step_emb, jnp.transpose(b_in, (1, 0, 2)), jnp.transpose(short_taps, (1, 2, 0, 3)),
            skip_gain, b_out, jnp.transpose(short_state, (0, 1, 3, 2, 4)), w_in0, w_out0, lags,
            w_in, w_out, w_up, w_down)
        hidden, states, v_new, z_new = put_call(hidden, states, rows, v_new, z_new)
        return hidden, v_new, z_new, jnp.transpose(states, (0, 1, 3, 2, 4))

    specs_in = (
        P(None, "dp", None),
        P(None, "dp", "sp", "tp"),
        P(None, "dp", "sp", "tp"),
        P(None, "dp", None, None, "tp"),
        P(None, None, None, "tp"),
        P(None, None, "tp"),
        P(None, None, None, "tp"),
        P(None, None, None, "tp"),
        P(None, None, "tp"),
        P(None, "tp", None),
        P(None, None),
        P(None, None, "tp"),
        P(None, "tp", None),
    )
    specs_out = (
        P(None, "dp", None),
        P(None, "dp", "sp", "tp"),
        P(None, "dp", "sp", "tp"),
        P(None, "dp", None, None, "tp"),
    )
    return jax.shard_map(device_fn, mesh=mesh, in_specs=specs_in, out_specs=specs_out, check_vma=False)
```

```python
import functools

import jax
import jax.numpy as jnp
from jax import lax
from jax.experimental import pallas as pl
from jax.experimental.pallas import tpu as pltpu
from jax.sharding import PartitionSpec as P

F32 = jnp.float32
BF16 = jnp.bfloat16
NUM_STEPS = 4
NUM_LAYERS = 2
SEQ = 32
BLK = 8
DIM = 1024
CH = 512
UP = 2048
SHARD = 256
NCH = 2
CW = DIM // NCH
GROUPS = 2
GSTEPS = NUM_STEPS // GROUPS
MESH = pl.DeviceIdType.MESH


def pair_rows(lo, hi, shift):
    clear = (lax.broadcasted_iota(jnp.int32, (8, 128), 0) // shift) % 2 == 0
    if shift == 4:
        return jnp.where(clear, lo, hi) + pltpu.roll(jnp.where(clear, hi, lo), 4, 0)
    return jnp.where(clear, lo + pltpu.roll(lo, 8 - shift, 0), hi + pltpu.roll(hi, shift, 0))


def fill_window(win, filt_rows, ct):
    flip = 7 - lax.broadcasted_iota(jnp.int32, (8, 128), 0)
    lanes = pl.ds(pl.multiple_of(ct * 128, 128), 128)
    for m in range(SHARD // 8 + 1):
        rows = filt_rows[SHARD - 8 * m:SHARD - 8 * m + 8, lanes]
        win[ct, 8 * m:8 * m + 8] = jnp.take_along_axis(rows, flip, axis=0)


def conv_block(src, win, dst, ready):
    @pl.loop(0, CH // 128)
    def _(ct):
        ready(ct)
        lanes = pl.ds(pl.multiple_of(ct * 128, 128), 128)
        half = []
        for seqs in ((0, 4, 1, 5), (2, 6, 3, 7)):
            accs = [[None] * NUM_STEPS for _ in seqs]
            for pt in range(SHARD // 16):
                w = [[win[ct, 16 * pt + 8 * h + 7 - j:16 * pt + 8 * h + 15 - j] for h in range(2)] for j in range(NUM_STEPS)]
                for i, b in enumerate(seqs):
                    x = src[b, 16 * pt:16 * pt + 16, lanes].astype(F32)
                    for j in range(NUM_STEPS):
                        for h in range(2):
                            term = x[8 * h:8 * h + 8] * w[j][h]
                            accs[i][j] = term if accs[i][j] is None else accs[i][j] + term
            half.append([[pair_rows(accs[0][j], accs[1][j], 4), pair_rows(accs[2][j], accs[3][j], 4)] for j in range(NUM_STEPS)])
        for j in range(NUM_STEPS):
            dst[j, :, lanes] = pair_rows(pair_rows(half[0][j][0], half[1][j][0], 2), pair_rows(half[0][j][1], half[1][j][1], 2), 1)


def stream_kernel(layer, num_in, *refs):
    v_in, z_in = refs[:2]
    if layer == 0:
        filt = refs[2]
        v_out, z_out, *parts, carry, rows_next = refs[num_in:num_in + 8]
        ring, win, in_sem, out_sem, rows, filt_sem, lane_sem, carry_sem = refs[num_in + 8:]
    else:
        carry, rows, w_in_hbm, w_out_hbm, filt = refs[4:9]
        v_out, z_out, *parts, w_in0, w_out0, lags = refs[num_in:num_in + 9]
        ring, win, in_sem, out_sem, carry_sem = refs[num_in + 9:]
    units = [(f, d) for f in range(2) for d in range(4)]
    k = lax.axis_index("sp")
    first = pl.multiple_of(jnp.maximum(2 - k, 0) * SHARD, SHARD)

    def seqs(u):
        return pl.ds(pl.multiple_of(lax.rem(k + units[u][1], 4) * BLK, BLK), BLK)

    def slot(u):
        return carry if layer == 1 and u == 0 else ring.at[u]

    def in_copy(u):
        return pltpu.make_async_copy((v_in, z_in)[units[u][0]].at[layer, seqs(u)], ring.at[u], in_sem.at[u])

    def lane_copy(ct):
        lanes = pl.ds(pl.multiple_of(ct * 128, 128), 128)
        return pltpu.make_async_copy(v_in.at[0, seqs(0), :, lanes], ring.at[0, :, :, lanes], lane_sem.at[ct])

    def out_copy(u):
        return pltpu.make_async_copy(slot(u), (v_out, z_out)[units[u][0]].at[layer, seqs(u)], out_sem.at[u])

    def filt_copy(f):
        return pltpu.make_async_copy(filt.at[0, f, pl.ds(first, SHARD + 8)], rows.at[f], filt_sem.at[f])

    def carry_copies():
        if layer == 1:
            return [pltpu.make_async_copy(w_in_hbm.at[0], w_in0, carry_sem.at[0]),
                    pltpu.make_async_copy(w_out_hbm.at[0], w_out0, carry_sem.at[1]),
                    pltpu.make_async_copy(filt.at[:, :, 0:8], lags, carry_sem.at[2])]
        return [pltpu.make_async_copy(v_in.at[1, seqs(0)], carry, carry_sem.at[2])] + [
            pltpu.make_async_copy(filt.at[1, f, pl.ds(first, SHARD + 8)], rows_next.at[f], carry_sem.at[f]) for f in range(2)]

    reads = {0: (2,), 1: (3, 4), 2: (5, 6), 3: (7,)}
    writes = {3: (0, 1), 4: (2, 3), 5: (4, 5), 6: (6, 7)}
    if layer == 0:
        filt_copy(0).start()
        for ct in range(CH // 128):
            lane_copy(ct).start()
        filt_copy(0).wait()
    in_copy(1).start()
    for u, (f, d) in enumerate(units):
        if 0 < u < 7:
            in_copy(u).wait()
        if u == 6:
            in_copy(7).wait()
        if layer == 0 or u > 0:
            for nxt in reads.get(u, ()):
                in_copy(nxt).start()
        for nxt in writes.get(u, ()):
            out_copy(nxt).start()
        if layer == 0 and u == 1:
            filt_copy(1).start()
        if layer == 0 and u == 4:
            filt_copy(1).wait()
        if u == (5 if layer == 0 else 4):
            for copy in carry_copies():
                copy.start()

        def ready(ct, u=u, f=f, d=d):
            if d == 0:
                fill_window(win, rows.at[f], ct)
            if layer == 0 and u == 0:
                lane_copy(ct).wait()
            if layer == 1 and u == 0:
                @pl.when(ct == 1)
                def _():
                    in_copy(2).start()

        conv_block(slot(u), win, parts[d].at[f], ready)
    for u in range(len(units)):
        out_copy(u).wait()
    for copy in carry_copies():
        copy.wait()


def stream_call(layer, *operands):
    hbm = pl.BlockSpec(memory_space=pltpu.HBM)
    vm = pl.BlockSpec(memory_space=pltpu.VMEM)
    cache = jax.ShapeDtypeStruct(operands[0].shape, BF16)
    outs = (cache, cache) + (jax.ShapeDtypeStruct((2, NUM_STEPS, BLK, CH), F32),) * 4
    scratch = [
        pltpu.VMEM((8, BLK, SHARD, CH), BF16),
        pltpu.VMEM((CH // 128, SHARD + 8, 128), F32),
        pltpu.SemaphoreType.DMA((8,)),
        pltpu.SemaphoreType.DMA((8,)),
    ]
    if layer == 0:
        in_specs = [hbm] * 3
        outs += (jax.ShapeDtypeStruct((BLK, SHARD, CH), BF16), jax.ShapeDtypeStruct((2, SHARD + 8, CH), F32))
        scratch += [
            pltpu.VMEM((2, SHARD + 8, CH), F32),
            pltpu.SemaphoreType.DMA((2,)),
            pltpu.SemaphoreType.DMA((CH // 128,)),
            pltpu.SemaphoreType.DMA((3,)),
        ]
    else:
        in_specs = [hbm] * 4 + [vm] * 2 + [hbm] * 3
        outs += (jax.ShapeDtypeStruct((3, DIM, CH), BF16), jax.ShapeDtypeStruct((CH, DIM), BF16),
                 jax.ShapeDtypeStruct((NUM_LAYERS, 2, 8, CH), F32))
        scratch += [pltpu.SemaphoreType.DMA((3,))]
    return pl.pallas_call(
        functools.partial(stream_kernel, layer, len(operands)),
        out_shape=outs,
        in_specs=in_specs,
        out_specs=[hbm] * 2 + [vm] * (len(outs) - 2),
        scratch_shapes=scratch,
        input_output_aliases={} if layer == 0 else {2: 0, 3: 1},
        cost_estimate=pl.CostEstimate(flops=SEQ * SHARD * CH * 16, bytes_accessed=4 * SEQ * SHARD * CH * 2, transcendentals=0),
        compiler_params=pltpu.CompilerParams(vmem_limit_bytes=30 << 20),
        name=f"stream_{layer}",
    )(*operands)


def norm_rows(rows_in):
    mean_val = jnp.mean(rows_in, axis=-1, keepdims=True)
    centered = rows_in - mean_val
    var_val = jnp.mean(centered * centered, axis=-1, keepdims=True)
    return centered * lax.rsqrt(var_val + 1e-5)


def round_bf16(x):
    return x.astype(BF16).astype(F32)


def layer_kernel(*refs):
    sums0 = refs[:4]
    parts1 = refs[4:8]
    (emb_ref, b_in_ref, taps_ref, gain_ref, b_out_ref, state, w_in0, w_out0, lags, w_in_hbm, w_out_hbm, w_up_hbm, w_down_hbm,
     hid_ref, st_ref, rows_ref,
     w_in, w_out, w_up, w_down, emb32, rs_buf, st0_buf, x_send, x_recv, y_recv, hid_buf, st_buf, row_buf,
     w_sem, rs_send, rs_recv, x_ssem, x_rsem, y_ssem, y_rsem, st_ssem, st_rsem, row_ssem, row_rsem, g_ssem, g_rsem) = refs[8:]
    k = lax.axis_index("sp")
    t = lax.axis_index("tp")
    others = [lax.rem(k + d, 4) for d in range(1, 4)]
    mate = k + 1 - 2 * lax.rem(k, 2)
    across = lax.rem(k + 2, 4)
    own = pl.ds(pl.multiple_of(k * BLK, BLK), BLK)

    w_pairs = ((w_in_hbm, w_in), (w_out_hbm, w_out), (w_up_hbm, w_up), (w_down_hbm, w_down))
    w_copies = [None if layer == 0 and idx < 2 else
                pltpu.make_async_copy(src.at[layer], dst if idx < 2 else dst.at[layer], w_sem.at[layer, idx])
                for layer in range(NUM_LAYERS) for idx, (src, dst) in enumerate(w_pairs)]
    w_copies[2].start()

    barrier = pltpu.get_barrier_semaphore()
    for dev in others:
        pl.semaphore_signal(barrier, inc=1, device_id={"sp": dev}, device_id_type=MESH)
    pl.semaphore_signal(barrier, inc=1, device_id={"tp": 1 - t}, device_id_type=MESH)
    pl.semaphore_signal(barrier, inc=1, device_id={"sp": across, "tp": 1 - t}, device_id_type=MESH)
    pl.semaphore_wait(barrier, 5)

    def rs_copy(f, d):
        return pltpu.make_async_remote_copy(
            src_ref=parts1[d].at[f], dst_ref=rs_buf.at[d - 1, f], send_sem=rs_send.at[f, d - 1], recv_sem=rs_recv.at[f, d - 1],
            device_id={"sp": others[d - 1]}, device_id_type=MESH)

    def cached_sum(layer, f, j):
        if layer == 0:
            return (sums0[0][f, j] + sums0[1][f, j]) + (sums0[2][f, j] + sums0[3][f, j])
        return (parts1[0][f, j] + rs_buf[0, f, j]) + (rs_buf[1, f, j] + rs_buf[2, f, j])

    def x_copy(n, h, c):
        return pltpu.make_async_remote_copy(
            src_ref=x_send.at[n, h, c], dst_ref=x_recv.at[n, h, c], send_sem=x_ssem.at[n, h, c], recv_sem=x_rsem.at[n, h, c],
            device_id={"tp": 1 - t}, device_id_type=MESH)

    def row_copy(which, layer, src=None):
        piece = row_buf.at[which, layer, own if src is None else pl.ds(src * BLK, BLK)]
        return pltpu.make_async_remote_copy(
            src_ref=piece, dst_ref=piece, send_sem=row_ssem.at[which, layer],
            recv_sem=row_rsem.at[which, layer, k if src is None else src],
            device_id={"sp": 3}, device_id_type=MESH)

    def block_of(hop):
        return pl.ds(pl.multiple_of((k if hop < 2 else across) * BLK, BLK), BLK)

    def st_copy(hop):
        piece = st_buf.at[block_of(hop)]
        return pltpu.make_async_remote_copy(
            src_ref=piece, dst_ref=piece, send_sem=st_ssem.at[hop], recv_sem=st_rsem.at[hop],
            device_id={"sp": across if hop == 1 else mate}, device_id_type=MESH)

    def keep_rows(which, layer, vals):
        for b in range(BLK):
            for j in range(NUM_STEPS):
                row_buf[which, layer, k * BLK + b, j:j + 1, :] = vals[j][b:b + 1]

        @pl.when(k < 3)
        def _():
            row_copy(which, layer).start()

    def long_conv(layer, f, j, vals):
        acc = cached_sum(layer, f, j)
        for i in range(j + 1):
            acc = acc + lags[layer, f, j - i:j - i + 1] * vals[i]
        return acc + gain_ref[layer, f:f + 1] * vals[j]

    proj_rows = [[None] * 3 for _ in range(NUM_LAYERS)]
    v_rows = [[], []]
    z_rows = [[], []]

    def y_copy(h, c, other):
        return pltpu.make_async_remote_copy(
            src_ref=x_send.at[3, h, c], dst_ref=y_recv.at[other, h, c], send_sem=y_ssem.at[other, h, c], recv_sem=y_rsem.at[other, h, c],
            device_id={"sp": across, "tp": (1 - t) if other else t}, device_id_type=MESH)

    def matmul_exchange(n, h, lhs, w_ref, base=None):
        for c in range(NCH):
            part = jnp.dot(lhs, w_ref[:, c * CW:(c + 1) * CW], preferred_element_type=F32)
            if base is not None:
                part = part + jnp.where(t == 0, base[:, c * CW:(c + 1) * CW], 0.0)
            x_send[n, h, c] = part
            if base is not None:
                y_copy(h, c, 1).start()
                y_copy(h, c, 0).start()
            x_copy(n, h, c).start()

    def add_exchange(n, h, base):
        outs = []
        for c in range(NCH):
            x_copy(n, h, c).wait_recv()
            outs.append(base[:, c * CW:(c + 1) * CW] + (x_send[n, h, c] + x_recv[n, h, c]))
        return jnp.concatenate(outs, axis=1)

    def front(layer, h, rows_in):
        normed = norm_rows(rows_in).astype(BF16)
        if layer == 1 and h == 0:
            w_copies[4].wait()
        mixed = []
        for g in range(3):
            proj = jnp.dot(normed, (w_in0 if layer == 0 else w_in)[g], preferred_element_type=F32) + b_in_ref[g, layer:layer + 1]
            proj = round_bf16(proj)
            if h == 0:
                proj_rows[layer][g] = [
                    jnp.concatenate([state[layer, k * BLK + b, g, s:s + 1].astype(F32) for b in range(BLK)], axis=0) for s in range(2)]
            seq = proj_rows[layer][g]
            seq += [proj[BLK * i:BLK * i + BLK] for i in range(GSTEPS)]
            tap = [taps_ref[i, g, layer:layer + 1] for i in range(3)]
            mixed.append([tap[0] * seq[j + 2] + tap[1] * seq[j + 1] + tap[2] * seq[j] for j in range(GSTEPS * h, GSTEPS * h + GSTEPS)])
        ys = []
        v_rows[layer] += [round_bf16(x) for x in mixed[2]]
        if layer == 1 and h == 0:
            for f in range(2):
                for d in range(1, 4):
                    rs_copy(f, d).wait_recv()
        for i in range(GSTEPS):
            a = long_conv(layer, 0, GSTEPS * h + i, v_rows[layer])
            z_rows[layer].append(round_bf16(mixed[0][i] * a))
            ys.append(mixed[1][i] * long_conv(layer, 1, GSTEPS * h + i, z_rows[layer]))
        if layer == 1 and h == 0:
            w_copies[5].wait()
        matmul_exchange(layer * 2, h, jnp.concatenate(ys, axis=0).astype(BF16), w_out0 if layer == 0 else w_out)

    def send_kept(layer):
        keep_rows(0, layer, v_rows[layer])
        keep_rows(1, layer, z_rows[layer])
    def middle(layer, h, rows_in):
        out = add_exchange(layer * 2, h, rows_in) + b_out_ref[layer:layer + 1]
        act = norm_rows(out).astype(BF16)
        if h == 0:
            w_copies[layer * 4 + 2].wait()
        inner = jax.nn.gelu(jnp.dot(act, w_up[layer], preferred_element_type=F32)).astype(BF16)
        if h == 0:
            w_copies[layer * 4 + 3].wait()
        matmul_exchange(layer * 2 + 1, h, inner, w_down.at[layer], out if layer == 1 else None)
        return out

    rows_in = []
    for h in range(GROUPS):
        emb32[...] = emb_ref[GSTEPS * h:GSTEPS * h + GSTEPS].astype(F32)
        rows_in.append(jnp.concatenate([emb32[i, own] for i in range(GSTEPS)], axis=0))
    for h in range(GROUPS):
        front(0, h, rows_in[h])
        if h == 0:
            w_copies[3].start()
    for copy in w_copies[4:6]:
        copy.start()
    for f in range(2):
        for d in range(1, 4):
            rs_copy(f, d).start()
    send_kept(0)
    outs = [middle(0, h, rows_in[h]) for h in range(GROUPS)]
    for copy in w_copies[6:8]:
        copy.start()

    normed = norm_rows(emb_ref[2:4].astype(F32).reshape(2 * SEQ, DIM)).astype(BF16)
    for g in range(3):
        proj = jnp.dot(normed, w_in0[g], preferred_element_type=F32) + b_in_ref[g, 0:1]
        for s in range(2):
            for b in range(SEQ):
                st0_buf[b, g, s:s + 1, :] = proj[s * SEQ + b:s * SEQ + b + 1]
    st_ref[0] = st0_buf[...].astype(BF16)

    rows_in = []
    for h in range(GROUPS):
        rows_in.append(add_exchange(1, h, outs[h]))
        front(1, h, rows_in[h])
    for g in range(3):
        for s in range(2):
            for i in range(BLK):
                st_buf[k * BLK + i, g, s:s + 1, :] = proj_rows[1][g][4 + s][i:i + 1]
    st_copy(1).start()
    st_copy(0).start()
    send_kept(1)
    outs = [middle(1, h, rows_in[h]) for h in range(GROUPS)]
    st_copy(1).wait_recv()
    st_copy(2).start()

    def g_copy(h, c, hop):
        piece = hid_buf.at[h, c, :, block_of(hop)]
        return pltpu.make_async_remote_copy(
            src_ref=piece, dst_ref=piece, send_sem=g_ssem.at[h, c, hop], recv_sem=g_rsem.at[h, c, hop],
            device_id={"sp": across if hop == 1 else mate}, device_id_type=MESH)

    chunks = [(h, c) for h in range(GROUPS) for c in range(NCH)]
    def keep_sum(h, c, total, hop):
        for i in range(GSTEPS):
            hid_buf[h, c, i, block_of(hop)] = total[BLK * i:BLK * i + BLK]
        g_copy(h, c, hop).start()

    for h in range(GROUPS):
        for c in range(NCH):
            x_copy(3, h, c).wait_recv()
            keep_sum(h, c, x_send[3, h, c] + x_recv[3, h, c], 0)
        for c in range(NCH):
            y_copy(h, c, 0).wait_recv()
            y_copy(h, c, 1).wait_recv()
            keep_sum(h, c, y_recv[0, h, c] + y_recv[1, h, c], 2)
    st_copy(0).wait_recv()
    st_copy(2).wait_recv()
    st_ref[1] = st_buf[...].astype(BF16)

    @pl.when(k == 3)
    def _():
        for layer in range(NUM_LAYERS):
            for which in range(2):
                for src in range(3):
                    row_copy(which, layer, src).wait_recv()
        rows_ref[...] = row_buf[...]

    for h, c in chunks:
        g_copy(h, c, 0).wait_recv()
        g_copy(h, c, 2).wait_recv()
        hid_ref[GSTEPS * h:GSTEPS * h + GSTEPS, :, c * CW:(c + 1) * CW] = hid_buf[h, c]

    for h, c in chunks:
        for n in range(4):
            x_copy(n, h, c).wait_send()
        for hop in (0, 2):
            g_copy(h, c, hop).wait_send()
        for other in range(2):
            y_copy(h, c, other).wait_send()
    for f in range(2):
        for d in range(1, 4):
            rs_copy(f, d).wait_send()
    for hop in range(3):
        st_copy(hop).wait_send()

    @pl.when(k < 3)
    def _():
        for layer in range(NUM_LAYERS):
            for which in range(2):
                row_copy(which, layer).wait_send()


def layer_call(sums0, parts1, step_emb, b_in, taps, gain, b_out, state, w_in0, w_out0, lags, w_in, w_out, w_up, w_down):
    vm = pl.BlockSpec(memory_space=pltpu.VMEM)
    hbm = pl.BlockSpec(memory_space=pltpu.HBM)
    dma = pltpu.SemaphoreType.DMA
    return pl.pallas_call(
        layer_kernel,
        out_shape=(
            jax.ShapeDtypeStruct((NUM_STEPS, SEQ, DIM), F32),
            jax.ShapeDtypeStruct((NUM_LAYERS, SEQ, 3, 2, CH), BF16),
            jax.ShapeDtypeStruct((2, NUM_LAYERS, SEQ, NUM_STEPS, CH), F32),
        ),
        in_specs=[vm] * 17 + [hbm] * 4,
        out_specs=[vm] * 3,
        scratch_shapes=[
            pltpu.VMEM(w_in.shape[1:], BF16),
            pltpu.VMEM(w_out.shape[1:], BF16),
            pltpu.VMEM(w_up.shape, BF16),
            pltpu.VMEM(w_down.shape, BF16),
            pltpu.VMEM((GSTEPS, SEQ, DIM), F32),
            pltpu.VMEM((3, 2, NUM_STEPS, BLK, CH), F32),
            pltpu.VMEM((SEQ, 3, 2, CH), F32),
            pltpu.VMEM((4, GROUPS, NCH, GSTEPS * BLK, CW), F32),
            pltpu.VMEM((4, GROUPS, NCH, GSTEPS * BLK, CW), F32),
            pltpu.VMEM((2, GROUPS, NCH, GSTEPS * BLK, CW), F32),
            pltpu.VMEM((GROUPS, NCH, GSTEPS, SEQ, CW), F32),
            pltpu.VMEM((SEQ, 3, 2, CH), F32),
            pltpu.VMEM((2, NUM_LAYERS, SEQ, NUM_STEPS, CH), F32),
            dma((NUM_LAYERS, 4)),
            dma((2, 3)),
            dma((2, 3)),
            dma((4, GROUPS, NCH)),
            dma((4, GROUPS, NCH)),
            dma((2, GROUPS, NCH)),
            dma((2, GROUPS, NCH)),
            dma((3,)),
            dma((3,)),
            dma((2, NUM_LAYERS)),
            dma((2, NUM_LAYERS, 4)),
            dma((GROUPS, NCH, 3)),
            dma((GROUPS, NCH, 3)),
        ],
        compiler_params=pltpu.CompilerParams(collective_id=0, has_side_effects=True, vmem_limit_bytes=44 << 20),
        name="layers",
    )(*sums0, *parts1, step_emb, b_in, taps, gain, b_out, state, w_in0, w_out0, lags, w_in, w_out, w_up, w_down)


def put_kernel(hid_in, st_in, rows_ref, v_in, z_in, hid_out, st_out, v_out, z_out, wide, tile, sems, o_sem):
    copies = [pltpu.make_async_copy(hid_in, hid_out, o_sem.at[0]), pltpu.make_async_copy(st_in, st_out, o_sem.at[1])]
    for copy in copies:
        copy.start()

    @pl.when(lax.axis_index("sp") == 3)
    def _():
        row_copies = []
        for which, dst in enumerate((v_out, z_out)):
            for layer in range(NUM_LAYERS):
                wide[:, 4:8, :] = jnp.zeros((SEQ, 4, CH), F32)
                wide[:, 0:4, :] = rows_ref[which, layer]
                tile[which, layer] = wide[...].astype(BF16)
                copy = pltpu.make_async_copy(tile.at[which, layer], dst.at[layer, :, 0:8, :], sems.at[which, layer])
                copy.start()
                row_copies.append(copy)
        for copy in row_copies:
            copy.wait()

    for copy in copies:
        copy.wait()


def put_call(hidden, states, rows, v_new, z_new):
    hbm = pl.BlockSpec(memory_space=pltpu.HBM)
    vm = pl.BlockSpec(memory_space=pltpu.VMEM)
    return pl.pallas_call(
        put_kernel,
        out_shape=(jax.ShapeDtypeStruct(hidden.shape, F32), jax.ShapeDtypeStruct(states.shape, BF16),
                   jax.ShapeDtypeStruct(v_new.shape, BF16), jax.ShapeDtypeStruct(z_new.shape, BF16)),
        in_specs=[vm] * 3 + [hbm] * 2,
        out_specs=[hbm] * 4,
        scratch_shapes=[
            pltpu.VMEM((SEQ, 8, CH), F32),
            pltpu.VMEM((2, NUM_LAYERS, SEQ, 8, CH), BF16),
            pltpu.SemaphoreType.DMA((2, NUM_LAYERS)),
            pltpu.SemaphoreType.DMA((2,)),
        ],
        input_output_aliases={3: 2, 4: 3},
        compiler_params=pltpu.CompilerParams(vmem_limit_bytes=16 << 20),
        name="put_rows",
    )(hidden, states, rows, v_new, z_new)


def solution(mesh):
    def device_fn(step_emb, v_cache, z_cache, short_state, w_in, b_in, short_taps, long_filt, skip_gain, w_out, b_out, w_up, w_down):
        v_cache, z_cache, long_filt, w_in, w_out, w_up, w_down = [
            pltpu.with_memory_space_constraint(x, pltpu.HBM)
            for x in (v_cache, z_cache, long_filt, jnp.transpose(w_in, (0, 2, 1, 3)), w_out, w_up, w_down)]
        v_new, z_new, *parts0, carry, rows_next = stream_call(0, v_cache, z_cache, long_filt)
        sums0 = [parts0[0]] + [lax.ppermute(parts0[d], "sp", [(i, (i + d) % 4) for i in range(4)]) for d in range(1, 4)]
        v_new, z_new, *parts1, w_in0, w_out0, lags = stream_call(1, v_cache, z_cache, v_new, z_new, carry, rows_next, w_in, w_out, long_filt)
        hidden, states, rows = layer_call(
            sums0, parts1, step_emb, jnp.transpose(b_in, (1, 0, 2)), jnp.transpose(short_taps, (1, 2, 0, 3)),
            skip_gain, b_out, jnp.transpose(short_state, (0, 1, 3, 2, 4)), w_in0, w_out0, lags,
            w_in, w_out, w_up, w_down)
        hidden, states, v_new, z_new = put_call(hidden, states, rows, v_new, z_new)
        return hidden, v_new, z_new, jnp.transpose(states, (0, 1, 3, 2, 4))

    specs_in = (
        P(None, "dp", None),
        P(None, "dp", "sp", "tp"),
        P(None, "dp", "sp", "tp"),
        P(None, "dp", None, None, "tp"),
        P(None, None, None, "tp"),
        P(None, None, "tp"),
        P(None, None, None, "tp"),
        P(None, None, None, "tp"),
        P(None, None, "tp"),
        P(None, "tp", None),
        P(None, None),
        P(None, None, "tp"),
        P(None, "tp", None),
    )
    specs_out = (
        P(None, "dp", None),
        P(None, "dp", "sp", "tp"),
        P(None, "dp", "sp", "tp"),
        P(None, "dp", None, None, "tp"),
    )
    return jax.shard_map(device_fn, mesh=mesh, in_specs=specs_in, out_specs=specs_out, check_vma=False)
```

```python
import functools

import jax
import jax.numpy as jnp
from jax import lax
from jax.experimental import pallas as pl
from jax.experimental.pallas import tpu as pltpu
from jax.sharding import PartitionSpec as P

F32 = jnp.float32
BF16 = jnp.bfloat16
NUM_STEPS = 4
NUM_LAYERS = 2
SEQ = 32
BLK = 8
DIM = 1024
CH = 512
UP = 2048
SHARD = 256
NCH = 1
CW = DIM // NCH
GROUPS = 2
GSTEPS = NUM_STEPS // GROUPS
MESH = pl.DeviceIdType.MESH


def pair_rows(lo, hi, shift):
    clear = (lax.broadcasted_iota(jnp.int32, (8, 128), 0) // shift) % 2 == 0
    if shift == 4:
        return jnp.where(clear, lo, hi) + pltpu.roll(jnp.where(clear, hi, lo), 4, 0)
    return jnp.where(clear, lo + pltpu.roll(lo, 8 - shift, 0), hi + pltpu.roll(hi, shift, 0))


def fill_window(win, filt_rows, ct):
    flip = 7 - lax.broadcasted_iota(jnp.int32, (8, 128), 0)
    lanes = pl.ds(pl.multiple_of(ct * 128, 128), 128)
    for m in range(SHARD // 8 + 1):
        rows = filt_rows[SHARD - 8 * m:SHARD - 8 * m + 8, lanes]
        win[ct, 8 * m:8 * m + 8] = jnp.take_along_axis(rows, flip, axis=0)


def conv_block(src, win, dst, ready):
    @pl.loop(0, CH // 128)
    def _(ct):
        ready(ct)
        lanes = pl.ds(pl.multiple_of(ct * 128, 128), 128)
        half = []
        for seqs in ((0, 4, 1, 5), (2, 6, 3, 7)):
            accs = [[None] * NUM_STEPS for _ in seqs]
            for pt in range(SHARD // 16):
                w = [[win[ct, 16 * pt + 8 * h + 7 - j:16 * pt + 8 * h + 15 - j] for h in range(2)] for j in range(NUM_STEPS)]
                for i, b in enumerate(seqs):
                    x = src[b, 16 * pt:16 * pt + 16, lanes].astype(F32)
                    for j in range(NUM_STEPS):
                        for h in range(2):
                            term = x[8 * h:8 * h + 8] * w[j][h]
                            accs[i][j] = term if accs[i][j] is None else accs[i][j] + term
            half.append([[pair_rows(accs[0][j], accs[1][j], 4), pair_rows(accs[2][j], accs[3][j], 4)] for j in range(NUM_STEPS)])
        for j in range(NUM_STEPS):
            dst[j, :, lanes] = pair_rows(pair_rows(half[0][j][0], half[1][j][0], 2), pair_rows(half[0][j][1], half[1][j][1], 2), 1)


def stream_kernel(layer, num_in, *refs):
    v_in, z_in = refs[:2]
    if layer == 0:
        filt = refs[2]
        v_out, z_out, *parts, carry, rows_next = refs[num_in:num_in + 8]
        ring, win, in_sem, out_sem, rows, filt_sem, lane_sem, carry_sem = refs[num_in + 8:]
    else:
        carry, rows, w_in_hbm, w_out_hbm, filt = refs[4:9]
        v_out, z_out, *parts, w_in0, w_out0, lags = refs[num_in:num_in + 9]
        ring, win, in_sem, out_sem, carry_sem = refs[num_in + 9:]
    units = [(f, d) for f in range(2) for d in range(4)]
    k = lax.axis_index("sp")
    first = pl.multiple_of(jnp.maximum(2 - k, 0) * SHARD, SHARD)

    def seqs(u):
        return pl.ds(pl.multiple_of(lax.rem(k + units[u][1], 4) * BLK, BLK), BLK)

    def slot(u):
        return carry if layer == 1 and u == 0 else ring.at[u]

    def in_copy(u):
        return pltpu.make_async_copy((v_in, z_in)[units[u][0]].at[layer, seqs(u)], ring.at[u], in_sem.at[u])

    def lane_copy(ct):
        lanes = pl.ds(pl.multiple_of(ct * 128, 128), 128)
        return pltpu.make_async_copy(v_in.at[0, seqs(0), :, lanes], ring.at[0, :, :, lanes], lane_sem.at[ct])

    def out_copy(u):
        return pltpu.make_async_copy(slot(u), (v_out, z_out)[units[u][0]].at[layer, seqs(u)], out_sem.at[u])

    def filt_copy(f):
        return pltpu.make_async_copy(filt.at[0, f, pl.ds(first, SHARD + 8)], rows.at[f], filt_sem.at[f])

    def carry_copies():
        if layer == 1:
            return [pltpu.make_async_copy(w_in_hbm.at[0], w_in0, carry_sem.at[0]),
                    pltpu.make_async_copy(w_out_hbm.at[0], w_out0, carry_sem.at[1]),
                    pltpu.make_async_copy(filt.at[:, :, 0:8], lags, carry_sem.at[2])]
        return [pltpu.make_async_copy(v_in.at[1, seqs(0)], carry, carry_sem.at[2])] + [
            pltpu.make_async_copy(filt.at[1, f, pl.ds(first, SHARD + 8)], rows_next.at[f], carry_sem.at[f]) for f in range(2)]

    reads = {0: (2,), 1: (3, 4), 2: (5, 6), 3: (7,)}
    writes = {3: (0, 1), 4: (2, 3), 5: (4, 5), 6: (6, 7)}
    if layer == 0:
        filt_copy(0).start()
        for ct in range(CH // 128):
            lane_copy(ct).start()
        filt_copy(0).wait()
    in_copy(1).start()
    for u, (f, d) in enumerate(units):
        if 0 < u < 7:
            in_copy(u).wait()
        if u == 6:
            in_copy(7).wait()
        for nxt in reads.get(u, ()):
            in_copy(nxt).start()
        for nxt in writes.get(u, ()):
            out_copy(nxt).start()
        if layer == 0 and u == 1:
            filt_copy(1).start()
        if layer == 0 and u == 4:
            filt_copy(1).wait()
        if u == (5 if layer == 0 else 4):
            for copy in carry_copies():
                copy.start()

        def ready(ct, u=u, f=f, d=d):
            if d == 0:
                fill_window(win, rows.at[f], ct)
            if layer == 0 and u == 0:
                lane_copy(ct).wait()

        conv_block(slot(u), win, parts[d].at[f], ready)
    for u in range(len(units)):
        out_copy(u).wait()
    for copy in carry_copies():
        copy.wait()


def stream_call(layer, *operands):
    hbm = pl.BlockSpec(memory_space=pltpu.HBM)
    vm = pl.BlockSpec(memory_space=pltpu.VMEM)
    cache = jax.ShapeDtypeStruct(operands[0].shape, BF16)
    outs = (cache, cache) + (jax.ShapeDtypeStruct((2, NUM_STEPS, BLK, CH), F32),) * 4
    scratch = [
        pltpu.VMEM((8, BLK, SHARD, CH), BF16),
        pltpu.VMEM((CH // 128, SHARD + 8, 128), F32),
        pltpu.SemaphoreType.DMA((8,)),
        pltpu.SemaphoreType.DMA((8,)),
    ]
    if layer == 0:
        in_specs = [hbm] * 3
        outs += (jax.ShapeDtypeStruct((BLK, SHARD, CH), BF16), jax.ShapeDtypeStruct((2, SHARD + 8, CH), F32))
        scratch += [
            pltpu.VMEM((2, SHARD + 8, CH), F32),
            pltpu.SemaphoreType.DMA((2,)),
            pltpu.SemaphoreType.DMA((CH // 128,)),
            pltpu.SemaphoreType.DMA((3,)),
        ]
    else:
        in_specs = [hbm] * 4 + [vm] * 2 + [hbm] * 3
        outs += (jax.ShapeDtypeStruct((3, DIM, CH), BF16), jax.ShapeDtypeStruct((CH, DIM), BF16),
                 jax.ShapeDtypeStruct((NUM_LAYERS, 2, 8, CH), F32))
        scratch += [pltpu.SemaphoreType.DMA((3,))]
    return pl.pallas_call(
        functools.partial(stream_kernel, layer, len(operands)),
        out_shape=outs,
        in_specs=in_specs,
        out_specs=[hbm] * 2 + [vm] * (len(outs) - 2),
        scratch_shapes=scratch,
        input_output_aliases={} if layer == 0 else {2: 0, 3: 1},
        cost_estimate=pl.CostEstimate(flops=SEQ * SHARD * CH * 16, bytes_accessed=4 * SEQ * SHARD * CH * 2, transcendentals=0),
        compiler_params=pltpu.CompilerParams(vmem_limit_bytes=30 << 20),
        name=f"stream_{layer}",
    )(*operands)


def norm_rows(rows_in):
    mean_val = jnp.mean(rows_in, axis=-1, keepdims=True)
    centered = rows_in - mean_val
    var_val = jnp.mean(centered * centered, axis=-1, keepdims=True)
    return centered * lax.rsqrt(var_val + 1e-5)


def round_bf16(x):
    return x.astype(BF16).astype(F32)


def layer_kernel(*refs):
    sums0 = refs[:4]
    parts1 = refs[4:8]
    (emb_ref, b_in_ref, taps_ref, gain_ref, b_out_ref, state, w_in0, w_out0, lags, w_in_hbm, w_out_hbm, w_up_hbm, w_down_hbm,
     hid_ref, st_ref, rows_ref,
     w_in, w_out, w_up, w_down, emb32, rs_buf, st0_buf, x_send, x_recv, y_recv, hid_buf, st_buf, row_buf,
     w_sem, rs_send, rs_recv, x_ssem, x_rsem, y_ssem, y_rsem, st_ssem, st_rsem, row_ssem, row_rsem, g_ssem, g_rsem) = refs[8:]
    k = lax.axis_index("sp")
    t = lax.axis_index("tp")
    others = [lax.rem(k + d, 4) for d in range(1, 4)]
    mate = k + 1 - 2 * lax.rem(k, 2)
    across = lax.rem(k + 2, 4)
    own = pl.ds(pl.multiple_of(k * BLK, BLK), BLK)

    w_pairs = ((w_in_hbm, w_in), (w_out_hbm, w_out), (w_up_hbm, w_up), (w_down_hbm, w_down))
    w_copies = [None if layer == 0 and idx < 2 else
                pltpu.make_async_copy(src.at[layer], dst if idx < 2 else dst.at[layer], w_sem.at[layer, idx])
                for layer in range(NUM_LAYERS) for idx, (src, dst) in enumerate(w_pairs)]
    w_copies[2].start()

    barrier = pltpu.get_barrier_semaphore()
    for dev in others:
        pl.semaphore_signal(barrier, inc=1, device_id={"sp": dev}, device_id_type=MESH)
    pl.semaphore_signal(barrier, inc=1, device_id={"tp": 1 - t}, device_id_type=MESH)
    pl.semaphore_signal(barrier, inc=1, device_id={"sp": across, "tp": 1 - t}, device_id_type=MESH)
    pl.semaphore_wait(barrier, 5)

    def rs_copy(f, d):
        return pltpu.make_async_remote_copy(
            src_ref=parts1[d].at[f], dst_ref=rs_buf.at[d - 1, f], send_sem=rs_send.at[f, d - 1], recv_sem=rs_recv.at[f, d - 1],
            device_id={"sp": others[d - 1]}, device_id_type=MESH)

    def cached_sum(layer, f, j):
        if layer == 0:
            return (sums0[0][f, j] + sums0[1][f, j]) + (sums0[2][f, j] + sums0[3][f, j])
        return (parts1[0][f, j] + rs_buf[0, f, j]) + (rs_buf[1, f, j] + rs_buf[2, f, j])

    def x_copy(n, h, c):
        return pltpu.make_async_remote_copy(
            src_ref=x_send.at[n, h, c], dst_ref=x_recv.at[n, h, c], send_sem=x_ssem.at[n, h, c], recv_sem=x_rsem.at[n, h, c],
            device_id={"tp": 1 - t}, device_id_type=MESH)

    def row_copy(which, layer, src=None):
        piece = row_buf.at[which, layer, own if src is None else pl.ds(src * BLK, BLK)]
        return pltpu.make_async_remote_copy(
            src_ref=piece, dst_ref=piece, send_sem=row_ssem.at[which, layer],
            recv_sem=row_rsem.at[which, layer, k if src is None else src],
            device_id={"sp": 3}, device_id_type=MESH)

    def block_of(hop):
        return pl.ds(pl.multiple_of((k if hop < 2 else across) * BLK, BLK), BLK)

    def st_copy(hop):
        piece = st_buf.at[block_of(hop)]
        return pltpu.make_async_remote_copy(
            src_ref=piece, dst_ref=piece, send_sem=st_ssem.at[hop], recv_sem=st_rsem.at[hop],
            device_id={"sp": across if hop == 1 else mate}, device_id_type=MESH)

    def keep_rows(which, layer, vals):
        for b in range(BLK):
            for j in range(NUM_STEPS):
                row_buf[which, layer, k * BLK + b, j:j + 1, :] = vals[j][b:b + 1]

        @pl.when(k < 3)
        def _():
            row_copy(which, layer).start()

    def long_conv(layer, f, j, vals):
        acc = cached_sum(layer, f, j)
        for i in range(j + 1):
            acc = acc + lags[layer, f, j - i:j - i + 1] * vals[i]
        return acc + gain_ref[layer, f:f + 1] * vals[j]

    proj_rows = [[None] * 3 for _ in range(NUM_LAYERS)]
    v_rows = [[], []]
    z_rows = [[], []]

    def y_copy(h, c, other):
        return pltpu.make_async_remote_copy(
            src_ref=x_send.at[3, h, c], dst_ref=y_recv.at[other, h, c], send_sem=y_ssem.at[other, h, c], recv_sem=y_rsem.at[other, h, c],
            device_id={"sp": across, "tp": (1 - t) if other else t}, device_id_type=MESH)

    def matmul_exchange(n, h, lhs, w_ref, base=None):
        for c in range(NCH):
            part = jnp.dot(lhs, w_ref[:, c * CW:(c + 1) * CW], preferred_element_type=F32)
            if base is not None:
                part = part + jnp.where(t == 0, base[:, c * CW:(c + 1) * CW], 0.0)
            x_send[n, h, c] = part
            if base is not None:
                y_copy(h, c, 1).start()
                y_copy(h, c, 0).start()
            x_copy(n, h, c).start()

    def add_exchange(n, h, base):
        outs = []
        for c in range(NCH):
            x_copy(n, h, c).wait_recv()
            outs.append(base[:, c * CW:(c + 1) * CW] + (x_send[n, h, c] + x_recv[n, h, c]))
        return jnp.concatenate(outs, axis=1)

    def front(layer, h, rows_in):
        normed = norm_rows(rows_in).astype(BF16)
        if layer == 1 and h == 0:
            w_copies[4].wait()
        mixed = []
        for g in range(3):
            proj = jnp.dot(normed, (w_in0 if layer == 0 else w_in)[g], preferred_element_type=F32) + b_in_ref[g, layer:layer + 1]
            proj = round_bf16(proj)
            if h == 0:
                proj_rows[layer][g] = [
                    jnp.concatenate([state[layer, k * BLK + b, g, s:s + 1].astype(F32) for b in range(BLK)], axis=0) for s in range(2)]
            seq = proj_rows[layer][g]
            seq += [proj[BLK * i:BLK * i + BLK] for i in range(GSTEPS)]
            tap = [taps_ref[i, g, layer:layer + 1] for i in range(3)]
            mixed.append([tap[0] * seq[j + 2] + tap[1] * seq[j + 1] + tap[2] * seq[j] for j in range(GSTEPS * h, GSTEPS * h + GSTEPS)])
        ys = []
        v_rows[layer] += [round_bf16(x) for x in mixed[2]]
        if layer == 1 and h == 0:
            for f in range(2):
                for d in range(1, 4):
                    rs_copy(f, d).wait_recv()
        for i in range(GSTEPS):
            a = long_conv(layer, 0, GSTEPS * h + i, v_rows[layer])
            z_rows[layer].append(round_bf16(mixed[0][i] * a))
            ys.append(mixed[1][i] * long_conv(layer, 1, GSTEPS * h + i, z_rows[layer]))
        if layer == 1 and h == 0:
            w_copies[5].wait()
        matmul_exchange(layer * 2, h, jnp.concatenate(ys, axis=0).astype(BF16), w_out0 if layer == 0 else w_out)

    def send_kept(layer):
        keep_rows(0, layer, v_rows[layer])
        keep_rows(1, layer, z_rows[layer])
    def middle(layer, h, rows_in):
        out = add_exchange(layer * 2, h, rows_in) + b_out_ref[layer:layer + 1]
        act = norm_rows(out).astype(BF16)
        if h == 0:
            w_copies[layer * 4 + 2].wait()
        inner = jax.nn.gelu(jnp.dot(act, w_up[layer], preferred_element_type=F32)).astype(BF16)
        if h == 0:
            w_copies[layer * 4 + 3].wait()
        matmul_exchange(layer * 2 + 1, h, inner, w_down.at[layer], out if layer == 1 else None)
        return out

    rows_in = []
    for h in range(GROUPS):
        emb32[...] = emb_ref[GSTEPS * h:GSTEPS * h + GSTEPS].astype(F32)
        rows_in.append(jnp.concatenate([emb32[i, own] for i in range(GSTEPS)], axis=0))
    for h in range(GROUPS):
        front(0, h, rows_in[h])
        if h == 0:
            w_copies[3].start()
    for copy in w_copies[4:6]:
        copy.start()
    for f in range(2):
        for d in range(1, 4):
            rs_copy(f, d).start()
    send_kept(0)
    outs = [middle(0, h, rows_in[h]) for h in range(GROUPS)]
    for copy in w_copies[6:8]:
        copy.start()

    normed = norm_rows(emb_ref[2:4].astype(F32).reshape(2 * SEQ, DIM)).astype(BF16)
    for g in range(3):
        proj = jnp.dot(normed, w_in0[g], preferred_element_type=F32) + b_in_ref[g, 0:1]
        for s in range(2):
            for b in range(SEQ):
                st0_buf[b, g, s:s + 1, :] = proj[s * SEQ + b:s * SEQ + b + 1]
    st_ref[0] = st0_buf[...].astype(BF16)

    rows_in = []
    for h in range(GROUPS):
        rows_in.append(add_exchange(1, h, outs[h]))
        front(1, h, rows_in[h])
    for g in range(3):
        for s in range(2):
            for i in range(BLK):
                st_buf[k * BLK + i, g, s:s + 1, :] = proj_rows[1][g][4 + s][i:i + 1]
    st_copy(1).start()
    st_copy(0).start()
    send_kept(1)
    outs = [middle(1, h, rows_in[h]) for h in range(GROUPS)]
    st_copy(1).wait_recv()
    st_copy(2).start()

    def g_copy(h, c, hop):
        piece = hid_buf.at[h, c, :, block_of(hop)]
        return pltpu.make_async_remote_copy(
            src_ref=piece, dst_ref=piece, send_sem=g_ssem.at[h, c, hop], recv_sem=g_rsem.at[h, c, hop],
            device_id={"sp": across if hop == 1 else mate}, device_id_type=MESH)

    chunks = [(h, c) for h in range(GROUPS) for c in range(NCH)]
    def keep_sum(h, c, total, hop):
        for i in range(GSTEPS):
            hid_buf[h, c, i, block_of(hop)] = total[BLK * i:BLK * i + BLK]
        g_copy(h, c, hop).start()

    for h in range(GROUPS):
        for c in range(NCH):
            x_copy(3, h, c).wait_recv()
            keep_sum(h, c, x_send[3, h, c] + x_recv[3, h, c], 0)
        for c in range(NCH):
            y_copy(h, c, 0).wait_recv()
            y_copy(h, c, 1).wait_recv()
            keep_sum(h, c, y_recv[0, h, c] + y_recv[1, h, c], 2)
    st_copy(0).wait_recv()
    st_copy(2).wait_recv()
    st_ref[1] = st_buf[...].astype(BF16)

    @pl.when(k == 3)
    def _():
        for layer in range(NUM_LAYERS):
            for which in range(2):
                for src in range(3):
                    row_copy(which, layer, src).wait_recv()
        rows_ref[...] = row_buf[...]

    for h, c in chunks:
        g_copy(h, c, 0).wait_recv()
        g_copy(h, c, 2).wait_recv()
        hid_ref[GSTEPS * h:GSTEPS * h + GSTEPS, :, c * CW:(c + 1) * CW] = hid_buf[h, c]

    for h, c in chunks:
        for n in range(4):
            x_copy(n, h, c).wait_send()
        for hop in (0, 2):
            g_copy(h, c, hop).wait_send()
        for other in range(2):
            y_copy(h, c, other).wait_send()
    for f in range(2):
        for d in range(1, 4):
            rs_copy(f, d).wait_send()
    for hop in range(3):
        st_copy(hop).wait_send()

    @pl.when(k < 3)
    def _():
        for layer in range(NUM_LAYERS):
            for which in range(2):
                row_copy(which, layer).wait_send()


def layer_call(sums0, parts1, step_emb, b_in, taps, gain, b_out, state, w_in0, w_out0, lags, w_in, w_out, w_up, w_down):
    vm = pl.BlockSpec(memory_space=pltpu.VMEM)
    hbm = pl.BlockSpec(memory_space=pltpu.HBM)
    dma = pltpu.SemaphoreType.DMA
    return pl.pallas_call(
        layer_kernel,
        out_shape=(
            jax.ShapeDtypeStruct((NUM_STEPS, SEQ, DIM), F32),
            jax.ShapeDtypeStruct((NUM_LAYERS, SEQ, 3, 2, CH), BF16),
            jax.ShapeDtypeStruct((2, NUM_LAYERS, SEQ, NUM_STEPS, CH), F32),
        ),
        in_specs=[vm] * 17 + [hbm] * 4,
        out_specs=[vm] * 3,
        scratch_shapes=[
            pltpu.VMEM(w_in.shape[1:], BF16),
            pltpu.VMEM(w_out.shape[1:], BF16),
            pltpu.VMEM(w_up.shape, BF16),
            pltpu.VMEM(w_down.shape, BF16),
            pltpu.VMEM((GSTEPS, SEQ, DIM), F32),
            pltpu.VMEM((3, 2, NUM_STEPS, BLK, CH), F32),
            pltpu.VMEM((SEQ, 3, 2, CH), F32),
            pltpu.VMEM((4, GROUPS, NCH, GSTEPS * BLK, CW), F32),
            pltpu.VMEM((4, GROUPS, NCH, GSTEPS * BLK, CW), F32),
            pltpu.VMEM((2, GROUPS, NCH, GSTEPS * BLK, CW), F32),
            pltpu.VMEM((GROUPS, NCH, GSTEPS, SEQ, CW), F32),
            pltpu.VMEM((SEQ, 3, 2, CH), F32),
            pltpu.VMEM((2, NUM_LAYERS, SEQ, NUM_STEPS, CH), F32),
            dma((NUM_LAYERS, 4)),
            dma((2, 3)),
            dma((2, 3)),
            dma((4, GROUPS, NCH)),
            dma((4, GROUPS, NCH)),
            dma((2, GROUPS, NCH)),
            dma((2, GROUPS, NCH)),
            dma((3,)),
            dma((3,)),
            dma((2, NUM_LAYERS)),
            dma((2, NUM_LAYERS, 4)),
            dma((GROUPS, NCH, 3)),
            dma((GROUPS, NCH, 3)),
        ],
        compiler_params=pltpu.CompilerParams(collective_id=0, has_side_effects=True, vmem_limit_bytes=44 << 20),
        name="layers",
    )(*sums0, *parts1, step_emb, b_in, taps, gain, b_out, state, w_in0, w_out0, lags, w_in, w_out, w_up, w_down)


def put_kernel(hid_in, st_in, rows_ref, v_in, z_in, hid_out, st_out, v_out, z_out, wide, tile, sems, o_sem):
    copies = [pltpu.make_async_copy(hid_in, hid_out, o_sem.at[0]), pltpu.make_async_copy(st_in, st_out, o_sem.at[1])]
    for copy in copies:
        copy.start()

    @pl.when(lax.axis_index("sp") == 3)
    def _():
        row_copies = []
        for which, dst in enumerate((v_out, z_out)):
            for layer in range(NUM_LAYERS):
                wide[:, 4:8, :] = jnp.zeros((SEQ, 4, CH), F32)
                wide[:, 0:4, :] = rows_ref[which, layer]
                tile[which, layer] = wide[...].astype(BF16)
                copy = pltpu.make_async_copy(tile.at[which, layer], dst.at[layer, :, 0:8, :], sems.at[which, layer])
                copy.start()
                row_copies.append(copy)
        for copy in row_copies:
            copy.wait()

    for copy in copies:
        copy.wait()


def put_call(hidden, states, rows, v_new, z_new):
    hbm = pl.BlockSpec(memory_space=pltpu.HBM)
    vm = pl.BlockSpec(memory_space=pltpu.VMEM)
    return pl.pallas_call(
        put_kernel,
        out_shape=(jax.ShapeDtypeStruct(hidden.shape, F32), jax.ShapeDtypeStruct(states.shape, BF16),
                   jax.ShapeDtypeStruct(v_new.shape, BF16), jax.ShapeDtypeStruct(z_new.shape, BF16)),
        in_specs=[vm] * 3 + [hbm] * 2,
        out_specs=[hbm] * 4,
        scratch_shapes=[
            pltpu.VMEM((SEQ, 8, CH), F32),
            pltpu.VMEM((2, NUM_LAYERS, SEQ, 8, CH), BF16),
            pltpu.SemaphoreType.DMA((2, NUM_LAYERS)),
            pltpu.SemaphoreType.DMA((2,)),
        ],
        input_output_aliases={3: 2, 4: 3},
        compiler_params=pltpu.CompilerParams(vmem_limit_bytes=16 << 20),
        name="put_rows",
    )(hidden, states, rows, v_new, z_new)


def solution(mesh):
    def device_fn(step_emb, v_cache, z_cache, short_state, w_in, b_in, short_taps, long_filt, skip_gain, w_out, b_out, w_up, w_down):
        v_cache, z_cache, long_filt, w_in, w_out, w_up, w_down = [
            pltpu.with_memory_space_constraint(x, pltpu.HBM)
            for x in (v_cache, z_cache, long_filt, jnp.transpose(w_in, (0, 2, 1, 3)), w_out, w_up, w_down)]
        v_new, z_new, *parts0, carry, rows_next = stream_call(0, v_cache, z_cache, long_filt)
        sums0 = [parts0[0]] + [lax.ppermute(parts0[d], "sp", [(i, (i + d) % 4) for i in range(4)]) for d in range(1, 4)]
        v_new, z_new, *parts1, w_in0, w_out0, lags = stream_call(1, v_cache, z_cache, v_new, z_new, carry, rows_next, w_in, w_out, long_filt)
        hidden, states, rows = layer_call(
            sums0, parts1, step_emb, jnp.transpose(b_in, (1, 0, 2)), jnp.transpose(short_taps, (1, 2, 0, 3)),
            skip_gain, b_out, jnp.transpose(short_state, (0, 1, 3, 2, 4)), w_in0, w_out0, lags,
            w_in, w_out, w_up, w_down)
        hidden, states, v_new, z_new = put_call(hidden, states, rows, v_new, z_new)
        return hidden, v_new, z_new, jnp.transpose(states, (0, 1, 3, 2, 4))

    specs_in = (
        P(None, "dp", None),
        P(None, "dp", "sp", "tp"),
        P(None, "dp", "sp", "tp"),
        P(None, "dp", None, None, "tp"),
        P(None, None, None, "tp"),
        P(None, None, "tp"),
        P(None, None, None, "tp"),
        P(None, None, None, "tp"),
        P(None, None, "tp"),
        P(None, "tp", None),
        P(None, None),
        P(None, None, "tp"),
        P(None, "tp", None),
    )
    specs_out = (
        P(None, "dp", None),
        P(None, "dp", "sp", "tp"),
        P(None, "dp", "sp", "tp"),
        P(None, "dp", None, None, "tp"),
    )
    return jax.shard_map(device_fn, mesh=mesh, in_specs=specs_in, out_specs=specs_out, check_vma=False)
```
